32 devices in a mesh: groups: 2 (over y), dp: 4 (over z), tensor: 4 (over x, core).
Axes of the slice: x: 2, y: 2, z: 4, core: 2. Of those that a mesh axis runs over, the one named last changes fastest.
Arguments:
- tokens: bfloat16 [4096, 4096], P(('groups', 'dp')), parts along dimension 0, may hold values from -6 to 6
- w_query: bfloat16 [4096, 4096], P('dp', 'tensor'), may hold values from -0.09375 to 0.09375
- w_key: bfloat16 [4096, 1024], P('dp', 'tensor'), may hold values from -0.09375 to 0.09375
- w_value: bfloat16 [4096, 1024], P('dp', 'tensor'), may hold values from -0.09375 to 0.09375
- a_query: bfloat16 [8, 4096, 32], P(('groups', 'dp'), 'tensor'), parts along dimension 0, may hold values from -0.09375 to 0.09375
- b_query: bfloat16 [8, 32, 4096], P(('groups', 'dp'), None, 'tensor'), parts along dimension 0, may hold values from -1 to 1
- a_value: bfloat16 [8, 4096, 32], P(('groups', 'dp'), 'tensor'), parts along dimension 0, may hold values from -0.09375 to 0.09375
- b_value: bfloat16 [8, 32, 1024], P(('groups', 'dp'), None, 'tensor'), parts along dimension 0, may hold values from -1 to 1
- adapter_ranks: int32 [8], P('groups'), parts along dimension 0, may hold values from 16 to 32
- adapter_slot: int32 [4], replicated, may hold values from 0 to 3, each once
- block_adapter: int32 [32, 1], P(('groups', 'dp')), parts along dimension 0, may hold values from 0 to 3
- live_tokens: int32 [8], P(('groups', 'dp')), parts along dimension 0, may hold values from 1 to 512, 1280 in all
- d_heads: bfloat16 [4096, 4096], P(('groups', 'dp'), 'tensor'), parts along dimension 0, may hold values from -0.29882812 to 0.29882812
Outputs:
- grad_a_query: float32 [8, 4096, 32], P(('groups', 'dp'), 'tensor'), parts along dimension 0
- grad_b_query: float32 [8, 32, 4096], P(('groups', 'dp'), None, 'tensor'), parts along dimension 0
- grad_a_value: float32 [8, 4096, 32], P(('groups', 'dp'), 'tensor'), parts along dimension 0
- grad_b_value: float32 [8, 32, 1024], P(('groups', 'dp'), None, 'tensor'), parts along dimension 0
The draws below stay inside these ranges and needn't reach their ends.
There are 2 independent parts, one for each index of `groups`. The reference program is written for one: setup_inputs(seed, part) draws one part's arguments, and reference() takes and returns one part's arrays. A program takes and returns all parts, laid end to end along the dimension named above; an argument that names none is the same for every part. Nothing has to cross between parts.
Inputs may be any that keep to these rules, and one draw needn't show every extreme that they name: `adapter_slot`: each slot holds exactly one adapter. `block_adapter`: every adapter is named by some block. `live_tokens`: one index of dp has all its rows live.
All inputs are finite; a program needn't handle non-finite values. No bound on the sum of `live_tokens` on one device may be relied on, other than what follows from the above.
Results may differ from the reference program's by a relative error of at most 0.02.
Values may be sent and summed in bfloat16 or wider, within the bound.
A program may use at most 64 MiB of HBM per device.

```python
import math
import jax
import jax.numpy as jnp
import numpy as np
from jax import lax

D = 4096
HEADS = 32
KVH = 8
HD = 128
R = 32
REQUEST_ROWS = 128
BLOCKS_DEV = 4
TOK_DEV = 512
TOKENS = 2048
ADAPTERS = 4
N_DP = 4


def touch_ends(result, rng, low, top_value):
    index_at = [jax.random.randint(jax.random.fold_in(rng, axis), (), 0, length) for axis, length in enumerate(result.shape)]
    widest = result.shape.index(max(result.shape))
    next_to = index_at[:widest] + [(index_at[widest] + 1) % result.shape[widest]] + index_at[widest + 1:]
    return result.at[tuple(index_at)].set(low).at[tuple(next_to)].set(top_value)


def block_scale(key, extent, pieces, low, top_value):
    def one(dim, blocks):
        steps = jax.random.uniform(jax.random.fold_in(jax.random.fold_in(key, 6), dim), (blocks,), jnp.float32, low / len(pieces), top_value / len(pieces))
        return jnp.repeat(jnp.exp(steps), extent[dim] // blocks).reshape((-1,) + (1,) * (len(extent) - dim - 1))

    gain = one(*pieces[0])
    for cut in pieces[1:]:
        gain = gain * one(*cut)
    return gain


def distinct(own_key, rows, number_of, top, lift):
    sequence = jax.random.permutation(jax.random.fold_in(own_key, 1), number_of)
    boost = sequence
    for power in range(3):
        boost = boost * boost // number_of
    boost = boost * lift // number_of
    chance = jax.random.randint(jax.random.fold_in(own_key, 2), (rows, number_of), 0, 4096) + boost
    sure = jax.random.permutation(jax.random.fold_in(own_key, 3), rows)[jnp.arange(number_of) % rows]
    chance = jnp.where(jnp.arange(rows)[:, None] == sure[None, :], 1 << 14, chance)
    priority = chance * number_of + jnp.arange(number_of)
    return lax.top_k(priority.astype(jnp.int32), top)[1].astype(jnp.int32)


def split_up(number_of, total, bound, skew):
    portions = [(1 << 20) // math.isqrt(grade ** skew) + 1 for grade in range(2, number_of + 1)]
    surplus, given = total - bound - (number_of - 1), [1] * (number_of - 1)
    while surplus > 0:
        free = [i for i in range(number_of - 1) if given[i] < bound]
        pool, budget = sum([portions[i] for i in free]), surplus
        for i in free:
            more = min(bound - given[i], max(1, budget * portions[i] // pool), surplus)
            given[i] = given[i] + more
            surplus = surplus - more
    return np.array([bound] + given)


def uneven(own_key, number_of, total, bound, skew):
    if number_of == 2:
        one = jax.random.randint(own_key, (), max(1, total - bound), min(bound, total - 1) + 1)
        return jnp.stack([one, total - one])
    lengths = jnp.asarray(split_up(number_of, total, bound, skew), jnp.int32)
    pairs = (number_of - 1) // 2
    source_of, receiver = lengths[1:1 + 2 * pairs:2], lengths[2:2 + 2 * pairs:2]
    slack = jnp.minimum(source_of - 1, bound - receiver)
    passed = jax.random.randint(jax.random.fold_in(own_key, 1), (pairs,), 0, 1 << 20) % (slack + 1)
    lengths = lengths.at[1:1 + 2 * pairs:2].set(source_of - passed).at[2:2 + 2 * pairs:2].set(receiver + passed)
    return lengths[jax.random.permutation(jax.random.fold_in(own_key, 2), number_of)]


def centred(rng, dims, scale, bound, split=(), kind=jnp.bfloat16):
    array = jax.random.normal(rng, dims, jnp.float32) * scale
    if len(split) > 0:
        array = block_scale(rng, dims, split, -0.22, 0.18) * array
    return jnp.clip(array, min=-bound, max=bound).astype(kind)


def setup_inputs(seed: int = 0, part: int = 0) -> dict:
    arg_keys = jax.random.split(jax.random.key(seed), 14)
    part_splits = jax.random.split(jax.random.fold_in(arg_keys[13], part), 14)
    tokens = centred(part_splits[0], (TOKENS, D), 1.0, 6.0, ((0, 4),))
    w_query = centred(arg_keys[1], (D, HEADS * HD), D ** -0.5, 0.09375, ((0, 4), (1, 4)))
    w_key = centred(arg_keys[2], (D, KVH * HD), D ** -0.5, 0.09375, ((0, 4), (1, 4)))
    w_value = centred(arg_keys[3], (D, KVH * HD), D ** -0.5, 0.09375, ((0, 4), (1, 4)))
    a_query = centred(part_splits[4], (ADAPTERS, D, R), D ** -0.5, 0.09375, ((0, 4), (1, 4)))
    b_query = centred(part_splits[5], (ADAPTERS, R, HEADS * HD), R ** -0.5, 1.0, ((0, 4), (2, 4)))
    a_value = centred(part_splits[6], (ADAPTERS, D, R), D ** -0.5, 0.09375, ((0, 4), (1, 4)))
    b_value = centred(part_splits[7], (ADAPTERS, R, KVH * HD), R ** -0.5, 1.0, ((0, 4), (2, 4)))
    adapter_ranks = touch_ends(jax.random.randint(part_splits[8], (ADAPTERS,), R // 2, R + 1), jax.random.fold_in(part_splits[8], 1), R // 2, R).astype(jnp.int32)
    adapter_slot = jax.random.permutation(arg_keys[9], ADAPTERS).astype(jnp.int32)
    block_adapter = distinct(part_splits[10], (TOKENS // REQUEST_ROWS), ADAPTERS, 1, 4096)
    live_tokens = uneven(part_splits[11], N_DP, N_DP * TOK_DEV * 5 // 8, TOK_DEV, 2).astype(jnp.int32)
    d_heads = centred(part_splits[12], (TOKENS, HEADS * HD), 0.05, 0.29882812, ((0, 4), (1, 4)))
    return {"tokens": tokens, "w_query": w_query, "w_key": w_key, "w_value": w_value, "a_query": a_query, "b_query": b_query, "a_value": a_value, "b_value": b_value, "adapter_ranks": adapter_ranks, "adapter_slot": adapter_slot, "block_adapter": block_adapter, "live_tokens": live_tokens, "d_heads": d_heads}


adapter_alpha_factor = 32.0
rope_theta = 500000.0


def rope_tables(length, width):
    halfway = width // 2
    spread = rope_theta ** (-2.0 * jnp.arange(halfway, dtype=jnp.float32) / width)
    angle = jnp.arange(length, dtype=jnp.float32)[:, None] * spread[None, :]
    return jnp.cos(angle), jnp.sin(angle)


def rotate(value_matrix, cosine, sine):
    halfway = value_matrix.shape[-1] // 2
    first = value_matrix[..., :halfway]
    second = value_matrix[..., halfway:]
    cos_grid = cosine[:, None, :]
    sin_grid = sine[:, None, :]
    return jnp.concatenate([first * cos_grid - second * sin_grid, second * cos_grid + first * sin_grid], axis=-1)


def attention_grads(queries, keys, value_matrix, dout, allowed, group):
    request_block_count, length, heads, depth = queries.shape
    kv_heads = keys.shape[2]
    grouped_q = queries.reshape(request_block_count, length, kv_heads, group, depth).astype(jnp.float32)
    grouped_d = dout.reshape(request_block_count, length, kv_heads, group, depth).astype(jnp.float32)
    key_rows = keys.astype(jnp.float32)
    value_rows = value_matrix.astype(jnp.float32)
    scores = jnp.einsum("ntkge,nske->nkgts", grouped_q, key_rows) * (depth ** -0.5)
    scores = jnp.where(allowed[:, None, None], scores, -1e30)
    summit = jnp.max(scores, axis=-1, keepdims=True)
    expo = jnp.exp(scores - summit)
    probs = expo / jnp.sum(expo, axis=-1, keepdims=True)
    dprobs = jnp.einsum("ntkge,nske->nkgts", grouped_d, value_rows)
    dscores = probs * (dprobs - jnp.sum(dprobs * probs, axis=-1, keepdims=True))
    dscore_b = dscores.astype(jnp.bfloat16).astype(jnp.float32)
    dquery = jnp.einsum("nkgts,nske->ntkge", dscore_b, key_rows) * (depth ** -0.5)
    prob_b = probs.astype(jnp.bfloat16).astype(jnp.float32)
    dvalue = jnp.einsum("nkgts,ntkge->nske", prob_b, grouped_d)
    return dquery.reshape(request_block_count, length, heads, depth), dvalue


def reference(tokens, w_query, w_key, w_value, a_query, b_query, a_value, b_value, adapter_ranks, adapter_slot, block_adapter, live_tokens, d_heads):
    cosine, sine = rope_tables(REQUEST_ROWS, HD)
    group = HEADS // KVH
    position = jnp.arange(REQUEST_ROWS, dtype=jnp.int32)
    causal = position[None, :] <= position[:, None]
    diagonal = position[None, :] == position[:, None]
    slot_grid = jnp.arange(ADAPTERS, dtype=jnp.int32)
    rank_grid = jnp.arange(R, dtype=jnp.int32)
    row_index = jnp.arange(TOK_DEV, dtype=jnp.int32).reshape(BLOCKS_DEV, REQUEST_ROWS)

    def device_terms(carry, inputs):
        tok_rows, block_ids, count, dout_rows = inputs
        slot_ids = adapter_slot[block_ids].astype(jnp.int32)
        rank_index_list = adapter_ranks[block_ids]
        adapter_scale = (adapter_alpha_factor / rank_index_list.astype(jnp.float32))[:, None, None]
        keep = (rank_grid[None, :] < rank_index_list[:, None]).astype(jnp.float32)[:, None, :]
        block_tokens = tok_rows.reshape(BLOCKS_DEV, REQUEST_ROWS, D).astype(jnp.float32)
        aq_sel = a_query[slot_ids].astype(jnp.float32)
        av_sel = a_value[slot_ids].astype(jnp.float32)
        selected_query_up = b_query[slot_ids].astype(jnp.float32)
        selected_value_up = b_value[slot_ids].astype(jnp.float32)
        query_down_weight = (jnp.einsum("ntd,ndr->ntr", block_tokens, aq_sel) * keep).astype(jnp.bfloat16).astype(jnp.float32)
        value_down_weight = (jnp.einsum("ntd,ndr->ntr", block_tokens, av_sel) * keep).astype(jnp.bfloat16).astype(jnp.float32)
        frozen_query = jnp.dot(tok_rows, w_query, preferred_element_type=jnp.float32).reshape(BLOCKS_DEV, REQUEST_ROWS, HEADS * HD)
        full_q = frozen_query + adapter_scale * jnp.einsum("zwf,zfy->zwy", query_down_weight, selected_query_up)
        queries = rotate(full_q.reshape(BLOCKS_DEV, REQUEST_ROWS, HEADS, HD), cosine, sine).astype(jnp.bfloat16)
        base_k = jnp.dot(tok_rows, w_key, preferred_element_type=jnp.float32).reshape(BLOCKS_DEV, REQUEST_ROWS, KVH, HD)
        keys = rotate(base_k, cosine, sine).astype(jnp.bfloat16)
        frozen_value = jnp.dot(tok_rows, w_value, preferred_element_type=jnp.float32).reshape(BLOCKS_DEV, REQUEST_ROWS, KVH * HD)
        value_matrix = (frozen_value + adapter_scale * jnp.einsum("zwf,zfy->zwy", value_down_weight, selected_value_up)).astype(jnp.bfloat16)
        value_matrix = value_matrix.reshape(BLOCKS_DEV, REQUEST_ROWS, KVH, HD)
        live = row_index < count
        allowed = causal[None] & (live[:, None, :] | diagonal[None])
        dout = jnp.where(live[:, :, None], dout_rows.reshape(BLOCKS_DEV, REQUEST_ROWS, HEADS * HD), jnp.zeros((), jnp.bfloat16))
        dquery, dvalue = attention_grads(queries, keys, value_matrix, dout.reshape(BLOCKS_DEV, REQUEST_ROWS, HEADS, HD), allowed, group)
        grad_q = rotate(dquery, cosine, -sine).reshape(BLOCKS_DEV, REQUEST_ROWS, HEADS * HD).astype(jnp.bfloat16).astype(jnp.float32)
        grad_v = dvalue.reshape(BLOCKS_DEV, REQUEST_ROWS, KVH * HD).astype(jnp.bfloat16).astype(jnp.float32)
        up_q = adapter_scale * jnp.einsum("ntr,ntc->nrc", query_down_weight, grad_q)
        up_v = adapter_scale * jnp.einsum("ntr,ntc->nrc", value_down_weight, grad_v)
        back_q = (adapter_scale * jnp.einsum("ntc,nrc->ntr", grad_q, selected_query_up) * keep).astype(jnp.bfloat16).astype(jnp.float32)
        back_v = (adapter_scale * jnp.einsum("ntc,nrc->ntr", grad_v, selected_value_up) * keep).astype(jnp.bfloat16).astype(jnp.float32)
        low_q = jnp.einsum("ntd,ntr->ndr", block_tokens, back_q)
        low_v = jnp.einsum("ntd,ntr->ndr", block_tokens, back_v)
        onehot = (slot_grid[:, None] == slot_ids[None, :]).astype(jnp.float32)
        terms = (low_q, up_q, low_v, up_v)
        placed = tuple(jnp.einsum("an,nxy->axy", onehot, item).astype(jnp.bfloat16).astype(jnp.float32) for item in terms)
        return tuple(total + extra for total, extra in zip(carry, placed)), None

    start = (jnp.zeros((ADAPTERS, D, R), jnp.float32), jnp.zeros((ADAPTERS, R, HEADS * HD), jnp.float32),
             jnp.zeros((ADAPTERS, D, R), jnp.float32), jnp.zeros((ADAPTERS, R, KVH * HD), jnp.float32))
    inputs = (tokens.reshape(N_DP, TOK_DEV, D), block_adapter.reshape(N_DP, BLOCKS_DEV), live_tokens,
              d_heads.reshape(N_DP, TOK_DEV, HEADS * HD))
    totals, unused = lax.scan(device_terms, start, inputs)
    return (totals[0], totals[1], totals[2], totals[3])
```

```python
import functools

import jax
import jax.numpy as jnp
import numpy as np
from jax import lax
from jax.experimental import pallas as pl
from jax.experimental.pallas import tpu as pltpu
from jax.sharding import PartitionSpec as P

HD = 128
R = 32
REQUEST_ROWS = 128
MESH = pl.DeviceIdType.MESH

adapter_alpha_factor = 32.0
rope_theta = 500000.0

SUBS = 4
TOKEN_SUBS = 2
FACTORS = 1


def rope_tables(length, width):
    halfway = width // 2
    spread = rope_theta ** (-2.0 * np.arange(halfway, dtype=np.float32) / width)
    angle = np.arange(length, dtype=np.float32)[:, None] * spread.astype(np.float32)[None, :]
    return np.cos(angle).astype(np.float32), np.sin(angle).astype(np.float32)


def scale_of(rank):
    return (adapter_alpha_factor / jnp.full((1, 128), rank, jnp.int32).astype(jnp.float32))[:, :1]


def dot(a, c, left, right):
    return lax.dot_general(
        a, c, (((left,), (right,)), ((), ())), preferred_element_type=jnp.float32
    )


def layer_kernel(
    G,
    block_ref,
    slot_ref,
    rank_ref,
    live_ref,
    x_hbm,
    wq_hbm,
    wk_hbm,
    wv_hbm,
    aq_hbm,
    av_hbm,
    bq_hbm,
    bv_hbm,
    d_hbm,
    cos_ref,
    sin_ref,
    lowq_out,
    lowv_out,
    upq_out,
    upv_out,
    x_all,
    w_kv,
    w_a,
    w_b,
    down_all,
    b_all,
    d_all,
    acc_kv,
    acc_a,
    acc_b,
    parts,
    u_all,
    keys_all,
    values_all,
    gv_acc,
    back_acc,
    upq_sum,
    upv_sum,
    upq_send,
    upv_send,
    upq_got,
    upv_got,
    back_send,
    back_got,
    low_send,
    low_got,
    meta,
    local_sem,
    z_send,
    z_recv,
    yb_send,
    yb_recv,
    yt_send,
    yt_recv,
    tx_send,
    tx_recv,
    tp_send,
    tp_recv,
    part_send,
    part_recv,
    yu_send,
    yu_recv,
    us_send,
    us_recv,
    bk_send,
    bk_recv,
    lo_send,
    lo_recv,
):
    n = lax.axis_size("dp")
    ng = lax.axis_size("groups")
    nt = lax.axis_size("tensor")
    me = lax.axis_index("dp")
    g = lax.axis_index("groups")
    t = lax.axis_index("tensor")
    split = G > 1
    gi = g if split else 0
    rows = x_hbm.shape[0]
    depth, qcols = wq_hbm.shape
    kcols = wk_hbm.shape[1]
    hq, hk = qcols // G, kcols // G
    hc = hq // 2
    kv_heads = hk // HD
    group = hq // hk
    blocks = rows // REQUEST_ROWS
    width = down_all.shape[2]
    step = depth // SUBS
    weights = (w_kv, None, w_a, w_b)
    accs = (acc_kv, None, acc_a, acc_b)

    def at_group(index, **rest):
        if split:
            rest["groups"] = index
        return rest

    def remote(src, dst, send, recv, to):
        return pltpu.make_async_remote_copy(
            src_ref=src, dst_ref=dst, send_sem=send, recv_sem=recv, device_id=to, device_id_type=MESH
        )

    mine = pl.ds(pl.multiple_of(me * depth, depth), depth)
    qs = pl.ds(pl.multiple_of(gi * hq, 128), hq)
    ks = pl.ds(pl.multiple_of(gi * hk, 128), hk)
    loads = [
        (wk_hbm.at[:, ks], w_kv.at[mine, pl.ds(0, hk)]),
        (wv_hbm.at[:, ks], w_kv.at[mine, pl.ds(hk, hk)]),
        (aq_hbm, down_all.at[me, pl.ds(0, R), :]),
        (av_hbm, down_all.at[me, pl.ds(R, R), :]),
        (bq_hbm.at[:, qs], b_all.at[me, gi, :, pl.ds(0, hq)]),
        (bv_hbm.at[:, ks], b_all.at[me, gi, :, pl.ds(hq, hk)]),
        (wq_hbm.at[:, pl.ds(pl.multiple_of(gi * hq, 128), hc)], w_a.at[mine, :]),
        (wq_hbm.at[:, pl.ds(pl.multiple_of(gi * hq + hc, 128), hc)], w_b.at[mine, :]),
        (x_hbm, x_all.at[gi]),
        (d_hbm.at[:, qs], d_all.at[gi]),
    ]
    loads = [pltpu.make_async_copy(s, d, local_sem.at[i]) for i, (s, d) in enumerate(loads)]
    for copy in loads:
        copy.start()

    for b in range(blocks):
        adapter = block_ref[b]
        meta[gi, b] = slot_ref[adapter]
        meta[gi, blocks + b] = rank_ref[adapter]
    meta[gi, 2 * blocks] = live_ref[0]

    barrier = pltpu.get_barrier_semaphore()

    @pl.loop(1, n * G)
    def _(j):
        k = lax.rem(me * G + gi + j, n * G)
        pl.semaphore_signal(
            barrier, inc=1, device_id=at_group(lax.rem(k, G), dp=lax.div(k, G)), device_id_type=MESH
        )

    for j in range(1, nt):
        for e in range(G):
            pl.semaphore_signal(
                barrier,
                inc=1,
                device_id=at_group(lax.rem(gi + e, G), tensor=lax.rem(t + j, nt)),
                device_id_type=MESH,
            )
    pl.semaphore_wait(barrier, n * G - 1 + G * (nt - 1))

    def z_copy(item, s, p, way):
        if item == FACTORS:
            ref = down_all.at[s] if p == 0 else b_all.at[s]
        else:
            ref = weights[item].at[pl.ds(pl.multiple_of(s * depth + p * step, step), step), :]
        target = jnp.clip(me + (1 if way == 0 else -1), 0, n - 1)
        return remote(
            ref, ref, z_send.at[way, item, s, p], z_recv.at[item, s, p], {"dp": target}
        )

    def pieces_of(item):
        return range(2) if item == FACTORS else range(SUBS)

    def send_own(item, pieces=None):
        for p in pieces_of(item) if pieces is None else pieces:

            @pl.when(me < n - 1)
            def _():
                z_copy(item, me, p, 0).start()

            @pl.when(me > 0)
            def _():
                z_copy(item, me, p, 1).start()

    def forward(item, d):
        for p in pieces_of(item):
            for way in (0, 1):
                s = me - d if way == 0 else me + d
                valid = (s >= 0) if way == 0 else (s < n)
                onward = (me < n - 1) if way == 0 else (me > 0)

                @pl.when(valid)
                def _():
                    z_copy(item, s, p, way).wait_recv()

                    @pl.when(onward)
                    def _():
                        z_copy(item, s, p, way).start()

    def line(item, after=None, hooks=()):
        hooks = dict(hooks)
        if n <= 8:
            for d in range(1, n):
                forward(item, d)
                if after is not None:
                    after(d)
                if d in hooks:
                    hooks.pop(d)()
        else:

            @pl.loop(1, n)
            def _(d):
                forward(item, d)
                if after is not None:
                    after(d)

        for hook in hooks.values():
            hook()

    def y_copies(j, arriving):
        peer = lax.rem(gi + G - j, G) if arriving else lax.rem(gi + j, G)
        at = peer if arriving else gi
        to = {"groups": peer}
        pq = pl.ds(pl.multiple_of(peer * hq, 128), hq)
        pk = pl.ds(pl.multiple_of(peer * hk, 128), hk)
        sources = (
            (bq_hbm.at[:, pq], b_all.at[me, at, :, pl.ds(0, hq)]),
            (bv_hbm.at[:, pk], b_all.at[me, at, :, pl.ds(hq, hk)]),
            (meta.at[at], meta.at[at]),
            (d_hbm.at[:, pq], d_all.at[at]),
        )
        return [
            remote(s, d, yb_send.at[j, i], yb_recv.at[j, i], to) for i, (s, d) in enumerate(sources)
        ]

    quarter = rows // nt
    sub = quarter // TOKEN_SUBS

    def token_piece(at, q, k):
        return x_all.at[at, pl.ds(pl.multiple_of(q * quarter + k * sub, sub), sub), :]

    def yt_copy(j, k, arriving):
        peer = lax.rem(gi + G - j, G) if arriving else lax.rem(gi + j, G)
        ref = token_piece(peer if arriving else gi, t, k)
        return remote(ref, ref, yt_send.at[j, k], yt_recv.at[j, k], {"groups": peer})

    pairs = nt // 2
    partner = t + 1 - 2 * lax.rem(t, 2)

    def tx_copy(j, i, k, arriving):
        at = lax.rem(gi + G - j, G)
        peer = lax.rem(t + nt - 2 * i, nt) if arriving else lax.rem(t + 2 * i, nt)
        ref = token_piece(at, peer if arriving else t, k)
        return remote(ref, ref, tx_send.at[j, i, k], tx_recv.at[j, i, k], {"tensor": peer})

    def tp_copy(j, q, k):
        at = lax.rem(gi + G - j, G)
        ref = token_piece(at, q, k)
        return remote(ref, ref, tp_send.at[j, q, k], tp_recv.at[j, q, k], {"tensor": partner})

    def relay_tokens(k):
        for j in range(1, G):
            yt_copy(j, k, True).wait_recv()
            for i in range(1, pairs):
                tx_copy(j, i, k, False).start()
            tp_copy(j, t, k).start()

    def pass_tokens():
        for j in range(1, G):
            for k in range(TOKEN_SUBS):
                for i in range(1, pairs):
                    tx_copy(j, i, k, True).wait_recv()
                    tp_copy(j, lax.rem(t + nt - 2 * i, nt), k).start()

    def settle_tokens():
        for j in range(1, G):
            for k in range(TOKEN_SUBS):
                for i in range(pairs):
                    tp_copy(j, lax.rem(partner + 2 * i, nt), k).wait_recv()

    tile = 256 if rows % 256 == 0 else 128

    def whole_product(item, r):
        @pl.loop(0, rows // tile)
        def _(i):
            span = pl.ds(pl.multiple_of(i * tile, tile), tile)
            accs[item][r, span, :] = jnp.dot(
                x_all[r, span, :], weights[item][...], preferred_element_type=jnp.float32
            )

    def slice_product(item, s, first):
        k_span = pl.ds(pl.multiple_of(s * depth, 128), depth)

        @pl.loop(0, G * rows // tile)
        def _(i):
            r = lax.div(i, rows // tile)
            span = pl.ds(pl.multiple_of(lax.rem(i, rows // tile) * tile, tile), tile)
            new = jnp.dot(
                x_all[r, span, k_span],
                weights[item][k_span, :],
                preferred_element_type=jnp.float32,
            )
            if first:
                accs[item][r, span, :] = new
            else:
                accs[item][r, span, :] += new

    cosine, sine = cos_ref[...], sin_ref[...]
    dims = (REQUEST_ROWS, REQUEST_ROWS)
    query_at = lax.broadcasted_iota(jnp.int32, dims, 0)
    key_at = lax.broadcasted_iota(jnp.int32, dims, 1)

    def turn(item, sign):
        return item * cosine + pltpu.roll(item, HD // 2, 1) * (sign * sine)

    def attend(index, ci):
        r, b = lax.div(index, blocks), lax.rem(index, blocks)
        span = pl.ds(pl.multiple_of(b * REQUEST_ROWS, REQUEST_ROWS), REQUEST_ROWS)
        slot = meta[r, b]
        scale = scale_of(meta[r, blocks + b])
        live = meta[r, 2 * blocks] - b * REQUEST_ROWS
        u = u_all[r, :, span]
        if ci == 0:
            added = scale * dot(u[R:], b_all[slot, r, :, hq:], 0, 0)
            for k in range(kv_heads):
                cs = slice(k * HD, (k + 1) * HD)
                keys_all[r, span, cs] = turn(acc_kv[r, span, cs], 1.0).astype(jnp.bfloat16)
            values_all[r, span, :] = (acc_kv[r, span, hk:] + added).astype(jnp.bfloat16)
        full = accs[2 + ci][r, span, :] + scale * dot(
            u[:R], b_all[slot, r, :, ci * hc : (ci + 1) * hc], 0, 0
        )
        live_rows = lax.broadcasted_iota(jnp.int32, (REQUEST_ROWS, HD), 0) < live
        allowed = (key_at <= query_at) & ((key_at < live) | (key_at == query_at))
        allowed = allowed.astype(jnp.float32)
        pieces = []
        for k in range(kv_heads):
            heads = [i for i in range(hc // HD) if (ci * (hc // HD) + i) // group == k]
            if not heads:
                continue
            kc = slice(k * HD, (k + 1) * HD)
            keys, values = keys_all[r, span, kc], values_all[r, span, kc]
            queries = jnp.concatenate(
                [turn(full[:, i * HD : (i + 1) * HD], 1.0).astype(jnp.bfloat16) for i in heads],
                axis=0,
            )
            dout = jnp.concatenate(
                [
                    jnp.where(
                        live_rows,
                        d_all[r, span, ci * hc + i * HD : ci * hc + (i + 1) * HD].astype(jnp.float32),
                        0.0,
                    ).astype(jnp.bfloat16)
                    for i in heads
                ],
                axis=0,
            )
            mask = jnp.concatenate([allowed] * len(heads), axis=0) > 0.5
            scores = dot(queries, keys, 1, 1) * HD ** (-0.5)
            scores = jnp.where(mask, scores, -1e30)
            expo = jnp.exp(scores - jnp.max(scores, axis=-1, keepdims=True))
            probs = expo / jnp.sum(expo, axis=-1, keepdims=True)
            dprobs = dot(dout, values, 1, 1)
            dscores = probs * (dprobs - jnp.sum(dprobs * probs, axis=-1, keepdims=True))
            dquery = dot(dscores.astype(jnp.bfloat16), keys, 1, 0) * HD ** (-0.5)
            for i in range(len(heads)):
                piece = dquery[i * REQUEST_ROWS : (i + 1) * REQUEST_ROWS]
                pieces.append(turn(piece, -1.0).astype(jnp.bfloat16))
            part_v = dot(probs.astype(jnp.bfloat16), dout, 0, 0)
            if heads[0] + ci * (hc // HD) == k * group:
                gv_acc[r, span, kc] = part_v
            else:
                gv_acc[r, span, kc] += part_v
        gq = jnp.concatenate(pieces, axis=1)
        slots = jnp.full((R, 128), slot, jnp.int32)[:, :1]

        def spread(total, value):
            for a in range(n) if n <= 8 else ():
                total[a] += jnp.where(slots == a, value, 0.0)
            if n > 8:

                @pl.loop(0, n)
                def _(a):
                    total[a] += jnp.where(slots == a, value, 0.0)

        spread(upq_sum.at[ci, r], scale * dot(u[:R], gq, 1, 0))
        back = scale * dot(b_all[slot, r, :, ci * hc : (ci + 1) * hc], gq, 1, 1)
        if ci == 0:
            back_acc[r, :R, span] = back
        else:
            back_acc[r, :R, span] += back
            gv = gv_acc[r, span, :].astype(jnp.bfloat16)
            spread(upv_sum.at[r], scale * dot(u[R:], gv, 1, 0))
            back_acc[r, R:, span] = scale * dot(b_all[slot, r, :, hq:], gv, 1, 1)

    def part_copy(j, arriving):
        peer = lax.rem(t + nt - j, nt) if arriving else lax.rem(t + j, nt)
        ref = parts.at[peer if arriving else t]
        return remote(ref, ref, part_send.at[j], part_recv.at[j], {"tensor": peer})

    def down_parts():
        wide = pl.ds(pl.multiple_of(t * width, 128), width)
        for b in range(blocks):
            span = slice(b * REQUEST_ROWS, (b + 1) * REQUEST_ROWS)
            parts[t, :, span] = dot(down_all[meta[gi, b]], x_all[gi, span, wide], 1, 1)
        for j in range(1, nt):
            part_copy(j, False).start()

    row_at = lax.broadcasted_iota(jnp.int32, (2 * R, REQUEST_ROWS), 0)
    row_at = jnp.where(row_at >= R, row_at - R, row_at)

    def yu_copy(j, arriving):
        peer = lax.rem(gi + G - j, G) if arriving else lax.rem(gi + j, G)
        ref = u_all.at[peer if arriving else gi]
        return remote(ref, ref, yu_send.at[j], yu_recv.at[j], {"groups": peer})

    def finish_down():
        for j in range(1, nt):
            part_copy(j, True).wait_recv()
        for b in range(blocks):
            span = slice(b * REQUEST_ROWS, (b + 1) * REQUEST_ROWS)
            total = parts[0, :, span]
            for j in range(1, nt):
                total = total + parts[j, :, span]
            kept = jnp.where(row_at < meta[gi, blocks + b], total, 0.0)
            u_all[gi, :, span] = kept.astype(jnp.bfloat16)
        for j in range(1, G):
            yu_copy(j, False).start()

    def up_copy(ci, e, a):
        there = lax.rem(gi + e, G)
        src = upv_send.at[there, a] if ci == 2 else upq_send.at[ci, there, a]
        dst = upv_got.at[me, gi] if ci == 2 else upq_got.at[ci, me, gi]
        return remote(
            src, dst, us_send.at[ci, e, a], us_recv.at[ci, me, gi], at_group(there, dp=a)
        )

    def up_arrival(ci, e, s):
        there = lax.rem(gi + e, G)
        dst = upv_got.at[s, there] if ci == 2 else upq_got.at[ci, s, there]
        return remote(dst, dst, us_send.at[ci, e, s], us_recv.at[ci, s, there], at_group(there, dp=s))

    def others(body):
        @pl.loop(0, n)
        def _(a):
            for e in range(G):
                if e == 0:

                    @pl.when(a != me)
                    def _():
                        body(e, a)

                else:
                    body(e, a)

    def send_ups(ci):
        if ci == 2:
            upv_send[...] = upv_sum[...].astype(jnp.bfloat16)
            upv_got[me, gi] = upv_send[gi, me]
        else:
            upq_send[ci] = upq_sum[ci].astype(jnp.bfloat16)
            upq_got[ci, me, gi] = upq_send[ci, gi, me]
        others(lambda e, a: up_copy(ci, e, a).start())

    own_w = (loads[0], loads[1])
    for copy in own_w:
        copy.wait()
    send_own(0)
    for j in range(1, G):
        for copy in y_copies(j, False)[:3]:
            copy.start()
    loads[8].wait()
    for j in range(1, G):
        for k in range(TOKEN_SUBS):
            yt_copy(j, k, False).start()
        y_copies(j, False)[3].start()
    for copy in loads[2:6]:
        copy.wait()
    send_own(FACTORS, (0,))
    for j in range(1, G):
        for copy in y_copies(j, True)[:3]:
            copy.wait_recv()
    send_own(FACTORS, (1,))
    upq_sum[...] = jnp.zeros_like(upq_sum)
    upv_sum[...] = jnp.zeros_like(upv_sum)
    for copy in loads[6:8] + loads[9:]:
        copy.wait()

    relays = [(1 + k, functools.partial(relay_tokens, k)) for k in range(TOKEN_SUBS)]
    line(0, hooks=relays)
    send_own(2)
    line(FACTORS, hooks=[(n - 1, down_parts)])
    pass_tokens()
    send_own(3)
    whole_product(0, gi)

    def tokens_done():
        settle_tokens()
        for j in range(1, G):
            whole_product(0, lax.rem(gi + j, G))

    line(2, hooks=[(1, finish_down), (2, tokens_done)])
    for e in range(G):
        whole_product(2, lax.rem(gi + e, G))
    for j in range(1, G):
        y_copies(j, True)[3].wait_recv()
        yu_copy(j, True).wait_recv()
    slice_product(3, me, True)
    total_blocks = G * blocks
    per = -(-total_blocks // (n - 1)) if n > 1 else total_blocks

    def last_step(d):
        for way in (0, 1):
            s = me - d if way == 0 else me + d

            @pl.when((s >= 0) if way == 0 else (s < n))
            def _():
                slice_product(3, s, False)

        @pl.loop(0, per)
        def _(i):
            index = (d - 1) * per + i

            @pl.when(index < total_blocks)
            def _():
                attend(index, 0)

    line(3, after=last_step)
    send_ups(0)

    @pl.loop(0, total_blocks)
    def _(index):
        attend(index, 1)

    for r in range(G):
        back_send[r] = back_acc[r].astype(jnp.bfloat16)

    def back_copy(e, j, arriving):
        there = lax.rem(gi + e, G)
        peer = lax.rem(t + nt - j, nt) if arriving else lax.rem(t + j, nt)
        if arriving:
            dst = back_got.at[there, peer]
            return remote(
                dst, dst, bk_send.at[e, j], bk_recv.at[there, peer], at_group(there, tensor=peer)
            )
        return remote(
            back_send.at[there],
            back_got.at[gi, t],
            bk_send.at[e, j],
            bk_recv.at[gi, t],
            at_group(there, tensor=peer),
        )

    crossing = [(e, j) for e in range(G) for j in range(nt) if (e, j) != (0, 0)]
    for e, j in crossing:
        back_copy(e, j, False).start()
    send_ups(1)
    send_ups(2)
    back_got[gi, t] = back_send[gi]
    for e, j in crossing:
        back_copy(e, j, True).wait_recv()
    total = jnp.zeros(back_acc.shape[1:], jnp.float32)
    for r in range(G):
        for j in range(nt):
            total = total + back_got[r, j].astype(jnp.float32)
    kept = []
    for b in range(blocks):
        span = slice(b * REQUEST_ROWS, (b + 1) * REQUEST_ROWS)
        kept.append(jnp.where(row_at < meta[gi, blocks + b], total[:, span], 0.0))
    wide = pl.ds(pl.multiple_of(t * width, 128), width)

    def low_copy(a):
        return remote(
            low_send.at[a], low_got.at[me], lo_send.at[a], lo_recv.at[me], {"dp": a}
        )

    stack = 4 if n % 4 == 0 else 1

    @pl.loop(0, n // stack)
    def _(q):
        chosen = jnp.concatenate(
            [
                jnp.concatenate(
                    [
                        jnp.where(
                            jnp.full((2 * R, REQUEST_ROWS), meta[gi, b], jnp.int32) == q * stack + i,
                            kept[b],
                            0.0,
                        )
                        for b in range(blocks)
                    ],
                    axis=1,
                )
                for i in range(stack)
            ],
            axis=0,
        ).astype(jnp.bfloat16)
        low = jnp.dot(chosen, x_all[gi, :, wide], preferred_element_type=jnp.float32)
        for i in range(stack):
            a = q * stack + i
            low_send[a] = low[i * 2 * R : (i + 1) * 2 * R].astype(jnp.bfloat16)

            @pl.when(a != me)
            def _():
                low_copy(a).start()

    low_got[me] = low_send[me]

    for ci in range(3):
        others(lambda e, s: up_arrival(ci, e, s).wait_recv())
    for e in range(G):
        for ci in range(2):
            out = jnp.zeros((R, hc), jnp.float32)
            out = lax.fori_loop(0, n, lambda s, v: v + upq_got[ci, s, e].astype(jnp.float32), out)
            upq_out[:, e * hq + ci * hc : e * hq + (ci + 1) * hc] = out
        out = jnp.zeros((R, hk), jnp.float32)
        out = lax.fori_loop(0, n, lambda s, v: v + upv_got[s, e].astype(jnp.float32), out)
        upv_out[:, e * hk : (e + 1) * hk] = out

    @pl.loop(0, n)
    def _(s):
        @pl.when(s != me)
        def _():
            remote(
                low_got.at[s], low_got.at[s], lo_send.at[s], lo_recv.at[s], {"dp": s}
            ).wait_recv()

    for i, out in enumerate((lowq_out, lowv_out)):
        out[...] = jnp.zeros_like(out)

        @pl.loop(0, n)
        def _(s):
            out[...] += low_got[s, i * R : (i + 1) * R, :].astype(jnp.float32)

    for item in range(4):

        @pl.loop(0, n)
        def _(s):
            for p in pieces_of(item):

                @pl.when((s <= me) & (me < n - 1))
                def _():
                    z_copy(item, s, p, 0).wait_send()

                @pl.when((s >= me) & (me > 0))
                def _():
                    z_copy(item, s, p, 1).wait_send()

    for j in range(1, G):
        for copy in y_copies(j, False):
            copy.wait_send()
        yu_copy(j, False).wait_send()
        for k in range(TOKEN_SUBS):
            yt_copy(j, k, False).wait_send()
            for i in range(1, pairs):
                tx_copy(j, i, k, False).wait_send()
            for i in range(pairs):
                tp_copy(j, lax.rem(t + 2 * i, nt), k).wait_send()
    for j in range(1, nt):
        part_copy(j, False).wait_send()
    for e, j in crossing:
        back_copy(e, j, False).wait_send()
    for ci in range(3):
        others(lambda e, a: up_copy(ci, e, a).wait_send())

    @pl.loop(0, n)
    def _(a):
        @pl.when(a != me)
        def _():
            low_copy(a).wait_send()


def layer(G, x, wq, wk, wv, aq, av, bq, bv, d, blocks_of, slots, ranks, live):
    n, nt = lax.axis_size("dp"), lax.axis_size("tensor")
    rows = x.shape[0]
    depth, qcols = wq.shape
    kcols = wk.shape[1]
    width = aq.shape[1]
    hq, hk = qcols // G, kcols // G
    hc = hq // 2
    span = n * depth
    blocks = rows // REQUEST_ROWS
    cosine, sine = rope_tables(REQUEST_ROWS, HD)
    cosine = np.concatenate([cosine, cosine], axis=-1)
    sine = np.concatenate([-sine, sine], axis=-1)
    smem = pl.BlockSpec(memory_space=pltpu.SMEM)
    vmem = pl.BlockSpec(memory_space=pltpu.VMEM)
    hbm = pl.BlockSpec(memory_space=pltpu.HBM)
    bf, f32 = jnp.bfloat16, jnp.float32
    V = pltpu.VMEM
    dma = pltpu.SemaphoreType.DMA
    return pl.pallas_call(
        functools.partial(layer_kernel, G),
        out_shape=(
            jax.ShapeDtypeStruct((R, width), f32),
            jax.ShapeDtypeStruct((R, width), f32),
            jax.ShapeDtypeStruct((R, qcols), f32),
            jax.ShapeDtypeStruct((R, kcols), f32),
        ),
        in_specs=[smem] * 4 + [hbm] * 9 + [vmem] * 2,
        out_specs=(vmem,) * 4,
        scratch_shapes=[
            V((G, rows, span), bf),
            V((span, 2 * hk), bf),
            V((span, hc), bf),
            V((span, hc), bf),
            V((n, 2 * R, width), bf),
            V((n, G, R, hq + hk), bf),
            V((G, rows, hq), bf),
            V((G, rows, 2 * hk), f32),
            V((G, rows, hc), f32),
            V((G, rows, hc), f32),
            V((nt, 2 * R, rows), f32),
            V((G, 2 * R, rows), bf),
            V((G, rows, hk), bf),
            V((G, rows, hk), bf),
            V((G, rows, hk), f32),
            V((G, 2 * R, rows), f32),
            V((2, G, n, R, hc), f32),
            V((G, n, R, hk), f32),
            V((2, G, n, R, hc), bf),
            V((G, n, R, hk), bf),
            V((2, n, G, R, hc), bf),
            V((n, G, R, hk), bf),
            V((G, 2 * R, rows), bf),
            V((G, nt, 2 * R, rows), bf),
            V((n, 2 * R, width), bf),
            V((n, 2 * R, width), bf),
            pltpu.SMEM((G, 128), jnp.int32),
            dma((10,)),
            dma((2, 4, n, SUBS)),
            dma((4, n, SUBS)),
            dma((G, 4)),
            dma((G, 4)),
            dma((G, TOKEN_SUBS)),
            dma((G, TOKEN_SUBS)),
            dma((G, max(1, nt // 2), TOKEN_SUBS)),
            dma((G, max(1, nt // 2), TOKEN_SUBS)),
            dma((G, nt, TOKEN_SUBS)),
            dma((G, nt, TOKEN_SUBS)),
            dma((nt,)),
            dma((nt,)),
            dma((G,)),
            dma((G,)),
            dma((3, G, n)),
            dma((3, n, G)),
            dma((G, nt)),
            dma((G, nt)),
            dma((n,)),
            dma((n,)),
        ],
        compiler_params=pltpu.CompilerParams(
            collective_id=0, has_side_effects=True, vmem_limit_bytes=62 * 1024 * 1024
        ),
        name="layer",
    )(blocks_of, slots, ranks, live, x, wq, wk, wv, aq, av, bq, bv, d, cosine, sine)


def on_device(
    tokens,
    w_query,
    w_key,
    w_value,
    a_query,
    b_query,
    a_value,
    b_value,
    adapter_ranks,
    adapter_slot,
    block_adapter,
    live_tokens,
    d_heads,
):
    ng, nt = lax.axis_size("groups"), lax.axis_size("tensor")
    kv_heads = w_key.shape[1] // HD
    G = ng if nt % 2 == 0 and kv_heads % ng == 0 else 1
    low_q, low_v, up_q, up_v = layer(
        G, tokens, w_query, w_key, w_value, a_query[0].T, a_value[0].T, b_query[0], b_value[0],
        d_heads, block_adapter.reshape(-1), adapter_slot, adapter_ranks, live_tokens,
    )
    return low_q.T[None], up_q[None], low_v.T[None], up_v[None]


def solution(mesh):
    in_specs = (
        P(("groups", "dp"), None),
        P("dp", "tensor"),
        P("dp", "tensor"),
        P("dp", "tensor"),
        P(("groups", "dp"), "tensor", None),
        P(("groups", "dp"), None, "tensor"),
        P(("groups", "dp"), "tensor", None),
        P(("groups", "dp"), None, "tensor"),
        P("groups"),
        P(),
        P(("groups", "dp"), None),
        P(("groups", "dp")),
        P(("groups", "dp"), "tensor"),
    )
    out_specs = (
        P(("groups", "dp"), "tensor", None),
        P(("groups", "dp"), None, "tensor"),
        P(("groups", "dp"), "tensor", None),
        P(("groups", "dp"), None, "tensor"),
    )
    return jax.shard_map(
        on_device, mesh=mesh, in_specs=in_specs, out_specs=out_specs, check_vma=False
    )
```

```python
import functools

import jax
import jax.numpy as jnp
import numpy as np
from jax import lax
from jax.experimental import pallas as pl
from jax.experimental.pallas import tpu as pltpu
from jax.sharding import PartitionSpec as P

HD = 128
R = 32
REQUEST_ROWS = 128
MESH = pl.DeviceIdType.MESH

adapter_alpha_factor = 32.0
rope_theta = 500000.0

SUBS = 4
TOKEN_SUBS = 2
FACTORS = 1


def rope_tables(length, width):
    halfway = width // 2
    spread = rope_theta ** (-2.0 * np.arange(halfway, dtype=np.float32) / width)
    angle = np.arange(length, dtype=np.float32)[:, None] * spread.astype(np.float32)[None, :]
    return np.cos(angle).astype(np.float32), np.sin(angle).astype(np.float32)


def scale_of(rank):
    return (adapter_alpha_factor / jnp.full((1, 128), rank, jnp.int32).astype(jnp.float32))[:, :1]


def dot(a, c, left, right):
    return lax.dot_general(
        a, c, (((left,), (right,)), ((), ())), preferred_element_type=jnp.float32
    )


def layer_kernel(
    G,
    relief,
    block_ref,
    slot_ref,
    rank_ref,
    live_ref,
    x_hbm,
    wq_hbm,
    wk_hbm,
    wv_hbm,
    aq_hbm,
    av_hbm,
    bq_hbm,
    bv_hbm,
    d_hbm,
    cos_ref,
    sin_ref,
    lowq_out,
    lowv_out,
    upq_out,
    upv_out,
    x_all,
    w_kv,
    w_a,
    w_b,
    down_all,
    b_all,
    d_all,
    acc_kv,
    acc_a,
    acc_b,
    parts,
    u_all,
    keys_all,
    values_all,
    gv_acc,
    back_acc,
    upq_sum,
    upv_sum,
    upq_send,
    upv_send,
    upq_got,
    upv_got,
    back_send,
    back_got,
    low_send,
    low_got,
    meta,
    x_far,
    x_down,
    parts_extra,
    p_b_send,
    p_a_send,
    p_b_got,
    p_a_got,
    local_sem,
    z_send,
    z_recv,
    yb_send,
    yb_recv,
    yt_send,
    yt_recv,
    tx_send,
    tx_recv,
    tp_send,
    tp_recv,
    part_send,
    part_recv,
    yu_send,
    yu_recv,
    us_send,
    us_recv,
    bk_send,
    bk_recv,
    lo_send,
    lo_recv,
    em_send,
    em_recv,
    et_send,
    et_recv,
    ey_send,
    ey_recv,
    eu_send,
    eu_recv,
    px_send,
    px_recv,
    ue_send,
    ue_recv,
    pp_send,
    pp_recv,
):
    n = lax.axis_size("dp")
    ng = lax.axis_size("groups")
    nt = lax.axis_size("tensor")
    me = lax.axis_index("dp")
    g = lax.axis_index("groups")
    t = lax.axis_index("tensor")
    split = G > 1
    low_end, high_end = (1, n - 2) if relief else (0, n - 1)
    end = (me < low_end) | (me > high_end)
    near = ((me == 1) | (me == n - 2)) if relief else None
    inward = jnp.where(me == 0, 1, n - 2) if relief else None
    outward = jnp.where(me == 1, 0, n - 1) if relief else None
    gi = g if split else 0
    rows = x_hbm.shape[0]
    depth, qcols = wq_hbm.shape
    kcols = wk_hbm.shape[1]
    hq, hk = qcols // G, kcols // G
    hc = hq // 2
    kv_heads = hk // HD
    group = hq // hk
    blocks = rows // REQUEST_ROWS
    width = down_all.shape[2]
    step = depth // SUBS
    weights = (w_kv, None, w_a, w_b)
    wide = pl.ds(pl.multiple_of(t * width, 128), width)
    accs = (acc_kv, None, acc_a, acc_b)
    sums_out, sums_in = {2: p_a_send, 3: p_b_send}, {2: p_a_got, 3: p_b_got}
    far = x_far.shape[2]
    far_of_near = jnp.where(me == 1, 2 * depth, 0)
    far_of_end = jnp.where(me == 0, 2 * depth, 0)
    close_of_end = jnp.where(me == 0, 0, far)

    def at_group(index, **rest):
        if split:
            rest["groups"] = index
        return rest

    def remote(src, dst, send, recv, to):
        return pltpu.make_async_remote_copy(
            src_ref=src, dst_ref=dst, send_sem=send, recv_sem=recv, device_id=to, device_id_type=MESH
        )

    mine = pl.ds(pl.multiple_of(me * depth, depth), depth)
    qs = pl.ds(pl.multiple_of(gi * hq, 128), hq)
    ks = pl.ds(pl.multiple_of(gi * hk, 128), hk)
    loads = [
        (wk_hbm.at[:, ks], w_kv.at[mine, pl.ds(0, hk)]),
        (wv_hbm.at[:, ks], w_kv.at[mine, pl.ds(hk, hk)]),
        (aq_hbm, down_all.at[me, pl.ds(0, R), :]),
        (av_hbm, down_all.at[me, pl.ds(R, R), :]),
        (bq_hbm.at[:, qs], b_all.at[me, gi, :, pl.ds(0, hq)]),
        (bv_hbm.at[:, ks], b_all.at[me, gi, :, pl.ds(hq, hk)]),
        (wq_hbm.at[:, pl.ds(pl.multiple_of(gi * hq, 128), hc)], w_a.at[mine, :]),
        (wq_hbm.at[:, pl.ds(pl.multiple_of(gi * hq + hc, 128), hc)], w_b.at[mine, :]),
        (x_hbm, x_all.at[gi]),
        (d_hbm.at[:, qs], d_all.at[gi]),
    ]
    loads = [pltpu.make_async_copy(s, d, local_sem.at[i]) for i, (s, d) in enumerate(loads)]
    for copy in loads:
        copy.start()

    for b in range(blocks):
        adapter = block_ref[b]
        meta[gi, b] = slot_ref[adapter]
        meta[gi, blocks + b] = rank_ref[adapter]
    meta[gi, 2 * blocks] = live_ref[0]

    with jax.named_scope("greet"):
        barrier = pltpu.get_barrier_semaphore()

        @pl.loop(1, n * G)
        def _(j):
            k = lax.rem(me * G + gi + j, n * G)
            pl.semaphore_signal(
                barrier, inc=1, device_id=at_group(lax.rem(k, G), dp=lax.div(k, G)), device_id_type=MESH
            )

        for j in range(1, nt):
            for e in range(G):
                pl.semaphore_signal(
                    barrier,
                    inc=1,
                    device_id=at_group(lax.rem(gi + e, G), tensor=lax.rem(t + j, nt)),
                    device_id_type=MESH,
                )
        pl.semaphore_wait(barrier, n * G - 1 + G * (nt - 1))

    def z_copy(item, s, p, way):
        if item == FACTORS:
            ref = down_all.at[s] if p == 0 else b_all.at[s]
        else:
            ref = weights[item].at[pl.ds(pl.multiple_of(s * depth + p * step, step), step), :]
        target = jnp.clip(me + (1 if way == 0 else -1), 0, n - 1)
        return remote(
            ref, ref, z_send.at[way, item, s, p], z_recv.at[item, s, p], {"dp": target}
        )

    def pieces_of(item):
        return range(2) if item == FACTORS else range(SUBS)

    def stays_inside(item, p, own):
        if item == FACTORS:
            return p == 0
        return item > FACTORS and not own

    def ups(item, p, own):
        return me < (high_end if stays_inside(item, p, own) else n - 1)

    def downs(item, p, own):
        return me > (low_end if stays_inside(item, p, own) else 0)

    def send_own(item, pieces=None, to_end=None):
        up, down = (me < n, me >= 0) if to_end is None else (me == n - 2, me == 1)
        if to_end is False:
            up, down = ~up, ~down
        for p in pieces_of(item) if pieces is None else pieces:

            @pl.when(ups(item, p, True) & up)
            def _():
                z_copy(item, me, p, 0).start()

            @pl.when(downs(item, p, True) & down)
            def _():
                z_copy(item, me, p, 1).start()

    def forward_piece(item, d, p, static_p):
        for way in (0, 1):
            s = me - d if way == 0 else me + d
            valid = (s >= 0) if way == 0 else (s < n)
            if relief and stays_inside(item, static_p, False):
                valid = valid & (~end if item == FACTORS else ~end | (d == 1))
            onward = ups(item, static_p, False) if way == 0 else downs(item, static_p, False)

            @pl.when(valid)
            def _():
                z_copy(item, s, p, way).wait_recv()

                @pl.when(onward)
                def _():
                    z_copy(item, s, p, way).start()

    def line(item, hooks=()):
        hooks = dict(hooks)
        last = pieces_of(item)[-1]
        if n <= 8:
            for d in range(1, n):
                for p in pieces_of(item):
                    forward_piece(item, d, p, p)
                    for key in ((d, p), (d, None) if p == last else None):
                        if key in hooks:
                            hooks.pop(key)()
        else:

            @pl.loop(1, n)
            def _(d):
                for p in pieces_of(item):
                    forward_piece(item, d, p, p)

        for hook in hooks.values():
            hook()

    def y_copies(j, arriving):
        peer = lax.rem(gi + G - j, G) if arriving else lax.rem(gi + j, G)
        at = peer if arriving else gi
        to = {"groups": peer}
        pq = pl.ds(pl.multiple_of(peer * hq, 128), hq)
        pk = pl.ds(pl.multiple_of(peer * hk, 128), hk)
        sources = (
            (bq_hbm.at[:, pq], b_all.at[me, at, :, pl.ds(0, hq)]),
            (bv_hbm.at[:, pk], b_all.at[me, at, :, pl.ds(hq, hk)]),
            (meta.at[at], meta.at[at]),
            (d_hbm.at[:, pq], d_all.at[at]),
        )
        return [
            remote(s, d, yb_send.at[j, i], yb_recv.at[j, i], to) for i, (s, d) in enumerate(sources)
        ]

    quarter = rows // nt
    sub = quarter // TOKEN_SUBS

    def token_piece(r, q, k, bank=0):
        ref = x_far if bank else x_all
        return ref.at[r, pl.ds(pl.multiple_of(q * quarter + k * sub, sub), sub), :]

    def yt_copy(j, k, arriving):
        peer = lax.rem(gi + G - j, G) if arriving else lax.rem(gi + j, G)
        ref = token_piece(peer if arriving else gi, t, k)
        return remote(ref, ref, yt_send.at[j, k], yt_recv.at[j, k], {"groups": peer})

    pairs = nt // 2
    partner = t + 1 - 2 * lax.rem(t, 2)

    def tx_copy(r, i, k, arriving, bank=0):
        peer = lax.rem(t + nt - 2 * i, nt) if arriving else lax.rem(t + 2 * i, nt)
        ref = token_piece(r, peer if arriving else t, k, bank)
        return remote(
            ref, ref, tx_send.at[bank * G + r, i, k], tx_recv.at[bank * G + r, i, k], {"tensor": peer}
        )

    def tp_copy(r, q, k, bank=0):
        ref = token_piece(r, q, k, bank)
        return remote(
            ref, ref, tp_send.at[bank * G + r, q, k], tp_recv.at[bank * G + r, q, k], {"tensor": partner}
        )

    def spread_tokens(r, k, bank=0):
        for i in range(1, pairs):
            tx_copy(r, i, k, False, bank).start()
        tp_copy(r, t, k, bank).start()

    def pass_tokens(r, bank=0):
        for k in range(TOKEN_SUBS):
            for i in range(1, pairs):
                tx_copy(r, i, k, True, bank).wait_recv()
                tp_copy(r, lax.rem(t + nt - 2 * i, nt), k, bank).start()

    def settle_tokens(r, bank=0):
        for k in range(TOKEN_SUBS):
            for i in range(pairs):
                tp_copy(r, lax.rem(partner + 2 * i, nt), k, bank).wait_recv()

    def drain_tokens(r, bank=0):
        for k in range(TOKEN_SUBS):
            for i in range(1, pairs):
                tx_copy(r, i, k, False, bank).wait_send()
            for i in range(pairs):
                tp_copy(r, lax.rem(t + 2 * i, nt), k, bank).wait_send()

    def relay_tokens(k):
        for j in range(1, G):
            yt_copy(j, k, True).wait_recv()
            spread_tokens(lax.rem(gi + G - j, G), k)

    def end_meta():
        return remote(meta.at[gi], meta.at[G], em_send, em_recv, {"dp": inward})

    def end_tokens(k):
        at = pl.ds(pl.multiple_of(t * quarter + k * sub, sub), sub)
        cols = pl.ds(pl.multiple_of(far_of_end, 128), far)
        return remote(
            x_all.at[gi, at, cols], token_piece(gi, t, k, 1), et_send.at[k], et_recv.at[k], {"dp": inward}
        )

    def end_down():
        return remote(x_all.at[gi, :, wide], x_down, eu_send, eu_recv, {"dp": inward})

    def ey_copy(j, k, arriving):
        peer = lax.rem(gi + G - j, G) if arriving else lax.rem(gi + j, G)
        ref = token_piece(peer if arriving else gi, t, k, 1)
        return remote(ref, ref, ey_send.at[j, k], ey_recv.at[j, k], {"groups": peer})

    def px_copy(j, arriving):
        peer = lax.rem(t + nt - j, nt) if arriving else lax.rem(t + j, nt)
        ref = parts_extra.at[peer if arriving else t]
        return remote(ref, ref, px_send.at[j], px_recv.at[j], {"tensor": peer})

    def ue_copy():
        return remote(u_all.at[G], u_all.at[gi], ue_send, ue_recv, {"dp": outward})

    def pp_copy(item, r):
        i = item - 2
        return remote(
            sums_out[item].at[r], sums_in[item].at[r], pp_send.at[i, r], pp_recv.at[i, r], {"dp": outward}
        )

    tile = 256 if rows % 256 == 0 else 128

    def whole_product(item, r):
        @pl.loop(0, rows // tile)
        def _(i):
            span = pl.ds(pl.multiple_of(i * tile, tile), tile)
            accs[item][r, span, :] = jnp.dot(
                x_all[r, span, :], weights[item][...], preferred_element_type=jnp.float32
            )

    def far_sums(item, r):
        rows_far = pl.ds(pl.multiple_of(far_of_near, 128), far)

        @pl.loop(0, rows // tile)
        def _(i):
            span = pl.ds(pl.multiple_of(i * tile, tile), tile)
            sums_out[item][r, span, :] = jnp.dot(
                x_far[r, span, :], weights[item][rows_far, :], preferred_element_type=jnp.float32
            ).astype(jnp.bfloat16)

        pp_copy(item, r).start()

    def close_product(item, r):
        close = pl.ds(pl.multiple_of(close_of_end, 128), 2 * depth)
        remote(
            sums_in[item].at[r], sums_in[item].at[r], pp_send.at[item - 2, r], pp_recv.at[item - 2, r],
            {"dp": inward},
        ).wait_recv()

        @pl.loop(0, rows // tile)
        def _(i):
            span = pl.ds(pl.multiple_of(i * tile, tile), tile)
            accs[item][r, span, :] = jnp.dot(
                x_all[r, span, close], weights[item][close, :], preferred_element_type=jnp.float32
            ) + sums_in[item][r, span, :].astype(jnp.float32)

    def slice_product(item, s, first):
        k_span = pl.ds(pl.multiple_of(s * depth, 128), depth)

        @pl.loop(0, G * rows // tile)
        def _(i):
            r = lax.div(i, rows // tile)
            span = pl.ds(pl.multiple_of(lax.rem(i, rows // tile) * tile, tile), tile)
            new = jnp.dot(
                x_all[r, span, k_span],
                weights[item][k_span, :],
                preferred_element_type=jnp.float32,
            )
            if first:
                accs[item][r, span, :] = new
            else:
                accs[item][r, span, :] += new

    cosine, sine = cos_ref[...], sin_ref[...]
    dims = (REQUEST_ROWS, REQUEST_ROWS)
    query_at = lax.broadcasted_iota(jnp.int32, dims, 0)
    key_at = lax.broadcasted_iota(jnp.int32, dims, 1)

    def turn(item, sign):
        return item * cosine + pltpu.roll(item, HD // 2, 1) * (sign * sine)

    def place(index):
        r, b = lax.div(index, blocks), lax.rem(index, blocks)
        span = pl.ds(pl.multiple_of(b * REQUEST_ROWS, REQUEST_ROWS), REQUEST_ROWS)
        return r, b, span

    def spread(total, slot, value):
        slots = jnp.full((R, 128), slot, jnp.int32)[:, :1]

        def add(a):
            total[a] += jnp.where(slots == a, value, 0.0)

        if n <= 8:
            for a in range(n):
                add(a)
        else:
            pl.loop(0, n)(add)

    def prepare(index):
        r, b, span = place(index)
        scale = scale_of(meta[r, blocks + b])
        added = scale * dot(u_all[r, R:, span], b_all[meta[r, b], r, :, hq:], 0, 0)
        for k in range(kv_heads):
            cs = slice(k * HD, (k + 1) * HD)
            keys_all[r, span, cs] = turn(acc_kv[r, span, cs], 1.0).astype(jnp.bfloat16)
        values_all[r, span, :] = (acc_kv[r, span, hk:] + added).astype(jnp.bfloat16)
        gv_acc[r, span, :] = jnp.zeros((REQUEST_ROWS, hk), jnp.float32)
        back_acc[r, :, span] = jnp.zeros((2 * R, REQUEST_ROWS), jnp.float32)

    def finish_values(index):
        r, b, span = place(index)
        slot = meta[r, b]
        scale = scale_of(meta[r, blocks + b])
        gv = gv_acc[r, span, :].astype(jnp.bfloat16)
        spread(upv_sum.at[r], slot, scale * dot(u_all[r, R:, span], gv, 1, 0))
        back_acc[r, R:, span] = scale * dot(b_all[slot, r, :, hq:], gv, 1, 1)

    def attend(index, ci):
        r, b, span = place(index)
        slot = meta[r, b]
        scale = scale_of(meta[r, blocks + b])
        live = meta[r, 2 * blocks] - b * REQUEST_ROWS
        u = u_all[r, :R, span]
        b_cols = b_all[slot, r, :, ci * hc : (ci + 1) * hc]
        full = accs[2 + ci][r, span, :] + scale * dot(u, b_cols, 0, 0)
        live_rows = lax.broadcasted_iota(jnp.int32, (REQUEST_ROWS, HD), 0) < live
        allowed = (key_at <= query_at) & ((key_at < live) | (key_at == query_at))
        allowed = allowed.astype(jnp.float32)
        pieces = []
        for k in range(kv_heads):
            heads = [i for i in range(hc // HD) if (ci * (hc // HD) + i) // group == k]
            if not heads:
                continue
            kc = slice(k * HD, (k + 1) * HD)
            keys, values = keys_all[r, span, kc], values_all[r, span, kc]
            queries = jnp.concatenate(
                [turn(full[:, i * HD : (i + 1) * HD], 1.0).astype(jnp.bfloat16) for i in heads],
                axis=0,
            )
            douts = []
            for i in heads:
                rows_in = d_all[r, span, ci * hc + i * HD : ci * hc + (i + 1) * HD]
                kept = jnp.where(live_rows, rows_in.astype(jnp.float32), 0.0)
                douts.append(kept.astype(jnp.bfloat16))
            dout = jnp.concatenate(douts, axis=0)
            mask = jnp.concatenate([allowed] * len(heads), axis=0) > 0.5
            scores = dot(queries, keys, 1, 1) * HD ** (-0.5)
            scores = jnp.where(mask, scores, -1e30)
            expo = jnp.exp(scores - jnp.max(scores, axis=-1, keepdims=True))
            probs = expo / jnp.sum(expo, axis=-1, keepdims=True)
            dprobs = dot(dout, values, 1, 1)
            dscores = probs * (dprobs - jnp.sum(dprobs * probs, axis=-1, keepdims=True))
            dquery = dot(dscores.astype(jnp.bfloat16), keys, 1, 0) * HD ** (-0.5)
            for i in range(len(heads)):
                piece = dquery[i * REQUEST_ROWS : (i + 1) * REQUEST_ROWS]
                pieces.append(turn(piece, -1.0).astype(jnp.bfloat16))
            gv_acc[r, span, kc] += dot(probs.astype(jnp.bfloat16), dout, 0, 0)
        gq = jnp.concatenate(pieces, axis=1)
        spread(upq_sum.at[ci, r], slot, scale * dot(u, gq, 1, 0))
        back_acc[r, :R, span] += scale * dot(b_cols, gq, 1, 1)

    def part_copy(j, arriving):
        peer = lax.rem(t + nt - j, nt) if arriving else lax.rem(t + j, nt)
        ref = parts.at[peer if arriving else t]
        return remote(ref, ref, part_send.at[j], part_recv.at[j], {"tensor": peer})

    def down_product(r, x_ref, into):
        for b in range(blocks):
            span = slice(b * REQUEST_ROWS, (b + 1) * REQUEST_ROWS)
            into[t, :, span] = dot(down_all[meta[r, b]], x_ref[span, :], 1, 1)

    def down_sum(r, terms):
        for b in range(blocks):
            span = slice(b * REQUEST_ROWS, (b + 1) * REQUEST_ROWS)
            total = terms[0, :, span]
            for j in range(1, nt):
                total = total + terms[j, :, span]
            kept = jnp.where(row_at < meta[r, blocks + b], total, 0.0)
            u_all[r, :, span] = kept.astype(jnp.bfloat16)

    def down_parts():
        @pl.when(~end)
        def _():
            down_product(gi, x_all.at[gi, :, wide], parts)
            for j in range(1, nt):
                part_copy(j, False).start()

    row_at = lax.broadcasted_iota(jnp.int32, (2 * R, REQUEST_ROWS), 0)
    row_at = jnp.where(row_at >= R, row_at - R, row_at)

    def yu_copy(j, arriving):
        peer = lax.rem(gi + G - j, G) if arriving else lax.rem(gi + j, G)
        ref = u_all.at[peer if arriving else gi]
        return remote(ref, ref, yu_send.at[j], yu_recv.at[j], {"groups": peer})

    def finish_down():
        @pl.when(~end)
        def _():
            for j in range(1, nt):
                part_copy(j, True).wait_recv()
            down_sum(gi, parts)

        if relief:

            @pl.when(end)
            def _():
                ue_copy().wait_recv()

        for j in range(1, G):
            yu_copy(j, False).start()

    def up_copy(ci, e, a):
        there = lax.rem(gi + e, G)
        src = upv_send.at[there, a] if ci == 2 else upq_send.at[ci, there, a]
        dst = upv_got.at[me, gi] if ci == 2 else upq_got.at[ci, me, gi]
        return remote(
            src, dst, us_send.at[ci, e, a], us_recv.at[ci, me, gi], at_group(there, dp=a)
        )

    def up_arrival(ci, e, s):
        there = lax.rem(gi + e, G)
        dst = upv_got.at[s, there] if ci == 2 else upq_got.at[ci, s, there]
        return remote(dst, dst, us_send.at[ci, e, s], us_recv.at[ci, s, there], at_group(there, dp=s))

    def others(body):
        @pl.loop(0, n)
        def _(a):
            for e in range(G):
                if e == 0:

                    @pl.when(a != me)
                    def _():
                        body(e, a)

                else:
                    body(e, a)

    def send_ups(ci):
        if ci == 2:
            upv_send[...] = upv_sum[...].astype(jnp.bfloat16)
            upv_got[me, gi] = upv_send[gi, me]
        else:
            upq_send[ci] = upq_sum[ci].astype(jnp.bfloat16)
            upq_got[ci, me, gi] = upq_send[ci, gi, me]
        others(lambda e, a: up_copy(ci, e, a).start())

    with jax.named_scope("start"):
        own_w = (loads[0], loads[1])
        for copy in own_w:
            copy.wait()
        send_own(0)
        for j in range(1, G):
            for copy in y_copies(j, False)[:3]:
                copy.start()
        if relief:

            @pl.when(end)
            def _():
                end_meta().start()

        loads[8].wait()
        for j in range(1, G):
            for k in range(TOKEN_SUBS):
                yt_copy(j, k, False).start()
            y_copies(j, False)[3].start()
        for copy in loads[2:6]:
            copy.wait()
        send_own(FACTORS, (0,))
        for j in range(1, G):
            for copy in y_copies(j, True)[:3]:
                copy.wait_recv()
        send_own(FACTORS, (1,))
        for copy in loads[6:8]:
            copy.wait()
        if relief:

            @pl.when(end)
            def _():
                for k in range(TOKEN_SUBS):
                    end_tokens(k).start()

        if relief:

            @pl.when(end)
            def _():
                send_own(2)
                end_down().start()
                send_own(3)

        upq_sum[...] = jnp.zeros_like(upq_sum)
        upv_sum[...] = jnp.zeros_like(upv_sum)
        loads[9].wait()
    other_planes = [lax.rem(gi + j, G) for j in range(1, G)]
    with jax.named_scope("line0"):
        keys_of = [(1, None), (2, 1)]
        line(0, hooks=[(keys_of[k], functools.partial(relay_tokens, k)) for k in range(TOKEN_SUBS)])

        @pl.when(~end)
        def _():
            send_own(2)

    if relief:
        with jax.named_scope("relay_extra"):

            @pl.when(near)
            def _():
                remote(meta.at[G], meta.at[G], em_send, em_recv, {"dp": outward}).wait_recv()
                for k in range(TOKEN_SUBS):
                    et = token_piece(gi, t, k, 1)
                    remote(et, et, et_send.at[k], et_recv.at[k], {"dp": outward}).wait_recv()
                    for j in range(1, G):
                        ey_copy(j, k, False).start()
                    spread_tokens(gi, k, 1)

    with jax.named_scope("pass"):
        for r in other_planes:
            pass_tokens(r)
    with jax.named_scope("linef"):
        line(FACTORS, hooks=[((n - 1, None), down_parts)])
        if relief:

            @pl.when(near)
            def _():
                send_own(3, to_end=True)


    def extra_pass():
        if relief:

            @pl.when(near)
            def _():
                pass_tokens(gi, 1)
                for j in range(1, G):
                    for k in range(TOKEN_SUBS):
                        ey_copy(j, k, True).wait_recv()
                        spread_tokens(lax.rem(gi + G - j, G), k, 1)

        whole_product(0, gi)

    def tokens_done():
        for r in other_planes:
            settle_tokens(r)
            whole_product(0, r)

        @pl.when(~end)
        def _():
            finish_down()

    with jax.named_scope("line2"):
        line(2, hooks=[((1, None), extra_pass), ((2, None), tokens_done)])

        @pl.when(~end)
        def _():
            send_own(3, to_end=False if relief else None)

    if relief:
        with jax.named_scope("far_sums"):

            @pl.when(near)
            def _():
                settle_tokens(gi, 1)
                far_sums(2, gi)

    with jax.named_scope("whole2"):

        @pl.when(~end)
        def _():
            for e in range(G):
                whole_product(2, lax.rem(gi + e, G))
            for j in range(1, G):
                yu_copy(j, True).wait_recv()

            slice_product(3, me, True)

        for j in range(1, G):
            y_copies(j, True)[3].wait_recv()
    total_blocks = G * blocks
    steps = (n - 1) * SUBS
    per = -(-total_blocks // SUBS)
    per_end = -(-total_blocks // (2 * SUBS))

    def first_unit(k):
        index = lax.rem(gi + lax.div(k, blocks), G) * blocks + lax.rem(k, blocks)
        prepare(index)
        attend(index, 0)

    def near_step(i):
        @pl.when(i == 0)
        def _():
            remote(x_down, x_down, eu_send, eu_recv, {"dp": outward}).wait_recv()
            down_product(G, x_down, parts_extra)
            for j in range(1, nt):
                px_copy(j, False).start()
            for r in other_planes:
                pass_tokens(r, 1)

        @pl.when(i == 1)
        def _():
            for j in range(1, nt):
                px_copy(j, True).wait_recv()
            down_sum(G, parts_extra)
            ue_copy().start()

        @pl.when(i == 2)
        def _():
            for r in other_planes:
                settle_tokens(r, 1)
                far_sums(2, r)

    def end_step(i):
        @pl.when(i == SUBS)
        def _():
            finish_down()
            close_product(2, gi)

        @pl.when(i == 2 * SUBS)
        def _():
            for r in other_planes:
                close_product(2, r)
            for j in range(1, G):
                yu_copy(j, True).wait_recv()

    with jax.named_scope("line3"):

        @pl.loop(0, steps)
        def _(i):
            d, p = lax.div(i, SUBS) + 1, lax.rem(i, SUBS)
            forward_piece(3, d, p, 0)

            @pl.when(p == SUBS - 1)
            def _():
                for way in (0, 1):
                    s = me - d if way == 0 else me + d

                    @pl.when(((s >= 0) if way == 0 else (s < n)) & ~end)
                    def _():
                        slice_product(3, s, False)

            if relief:
                pl.when(near)(lambda: near_step(i))
                pl.when(end)(lambda: end_step(i))
                start = jnp.where(end, (i - SUBS) * per_end, i * per)
                count = jnp.where(end, per_end, per)
            else:
                start, count = i * per, per

            @pl.loop(0, max(per, per_end))
            def _(j):
                @pl.when((j < count) & (start + j >= 0) & (start + j < total_blocks))
                def _():
                    first_unit(start + j)

        if not steps:
            pl.loop(0, total_blocks)(first_unit)
    with jax.named_scope("tail_attend"):
        if relief:

            @pl.when(near)
            def _():
                for e in range(G):
                    far_sums(3, lax.rem(gi + e, G))

        send_ups(0)

        @pl.loop(0, G)
        def _(e):
            r = lax.rem(gi + e, G)
            if relief:

                @pl.when(end)
                def _():
                    close_product(3, r)

            @pl.loop(0, blocks)
            def _(b):
                attend(r * blocks + b, 1)
                finish_values(r * blocks + b)

    with jax.named_scope("back"):
        for r in range(G):
            back_send[r] = back_acc[r].astype(jnp.bfloat16)

    def back_copy(e, j, arriving):
        there = lax.rem(gi + e, G)
        peer = lax.rem(t + nt - j, nt) if arriving else lax.rem(t + j, nt)
        if arriving:
            dst = back_got.at[there, peer]
            return remote(
                dst, dst, bk_send.at[e, j], bk_recv.at[there, peer], at_group(there, tensor=peer)
            )
        return remote(
            back_send.at[there],
            back_got.at[gi, t],
            bk_send.at[e, j],
            bk_recv.at[gi, t],
            at_group(there, tensor=peer),
        )

    crossing = [(e, j) for e in range(G) for j in range(nt) if (e, j) != (0, 0)]
    with jax.named_scope("backx"):
        for e, j in crossing:
            back_copy(e, j, False).start()
        send_ups(1)
        send_ups(2)
        back_got[gi, t] = back_send[gi]
        for e, j in crossing:
            back_copy(e, j, True).wait_recv()
    total = jnp.zeros(back_acc.shape[1:], jnp.float32)
    for r in range(G):
        for j in range(nt):
            total = total + back_got[r, j].astype(jnp.float32)
    kept = []
    for b in range(blocks):
        span = slice(b * REQUEST_ROWS, (b + 1) * REQUEST_ROWS)
        kept.append(jnp.where(row_at < meta[gi, blocks + b], total[:, span], 0.0))
    def low_copy(a):
        return remote(
            low_send.at[a], low_got.at[me], lo_send.at[a], lo_recv.at[me], {"dp": a}
        )

    stack = 4 if n % 4 == 0 else 1

    with jax.named_scope("low"):
        @pl.loop(0, n // stack)
        def _(q):
            chosen = jnp.concatenate(
                [
                    jnp.concatenate(
                        [
                            jnp.where(
                                jnp.full((2 * R, REQUEST_ROWS), meta[gi, b], jnp.int32) == q * stack + i,
                                kept[b],
                                0.0,
                            )
                            for b in range(blocks)
                        ],
                        axis=1,
                    )
                    for i in range(stack)
                ],
                axis=0,
            ).astype(jnp.bfloat16)
            low = jnp.dot(chosen, x_all[gi, :, wide], preferred_element_type=jnp.float32)
            for i in range(stack):
                a = q * stack + i
                low_send[a] = low[i * 2 * R : (i + 1) * 2 * R].astype(jnp.bfloat16)

                @pl.when(a != me)
                def _():
                    low_copy(a).start()

        low_got[me] = low_send[me]

    with jax.named_scope("upsum"):
        for ci in range(3):
            others(lambda e, s: up_arrival(ci, e, s).wait_recv())
        for e in range(G):
            for ci in range(2):
                out = jnp.zeros((R, hc), jnp.float32)
                out = lax.fori_loop(0, n, lambda s, v: v + upq_got[ci, s, e].astype(jnp.float32), out)
                upq_out[:, e * hq + ci * hc : e * hq + (ci + 1) * hc] = out
            out = jnp.zeros((R, hk), jnp.float32)
            out = lax.fori_loop(0, n, lambda s, v: v + upv_got[s, e].astype(jnp.float32), out)
            upv_out[:, e * hk : (e + 1) * hk] = out

    with jax.named_scope("lowx"):
        @pl.loop(0, n)
        def _(s):
            @pl.when(s != me)
            def _():
                remote(
                    low_got.at[s], low_got.at[s], lo_send.at[s], lo_recv.at[s], {"dp": s}
                ).wait_recv()

        for i, out in enumerate((lowq_out, lowv_out)):
            out[...] = jnp.zeros_like(out)

            @pl.loop(0, n)
            def _(s):
                out[...] += low_got[s, i * R : (i + 1) * R, :].astype(jnp.float32)

    with jax.named_scope("drain"):
        for item in range(4):

            @pl.loop(0, n)
            def _(s):
                for p in pieces_of(item):

                    for own in (True, False):

                        @pl.when(((s == me) if own else (s < me)) & ups(item, p, own))
                        def _():
                            z_copy(item, s, p, 0).wait_send()

                        @pl.when(((s == me) if own else (s > me)) & downs(item, p, own))
                        def _():
                            z_copy(item, s, p, 1).wait_send()

        for j in range(1, G):
            for copy in y_copies(j, False):
                copy.wait_send()
            yu_copy(j, False).wait_send()
            for k in range(TOKEN_SUBS):
                yt_copy(j, k, False).wait_send()
        for r in other_planes:
            drain_tokens(r)
        if relief:

            @pl.when(end)
            def _():
                end_meta().wait_send()
                end_down().wait_send()
                for k in range(TOKEN_SUBS):
                    end_tokens(k).wait_send()

            @pl.when(near)
            def _():
                for j in range(1, G):
                    for k in range(TOKEN_SUBS):
                        ey_copy(j, k, False).wait_send()
                for e in range(G):
                    drain_tokens(e, 1)
                    pp_copy(2, e).wait_send()
                    pp_copy(3, e).wait_send()
                for j in range(1, nt):
                    px_copy(j, False).wait_send()
                ue_copy().wait_send()

        @pl.when(~end)
        def _():
            for j in range(1, nt):
                part_copy(j, False).wait_send()

        for e, j in crossing:
            back_copy(e, j, False).wait_send()
        for ci in range(3):
            others(lambda e, a: up_copy(ci, e, a).wait_send())

        @pl.loop(0, n)
        def _(a):
            @pl.when(a != me)
            def _():
                low_copy(a).wait_send()


def layer(G, relief, x, wq, wk, wv, aq, av, bq, bv, d, blocks_of, slots, ranks, live):
    n, nt = lax.axis_size("dp"), lax.axis_size("tensor")
    rows = x.shape[0]
    depth, qcols = wq.shape
    kcols = wk.shape[1]
    width = aq.shape[1]
    hq, hk = qcols // G, kcols // G
    hc = hq // 2
    span = n * depth
    blocks = rows // REQUEST_ROWS
    far = (n - 2) * depth
    cosine, sine = rope_tables(REQUEST_ROWS, HD)
    cosine = np.concatenate([cosine, cosine], axis=-1)
    sine = np.concatenate([-sine, sine], axis=-1)
    smem = pl.BlockSpec(memory_space=pltpu.SMEM)
    vmem = pl.BlockSpec(memory_space=pltpu.VMEM)
    hbm = pl.BlockSpec(memory_space=pltpu.HBM)
    bf, f32 = jnp.bfloat16, jnp.float32
    V = pltpu.VMEM
    dma = pltpu.SemaphoreType.DMA

    def pairs_of(shape):
        return [dma(shape), dma(shape)]

    return pl.pallas_call(
        functools.partial(layer_kernel, G, relief),
        out_shape=(
            jax.ShapeDtypeStruct((R, width), f32),
            jax.ShapeDtypeStruct((R, width), f32),
            jax.ShapeDtypeStruct((R, qcols), f32),
            jax.ShapeDtypeStruct((R, kcols), f32),
        ),
        in_specs=[smem] * 4 + [hbm] * 9 + [vmem] * 2,
        out_specs=(vmem,) * 4,
        scratch_shapes=[
            V((G, rows, span), bf),
            V((span, 2 * hk), bf),
            V((span, hc), bf),
            V((span, hc), bf),
            V((n, 2 * R, width), bf),
            V((n, G, R, hq + hk), bf),
            V((G, rows, hq), bf),
            V((G, rows, 2 * hk), f32),
            V((G, rows, hc), f32),
            V((G, rows, hc), f32),
            V((nt, 2 * R, rows), f32),
            V((G + 1, 2 * R, rows), bf),
            V((G, rows, hk), bf),
            V((G, rows, hk), bf),
            V((G, rows, hk), f32),
            V((G, 2 * R, rows), f32),
            V((2, G, n, R, hc), f32),
            V((G, n, R, hk), f32),
            V((2, G, n, R, hc), bf),
            V((G, n, R, hk), bf),
            V((2, n, G, R, hc), bf),
            V((n, G, R, hk), bf),
            V((G, 2 * R, rows), bf),
            V((G, nt, 2 * R, rows), bf),
            V((n, 2 * R, width), bf),
            V((n, 2 * R, width), bf),
            pltpu.SMEM((G + 1, 128), jnp.int32),
            V((G, rows, far) if relief else (1, 16, 128), bf),
            V((rows, width) if relief else (16, 128), bf),
            V((nt, 2 * R, rows) if relief else (1, 8, 128), f32),
            V((G, rows, hc) if relief else (1, 16, 128), bf),
            V((G, rows, hc) if relief else (1, 16, 128), bf),
            V((G, rows, hc) if relief else (1, 16, 128), bf),
            V((G, rows, hc) if relief else (1, 16, 128), bf),
        ]
        + pairs_of((10,))[:1]
        + [dma((2, 4, n, SUBS)), dma((4, n, SUBS))]
        + pairs_of((G, 4))
        + pairs_of((G, TOKEN_SUBS))
        + pairs_of((2 * G, max(1, nt // 2), TOKEN_SUBS))
        + pairs_of((2 * G, nt, TOKEN_SUBS))
        + pairs_of((nt,))
        + pairs_of((G,))
        + [dma((3, G, n)), dma((3, n, G))]
        + pairs_of((G, nt))
        + pairs_of((n,))
        + [dma, dma]
        + pairs_of((TOKEN_SUBS,))
        + pairs_of((G, TOKEN_SUBS))
        + [dma, dma]
        + pairs_of((nt,))
        + [dma, dma]
        + pairs_of((2, G)),
        compiler_params=pltpu.CompilerParams(
            collective_id=0, has_side_effects=True, vmem_limit_bytes=62 * 1024 * 1024
        ),
        name="layer",
    )(blocks_of, slots, ranks, live, x, wq, wk, wv, aq, av, bq, bv, d, cosine, sine)


def on_device(
    tokens,
    w_query,
    w_key,
    w_value,
    a_query,
    b_query,
    a_value,
    b_value,
    adapter_ranks,
    adapter_slot,
    block_adapter,
    live_tokens,
    d_heads,
):
    ng, nt = lax.axis_size("groups"), lax.axis_size("tensor")
    kv_heads = w_key.shape[1] // HD
    G = ng if nt % 2 == 0 and kv_heads % ng == 0 else 1
    relief = G > 1 and lax.axis_size("dp") >= 4
    low_q, low_v, up_q, up_v = layer(
        G, relief, tokens, w_query, w_key, w_value, a_query[0].T, a_value[0].T, b_query[0], b_value[0],
        d_heads, block_adapter.reshape(-1), adapter_slot, adapter_ranks, live_tokens,
    )
    return low_q.T[None], up_q[None], low_v.T[None], up_v[None]


def solution(mesh):
    in_specs = (
        P(("groups", "dp"), None),
        P("dp", "tensor"),
        P("dp", "tensor"),
        P("dp", "tensor"),
        P(("groups", "dp"), "tensor", None),
        P(("groups", "dp"), None, "tensor"),
        P(("groups", "dp"), "tensor", None),
        P(("groups", "dp"), None, "tensor"),
        P("groups"),
        P(),
        P(("groups", "dp"), None),
        P(("groups", "dp")),
        P(("groups", "dp"), "tensor"),
    )
    out_specs = (
        P(("groups", "dp"), "tensor", None),
        P(("groups", "dp"), None, "tensor"),
        P(("groups", "dp"), "tensor", None),
        P(("groups", "dp"), None, "tensor"),
    )
    return jax.shard_map(
        on_device, mesh=mesh, in_specs=in_specs, out_specs=out_specs, check_vma=False
    )
```

```python
import functools

import jax
import jax.numpy as jnp
import numpy as np
from jax import lax
from jax.experimental import pallas as pl
from jax.experimental.pallas import tpu as pltpu
from jax.sharding import PartitionSpec as P

HD = 128
R = 32
REQUEST_ROWS = 128
MESH = pl.DeviceIdType.MESH

adapter_alpha_factor = 32.0
rope_theta = 500000.0

SUBS = 4
TOKEN_SUBS = 2
FACTORS = 1


def rope_tables(length, width):
    halfway = width // 2
    spread = rope_theta ** (-2.0 * np.arange(halfway, dtype=np.float32) / width)
    angle = np.arange(length, dtype=np.float32)[:, None] * spread.astype(np.float32)[None, :]
    return np.cos(angle).astype(np.float32), np.sin(angle).astype(np.float32)


def scale_of(rank):
    return (adapter_alpha_factor / jnp.full((1, 128), rank, jnp.int32).astype(jnp.float32))[:, :1]


def query_chunks(heads):
    quarter = heads // 4
    return [heads - 2 * quarter, quarter, quarter] if quarter else [heads]


def dot(a, c, left, right):
    return lax.dot_general(
        a, c, (((left,), (right,)), ((), ())), preferred_element_type=jnp.float32
    )


def layer_kernel(
    G,
    relief,
    block_ref,
    slot_ref,
    rank_ref,
    live_ref,
    x_hbm,
    wq_hbm,
    wk_hbm,
    wv_hbm,
    aq_hbm,
    av_hbm,
    bq_hbm,
    bv_hbm,
    d_hbm,
    cos_ref,
    sin_ref,
    out_ref,
    x_all,
    w_kv,
    w_q,
    down_all,
    b_all,
    d_all,
    acc_kv,
    acc_q,
    parts,
    u_all,
    keys_all,
    values_all,
    gv_acc,
    back_acc,
    upq_sum,
    upv_sum,
    upq_send,
    upv_send,
    upq_got,
    upv_got,
    back_send,
    back_got,
    low_send,
    low_got,
    meta,
    x_far,
    x_down,
    parts_extra,
    p_send,
    p_got,
    local_sem,
    z_send,
    z_recv,
    yb_send,
    yb_recv,
    yt_send,
    yt_recv,
    tx_send,
    tx_recv,
    tp_send,
    tp_recv,
    part_send,
    part_recv,
    yu_send,
    yu_recv,
    us_send,
    us_recv,
    bk_send,
    bk_recv,
    lo_send,
    lo_recv,
    em_send,
    em_recv,
    et_send,
    et_recv,
    ey_send,
    ey_recv,
    eu_send,
    eu_recv,
    px_send,
    px_recv,
    ue_send,
    ue_recv,
    pp_send,
    pp_recv,
):
    n = lax.axis_size("dp")
    ng = lax.axis_size("groups")
    nt = lax.axis_size("tensor")
    me = lax.axis_index("dp")
    g = lax.axis_index("groups")
    t = lax.axis_index("tensor")
    split = G > 1
    low_end, high_end = (1, n - 2) if relief else (0, n - 1)
    end = (me < low_end) | (me > high_end)
    near = ((me == 1) | (me == n - 2)) if relief else None
    inward = jnp.where(me == 0, 1, n - 2) if relief else None
    outward = jnp.where(me == 1, 0, n - 1) if relief else None
    gi = g if split else 0
    rows = x_hbm.shape[0]
    depth, qcols = wq_hbm.shape
    kcols = wk_hbm.shape[1]
    hq, hk = qcols // G, kcols // G
    kv_heads = hk // HD
    group = hq // hk
    blocks = rows // REQUEST_ROWS
    width = down_all.shape[2]
    step = depth // SUBS
    widths = [c * HD for c in query_chunks(hq // HD)]
    starts = [sum(widths[:i]) for i in range(len(widths))]
    last = len(widths) - 1
    weights = (w_kv, None) + tuple(w_q)
    wide = pl.ds(pl.multiple_of(t * width, 128), width)
    accs = (acc_kv, None) + tuple(acc_q)
    far = x_far.shape[2]
    far_of_near = jnp.where(me == 1, 2 * depth, 0)
    far_of_end = jnp.where(me == 0, 2 * depth, 0)
    close_of_end = jnp.where(me == 0, 0, far)

    def at_group(index, **rest):
        if split:
            rest["groups"] = index
        return rest

    def remote(src, dst, send, recv, to):
        return pltpu.make_async_remote_copy(
            src_ref=src, dst_ref=dst, send_sem=send, recv_sem=recv, device_id=to, device_id_type=MESH
        )

    mine = pl.ds(pl.multiple_of(me * depth, depth), depth)
    qs = pl.ds(pl.multiple_of(gi * hq, 128), hq)
    ks = pl.ds(pl.multiple_of(gi * hk, 128), hk)
    loads = [
        (wk_hbm.at[:, ks], w_kv.at[mine, pl.ds(0, hk)]),
        (wv_hbm.at[:, ks], w_kv.at[mine, pl.ds(hk, hk)]),
        (aq_hbm, down_all.at[me, pl.ds(0, R), :]),
        (av_hbm, down_all.at[me, pl.ds(R, R), :]),
        (bq_hbm.at[:, qs], b_all.at[me, gi, :, pl.ds(0, hq)]),
        (bv_hbm.at[:, ks], b_all.at[me, gi, :, pl.ds(hq, hk)]),
        (x_hbm, x_all.at[gi]),
        (d_hbm.at[:, qs], d_all.at[gi]),
    ] + [
        (wq_hbm.at[:, pl.ds(pl.multiple_of(gi * hq + c, 128), w)], ref.at[mine, :])
        for c, w, ref in zip(starts, widths, w_q)
    ]
    loads = [pltpu.make_async_copy(s, d, local_sem.at[i]) for i, (s, d) in enumerate(loads)]
    for copy in loads:
        copy.start()

    for b in range(blocks):
        adapter = block_ref[b]
        meta[gi, b] = slot_ref[adapter]
        meta[gi, blocks + b] = rank_ref[adapter]
    meta[gi, 2 * blocks] = live_ref[0]

    with jax.named_scope("greet"):
        barrier = pltpu.get_barrier_semaphore()

        @pl.loop(1, n * G)
        def _(j):
            k = lax.rem(me * G + gi + j, n * G)
            pl.semaphore_signal(
                barrier, inc=1, device_id=at_group(lax.rem(k, G), dp=lax.div(k, G)), device_id_type=MESH
            )

        for j in range(1, nt):
            for e in range(G):
                pl.semaphore_signal(
                    barrier,
                    inc=1,
                    device_id=at_group(lax.rem(gi + e, G), tensor=lax.rem(t + j, nt)),
                    device_id_type=MESH,
                )
        pl.semaphore_wait(barrier, n * G - 1 + G * (nt - 1))

    def z_copy(item, s, p, way):
        if item == FACTORS:
            ref = down_all.at[s] if p == 0 else b_all.at[s]
        else:
            ref = weights[item].at[pl.ds(pl.multiple_of(s * depth + p * step, step), step), :]
        target = jnp.clip(me + (1 if way == 0 else -1), 0, n - 1)
        return remote(
            ref, ref, z_send.at[way, item, s, p], z_recv.at[item, s, p], {"dp": target}
        )

    def pieces_of(item):
        return range(2) if item == FACTORS else range(SUBS)

    def stays_inside(item, p, own):
        if item == FACTORS:
            return p == 0
        return item > FACTORS and not own

    def ups(item, p, own):
        return me < (high_end if stays_inside(item, p, own) else n - 1)

    def downs(item, p, own):
        return me > (low_end if stays_inside(item, p, own) else 0)

    def send_own(item, pieces=None, to_end=None):
        up, down = (me < n, me >= 0) if to_end is None else (me == n - 2, me == 1)
        if to_end is False:
            up, down = ~up, ~down
        for p in pieces_of(item) if pieces is None else pieces:

            @pl.when(ups(item, p, True) & up)
            def _():
                z_copy(item, me, p, 0).start()

            @pl.when(downs(item, p, True) & down)
            def _():
                z_copy(item, me, p, 1).start()

    def forward_piece(item, d, p, static_p):
        for way in (0, 1):
            s = me - d if way == 0 else me + d
            valid = (s >= 0) if way == 0 else (s < n)
            if relief and stays_inside(item, static_p, False):
                valid = valid & (~end if item == FACTORS else ~end | (d == 1))
            onward = ups(item, static_p, False) if way == 0 else downs(item, static_p, False)
            if relief and item > 2:
                valid = valid & ~(near & (d == 1) & ((s == 0) | (s == n - 1)))

            @pl.when(valid)
            def _():
                z_copy(item, s, p, way).wait_recv()

                @pl.when(onward)
                def _():
                    z_copy(item, s, p, way).start()

    def forward_ends(item):
        for way, at in ((0, 1), (1, n - 2)):
            s = 0 if way == 0 else n - 1

            @pl.when(me == at)
            def _():
                for p in pieces_of(item):
                    z_copy(item, s, p, way).wait_recv()
                    z_copy(item, s, p, way).start()

    def line(item, after=None, hooks=()):
        hooks = dict(hooks)
        final = pieces_of(item)[-1]
        if n <= 8:
            for d in range(1, n):
                for p in pieces_of(item):
                    forward_piece(item, d, p, p)
                    if p == final and after is not None:
                        after(d)
                    for key in ((d, p), (d, None) if p == final else None):
                        if key in hooks:
                            hooks.pop(key)()
        else:

            @pl.loop(1, n)
            def _(d):
                for p in pieces_of(item):
                    forward_piece(item, d, p, p)
                if after is not None:
                    after(d)

        for hook in hooks.values():
            hook()

    def y_copies(j, arriving):
        peer = lax.rem(gi + G - j, G) if arriving else lax.rem(gi + j, G)
        at = peer if arriving else gi
        to = {"groups": peer}
        pq = pl.ds(pl.multiple_of(peer * hq, 128), hq)
        pk = pl.ds(pl.multiple_of(peer * hk, 128), hk)
        sources = (
            (bq_hbm.at[:, pq], b_all.at[me, at, :, pl.ds(0, hq)]),
            (bv_hbm.at[:, pk], b_all.at[me, at, :, pl.ds(hq, hk)]),
            (meta.at[at], meta.at[at]),
            (d_hbm.at[:, pq], d_all.at[at]),
        )
        return [
            remote(s, d, yb_send.at[j, i], yb_recv.at[j, i], to) for i, (s, d) in enumerate(sources)
        ]

    quarter = rows // nt
    sub = quarter // TOKEN_SUBS

    def token_piece(r, q, k, bank=0):
        ref = x_far if bank else x_all
        return ref.at[r, pl.ds(pl.multiple_of(q * quarter + k * sub, sub), sub), :]

    def yt_copy(j, k, arriving):
        peer = lax.rem(gi + G - j, G) if arriving else lax.rem(gi + j, G)
        ref = token_piece(peer if arriving else gi, t, k)
        return remote(ref, ref, yt_send.at[j, k], yt_recv.at[j, k], {"groups": peer})

    pairs = nt // 2
    partner = t + 1 - 2 * lax.rem(t, 2)

    def tx_copy(r, i, k, arriving, bank=0):
        peer = lax.rem(t + nt - 2 * i, nt) if arriving else lax.rem(t + 2 * i, nt)
        ref = token_piece(r, peer if arriving else t, k, bank)
        return remote(
            ref, ref, tx_send.at[bank * G + r, i, k], tx_recv.at[bank * G + r, i, k], {"tensor": peer}
        )

    def tp_copy(r, q, k, bank=0):
        ref = token_piece(r, q, k, bank)
        return remote(
            ref, ref, tp_send.at[bank * G + r, q, k], tp_recv.at[bank * G + r, q, k], {"tensor": partner}
        )

    def spread_tokens(r, k, bank=0):
        for i in range(1, pairs):
            tx_copy(r, i, k, False, bank).start()
        tp_copy(r, t, k, bank).start()

    def pass_tokens(r, bank=0):
        for k in range(TOKEN_SUBS):
            for i in range(1, pairs):
                tx_copy(r, i, k, True, bank).wait_recv()
                tp_copy(r, lax.rem(t + nt - 2 * i, nt), k, bank).start()

    def settle_tokens(r, bank=0):
        for k in range(TOKEN_SUBS):
            for i in range(pairs):
                tp_copy(r, lax.rem(partner + 2 * i, nt), k, bank).wait_recv()

    def drain_tokens(r, bank=0):
        for k in range(TOKEN_SUBS):
            for i in range(1, pairs):
                tx_copy(r, i, k, False, bank).wait_send()
            for i in range(pairs):
                tp_copy(r, lax.rem(t + 2 * i, nt), k, bank).wait_send()

    def relay_tokens(k):
        for j in range(1, G):
            yt_copy(j, k, True).wait_recv()
            spread_tokens(lax.rem(gi + G - j, G), k)

    def end_meta():
        return remote(meta.at[gi], meta.at[G], em_send, em_recv, {"dp": inward})

    def end_tokens(k):
        at = pl.ds(pl.multiple_of(t * quarter + k * sub, sub), sub)
        cols = pl.ds(pl.multiple_of(far_of_end, 128), far)
        return remote(
            x_all.at[gi, at, cols], token_piece(gi, t, k, 1), et_send.at[k], et_recv.at[k], {"dp": inward}
        )

    def end_down():
        return remote(x_all.at[gi, :, wide], x_down, eu_send, eu_recv, {"dp": inward})

    def ey_copy(j, k, arriving):
        peer = lax.rem(gi + G - j, G) if arriving else lax.rem(gi + j, G)
        ref = token_piece(peer if arriving else gi, t, k, 1)
        return remote(ref, ref, ey_send.at[j, k], ey_recv.at[j, k], {"groups": peer})

    def px_copy(j, arriving):
        peer = lax.rem(t + nt - j, nt) if arriving else lax.rem(t + j, nt)
        ref = parts_extra.at[peer if arriving else t]
        return remote(ref, ref, px_send.at[j], px_recv.at[j], {"tensor": peer})

    def ue_copy():
        return remote(u_all.at[G], u_all.at[gi], ue_send, ue_recv, {"dp": outward})

    def pp_copy(item, r):
        i = item - 2
        return remote(
            p_send[item - 2].at[r], p_got[item - 2].at[r], pp_send.at[i, r], pp_recv.at[i, r], {"dp": outward}
        )

    tile = 256 if rows % 256 == 0 else 128

    def whole_product(item, r):
        @pl.loop(0, rows // tile)
        def _(i):
            span = pl.ds(pl.multiple_of(i * tile, tile), tile)
            accs[item][r, span, :] = jnp.dot(
                x_all[r, span, :], weights[item][...], preferred_element_type=jnp.float32
            )

    def far_sums(item, r):
        rows_far = pl.ds(pl.multiple_of(far_of_near, 128), far)

        @pl.loop(0, rows // tile)
        def _(i):
            span = pl.ds(pl.multiple_of(i * tile, tile), tile)
            p_send[item - 2][r, span, :] = jnp.dot(
                x_far[r, span, :], weights[item][rows_far, :], preferred_element_type=jnp.float32
            ).astype(jnp.bfloat16)

        pp_copy(item, r).start()

    def close_product(item, r):
        close = pl.ds(pl.multiple_of(close_of_end, 128), 2 * depth)
        remote(
            p_got[item - 2].at[r], p_got[item - 2].at[r], pp_send.at[item - 2, r], pp_recv.at[item - 2, r],
            {"dp": inward},
        ).wait_recv()

        @pl.loop(0, rows // tile)
        def _(i):
            span = pl.ds(pl.multiple_of(i * tile, tile), tile)
            accs[item][r, span, :] = jnp.dot(
                x_all[r, span, close], weights[item][close, :], preferred_element_type=jnp.float32
            ) + p_got[item - 2][r, span, :].astype(jnp.float32)

    def slice_product(item, s, first):
        k_span = pl.ds(pl.multiple_of(s * depth, 128), depth)

        @pl.loop(0, G * rows // tile)
        def _(i):
            r = lax.div(i, rows // tile)
            span = pl.ds(pl.multiple_of(lax.rem(i, rows // tile) * tile, tile), tile)
            new = jnp.dot(
                x_all[r, span, k_span],
                weights[item][k_span, :],
                preferred_element_type=jnp.float32,
            )
            if first:
                accs[item][r, span, :] = new
            else:
                accs[item][r, span, :] += new

    cosine, sine = cos_ref[...], sin_ref[...]
    dims = (REQUEST_ROWS, REQUEST_ROWS)
    query_at = lax.broadcasted_iota(jnp.int32, dims, 0)
    key_at = lax.broadcasted_iota(jnp.int32, dims, 1)

    def turn(item, sign):
        return item * cosine + pltpu.roll(item, HD // 2, 1) * (sign * sine)

    def spread(total, slot, value):
        slots = jnp.full((R, 128), slot, jnp.int32)[:, :1]

        def add(a):
            total[a] += jnp.where(slots == a, value, 0.0)

        if n <= 8:
            for a in range(n):
                add(a)
        else:
            pl.loop(0, n)(add)

    def attend(r, b, ci):
        span = pl.ds(pl.multiple_of(b * REQUEST_ROWS, REQUEST_ROWS), REQUEST_ROWS)
        slot = meta[r, b]
        scale = scale_of(meta[r, blocks + b])
        live = meta[r, 2 * blocks] - b * REQUEST_ROWS
        u_q, u_v = u_all[r, :R, span], u_all[r, R:, span]
        b_cols = b_all[slot, r, :, starts[ci] : starts[ci] + widths[ci]]
        b_v = b_all[slot, r, :, hq:]
        stores = []
        heads_of = [slice(k * HD, (k + 1) * HD) for k in range(kv_heads)]
        if ci == 0:
            values = (acc_kv[r, span, hk:] + scale * dot(u_v, b_v, 0, 0)).astype(jnp.bfloat16)
            keys = [turn(acc_kv[r, span, kc], 1.0).astype(jnp.bfloat16) for kc in heads_of]
            keys = jnp.concatenate(keys, axis=1)
            yield

            def store_kv():
                keys_all[r, span, :] = keys
                values_all[r, span, :] = values

            if last:
                stores.append(store_kv)
            gv = [jnp.zeros((REQUEST_ROWS, HD), jnp.float32) for _ in heads_of]
            back = 0.0
        else:
            keys, values = keys_all[r, span, :], values_all[r, span, :]
            gv = [gv_acc[r, span, kc] for kc in heads_of]
            back = back_acc[r, :R, span]
        added = dot(u_q, b_cols, 0, 0)
        yield
        full = acc_q[ci][r, span, :] + scale * added
        live_rows = lax.broadcasted_iota(jnp.int32, (REQUEST_ROWS, HD), 0) < live
        allowed = (key_at <= query_at) & ((key_at < live) | (key_at == query_at))
        allowed = allowed.astype(jnp.float32)
        pieces = []
        first = starts[ci] // HD
        for k in range(kv_heads):
            heads = [i for i in range(widths[ci] // HD) if (first + i) // group == k]
            if not heads:
                continue
            head_keys, head_values = keys[:, heads_of[k]], values[:, heads_of[k]]
            queries = jnp.concatenate(
                [turn(full[:, i * HD : (i + 1) * HD], 1.0).astype(jnp.bfloat16) for i in heads],
                axis=0,
            )
            douts = []
            for i in heads:
                rows_in = d_all[r, span, (first + i) * HD : (first + i + 1) * HD]
                kept = jnp.where(live_rows, rows_in.astype(jnp.float32), 0.0)
                douts.append(kept.astype(jnp.bfloat16))
            dout = jnp.concatenate(douts, axis=0)
            yield
            scores = dot(queries, head_keys, 1, 1)
            dprobs = dot(dout, head_values, 1, 1)
            yield
            mask = jnp.concatenate([allowed] * len(heads), axis=0) > 0.5
            scores = jnp.where(mask, scores * HD ** (-0.5), -1e30)
            top = jnp.max(scores, axis=-1, keepdims=True)
            yield
            expo = jnp.exp(scores - top)
            total = jnp.sum(expo, axis=-1, keepdims=True)
            yield
            probs = expo / total
            mean = jnp.sum(dprobs * probs, axis=-1, keepdims=True)
            yield
            dscores = (probs * (dprobs - mean)).astype(jnp.bfloat16)
            dquery = dot(dscores, head_keys, 1, 0)
            gv[k] = gv[k] + dot(probs.astype(jnp.bfloat16), dout, 0, 0)
            yield
            dquery = dquery * HD ** (-0.5)
            for i in range(len(heads)):
                piece = dquery[i * REQUEST_ROWS : (i + 1) * REQUEST_ROWS]
                pieces.append(turn(piece, -1.0).astype(jnp.bfloat16))
            yield
        gq = jnp.concatenate(pieces, axis=1)
        up = dot(u_q, gq, 1, 0)
        back_new = dot(b_cols, gq, 1, 1)
        gv = jnp.concatenate(gv, axis=1)
        if ci == last:
            gv = gv.astype(jnp.bfloat16)
            up_v = dot(u_v, gv, 1, 0)
            back_v = dot(b_v, gv, 1, 1)
        yield
        up = scale * up
        back = back + scale * back_new
        if ci == last:
            up_v, back_v = scale * up_v, scale * back_v

        def store():
            back_acc[r, :R, span] = back
            spread(upq_sum[ci].at[r], slot, up)
            if ci == last:
                back_acc[r, R:, span] = back_v
                spread(upv_sum.at[r], slot, up_v)
            else:
                gv_acc[r, span, :] = gv

        yield stores + [store]

    together = 4 if blocks % 4 == 0 else 1

    def attend_chunk(ci):
        @pl.loop(0, G)
        def _(e):
            r = lax.rem(gi + e, G)
            if relief:

                @pl.when(end)
                def _():
                    close_product(2 + ci, r)

            if ci == 0:

                @pl.when(e == 1)
                def _():
                    for j in range(1, G):
                        yu_copy(j, True).wait_recv()

            @pl.loop(0, blocks // together)
            def _(i):
                running = [attend(r, i * together + j, ci) for j in range(together)]
                for step in zip(*running):
                    for store in [store for stores in step for store in stores or ()]:
                        store()

    def part_copy(j, arriving):
        peer = lax.rem(t + nt - j, nt) if arriving else lax.rem(t + j, nt)
        ref = parts.at[peer if arriving else t]
        return remote(ref, ref, part_send.at[j], part_recv.at[j], {"tensor": peer})

    def down_product(r, x_ref, into):
        for b in range(blocks):
            span = slice(b * REQUEST_ROWS, (b + 1) * REQUEST_ROWS)
            into[t, :, span] = dot(down_all[meta[r, b]], x_ref[span, :], 1, 1)

    def down_sum(r, terms):
        for b in range(blocks):
            span = slice(b * REQUEST_ROWS, (b + 1) * REQUEST_ROWS)
            total = terms[0, :, span]
            for j in range(1, nt):
                total = total + terms[j, :, span]
            kept = jnp.where(row_at < meta[r, blocks + b], total, 0.0)
            u_all[r, :, span] = kept.astype(jnp.bfloat16)

    def down_parts():
        @pl.when(~end)
        def _():
            down_product(gi, x_all.at[gi, :, wide], parts)
            for j in range(1, nt):
                part_copy(j, False).start()

    row_at = lax.broadcasted_iota(jnp.int32, (2 * R, REQUEST_ROWS), 0)
    row_at = jnp.where(row_at >= R, row_at - R, row_at)

    def yu_copy(j, arriving):
        peer = lax.rem(gi + G - j, G) if arriving else lax.rem(gi + j, G)
        ref = u_all.at[peer if arriving else gi]
        return remote(ref, ref, yu_send.at[j], yu_recv.at[j], {"groups": peer})

    def finish_down():
        @pl.when(~end)
        def _():
            for j in range(1, nt):
                part_copy(j, True).wait_recv()
            down_sum(gi, parts)

        if relief:

            @pl.when(end)
            def _():
                ue_copy().wait_recv()

        for j in range(1, G):
            yu_copy(j, False).start()

    def up_copy(ci, e, a):
        there = lax.rem(gi + e, G)
        src = upv_send.at[there, a] if ci > last else upq_send[ci].at[there, a]
        dst = upv_got.at[me, gi] if ci > last else upq_got[ci].at[me, gi]
        return remote(
            src, dst, us_send.at[ci, e, a], us_recv.at[ci, me, gi], at_group(there, dp=a)
        )

    def up_arrival(ci, e, s):
        there = lax.rem(gi + e, G)
        dst = upv_got.at[s, there] if ci > last else upq_got[ci].at[s, there]
        return remote(dst, dst, us_send.at[ci, e, s], us_recv.at[ci, s, there], at_group(there, dp=s))

    def others(body):
        @pl.loop(0, n)
        def _(a):
            for e in range(G):
                if e == 0:

                    @pl.when(a != me)
                    def _():
                        body(e, a)

                else:
                    body(e, a)

    def send_ups(ci):
        if ci > last:
            upv_send[...] = upv_sum[...].astype(jnp.bfloat16)
            upv_got[me, gi] = upv_send[gi, me]
        else:
            upq_send[ci][...] = upq_sum[ci][...].astype(jnp.bfloat16)
            upq_got[ci][me, gi] = upq_send[ci][gi, me]
        others(lambda e, a: up_copy(ci, e, a).start())

    with jax.named_scope("start"):
        own_w = (loads[0], loads[1])
        for copy in own_w:
            copy.wait()
        send_own(0)
        for j in range(1, G):
            for copy in y_copies(j, False)[:3]:
                copy.start()
        if relief:

            @pl.when(end)
            def _():
                end_meta().start()

        loads[6].wait()
        for j in range(1, G):
            for k in range(TOKEN_SUBS):
                yt_copy(j, k, False).start()
            y_copies(j, False)[3].start()
        for copy in loads[2:6]:
            copy.wait()
        send_own(FACTORS, (0,))
        for j in range(1, G):
            for copy in y_copies(j, True)[:3]:
                copy.wait_recv()
        send_own(FACTORS, (1,))
        for copy in loads[8:]:
            copy.wait()
        if relief:

            @pl.when(end)
            def _():
                for k in range(TOKEN_SUBS):
                    end_tokens(k).start()

        if relief:

            @pl.when(end)
            def _():
                send_own(2)
                send_own(3)
                end_down().start()
                send_own(4)

        for ref in upq_sum:
            ref[...] = jnp.zeros_like(ref)
        upv_sum[...] = jnp.zeros_like(upv_sum)
        loads[7].wait()
    other_planes = [lax.rem(gi + j, G) for j in range(1, G)]
    inward_only = False if relief else None

    def next_own(item, to_end):
        @pl.when(~end)
        def _():
            send_own(item, to_end=to_end)

    def after_first():
        next_own(2, None)
        relay_tokens(0)

    with jax.named_scope("line0"):
        relays = [((2, 1), functools.partial(relay_tokens, k)) for k in range(1, TOKEN_SUBS)]
        line(0, hooks=[((1, None), after_first)] + relays)
    if relief:
        with jax.named_scope("relay_extra"):

            @pl.when(near)
            def _():
                remote(meta.at[G], meta.at[G], em_send, em_recv, {"dp": outward}).wait_recv()
                for k in range(TOKEN_SUBS):
                    et = token_piece(gi, t, k, 1)
                    remote(et, et, et_send.at[k], et_recv.at[k], {"dp": outward}).wait_recv()
                    for j in range(1, G):
                        ey_copy(j, k, False).start()
                    spread_tokens(gi, k, 1)

    def pass_other():
        for r in other_planes:
            pass_tokens(r)

    with jax.named_scope("linef"):
        line(FACTORS, hooks=[((1, None), pass_other), ((n - 1, 1), down_parts)])
        if relief:

            @pl.when(near)
            def _():
                for item in range(3, 3 + last):
                    send_own(item, to_end=True)

    def extra_pass():
        if last:
            next_own(3, inward_only)
        if relief:
            forward_ends(3)
            next_own(4, inward_only)

            @pl.when(near)
            def _():
                pass_tokens(gi, 1)
                for j in range(1, G):
                    for k in range(TOKEN_SUBS):
                        ey_copy(j, k, True).wait_recv()
                        spread_tokens(lax.rem(gi + G - j, G), k, 1)

        whole_product(0, gi)

    def tokens_done():
        for r in other_planes:
            settle_tokens(r)
            whole_product(0, r)

        @pl.when(~end)
        def _():
            finish_down()

    with jax.named_scope("line2"):
        line(2, hooks=[((1, None), extra_pass), ((2, None), tokens_done)])

    if relief:
        with jax.named_scope("far_sums"):

            @pl.when(near)
            def _():
                settle_tokens(gi, 1)
                far_sums(2, gi)

    @pl.when(~end)
    def _():
        for ci in range(1, last + 1):
            slice_product(2 + ci, me, True)

    def before_attention():
        @pl.when(~end)
        def _():
            for e in range(G):
                whole_product(2, lax.rem(gi + e, G))

        for j in range(1, G):
            y_copies(j, True)[3].wait_recv()
        if relief:

            @pl.when(near)
            def _():
                for r in other_planes:
                    pass_tokens(r, 1)
                    settle_tokens(r, 1)
                    far_sums(2, r)

            @pl.when(end)
            def _():
                finish_down()

    def extra_down():
        remote(x_down, x_down, eu_send, eu_recv, {"dp": outward}).wait_recv()
        down_product(G, x_down, parts_extra)
        for j in range(1, nt):
            px_copy(j, False).start()

    def extra_down_sum():
        for j in range(1, nt):
            px_copy(j, True).wait_recv()
        down_sum(G, parts_extra)
        ue_copy().start()

    if not last:
        before_attention()
    for ci in range(1, last + 1):
        item = 2 + ci

        def products(d):
            for way in (0, 1):
                s = me - d if way == 0 else me + d

                @pl.when(((s >= 0) if way == 0 else (s < n)) & ~end)
                def _():
                    slice_product(item, s, False)

        def between_distances():
            if ci < last and not relief:
                next_own(item + 1, inward_only)
            if ci == 1:
                before_attention()
            if relief and ci == 1:
                pl.when(near)(extra_down)
            with jax.named_scope("att"):
                attend_chunk(ci - 1)
            if relief and ci == 1:
                forward_ends(4)
                pl.when(near)(extra_down_sum)

        with jax.named_scope(f"line{item}"):
            line(item, after=products, hooks=[((1, None), between_distances)])
        if relief:

            @pl.when(near)
            def _():
                for e in range(G):
                    far_sums(item, lax.rem(gi + e, G))

    with jax.named_scope("ups"):
        for ci in range(last):
            send_ups(ci)
    with jax.named_scope("tail_attend"):
        attend_chunk(last)

    with jax.named_scope("back"):
        for r in range(G):
            back_send[r] = back_acc[r].astype(jnp.bfloat16)

    def back_copy(e, j, arriving):
        there = lax.rem(gi + e, G)
        peer = lax.rem(t + nt - j, nt) if arriving else lax.rem(t + j, nt)
        if arriving:
            dst = back_got.at[there, peer]
            return remote(
                dst, dst, bk_send.at[e, j], bk_recv.at[there, peer], at_group(there, tensor=peer)
            )
        return remote(
            back_send.at[there],
            back_got.at[gi, t],
            bk_send.at[e, j],
            bk_recv.at[gi, t],
            at_group(there, tensor=peer),
        )

    crossing = [(e, j) for e in range(G) for j in range(nt) if (e, j) != (0, 0)]
    with jax.named_scope("backx"):
        for e, j in crossing:
            back_copy(e, j, False).start()
        send_ups(last)
        send_ups(last + 1)
        back_got[gi, t] = back_send[gi]
        for e, j in crossing:
            back_copy(e, j, True).wait_recv()
    total = jnp.zeros(back_acc.shape[1:], jnp.float32)
    for r in range(G):
        for j in range(nt):
            total = total + back_got[r, j].astype(jnp.float32)
    kept = []
    for b in range(blocks):
        span = slice(b * REQUEST_ROWS, (b + 1) * REQUEST_ROWS)
        kept.append(jnp.where(row_at < meta[gi, blocks + b], total[:, span], 0.0))
    def low_copy(a):
        return remote(
            low_send.at[a], low_got.at[me], lo_send.at[a], lo_recv.at[me], {"dp": a}
        )

    stack = 4 if n % 4 == 0 else 1

    with jax.named_scope("low"):
        @pl.loop(0, n // stack)
        def _(q):
            chosen = jnp.concatenate(
                [
                    jnp.concatenate(
                        [
                            jnp.where(
                                jnp.full((2 * R, REQUEST_ROWS), meta[gi, b], jnp.int32) == q * stack + i,
                                kept[b],
                                0.0,
                            )
                            for b in range(blocks)
                        ],
                        axis=1,
                    )
                    for i in range(stack)
                ],
                axis=0,
            ).astype(jnp.bfloat16)
            low = jnp.dot(chosen, x_all[gi, :, wide], preferred_element_type=jnp.float32)
            for i in range(stack):
                a = q * stack + i
                low_send[a] = low[i * 2 * R : (i + 1) * 2 * R].astype(jnp.bfloat16)

                @pl.when(a != me)
                def _():
                    low_copy(a).start()

        low_got[me] = low_send[me]

    with jax.named_scope("upsum"):
        for ci in range(last + 2):
            others(lambda e, s: up_arrival(ci, e, s).wait_recv())
        at = 2 * width
        for e in range(G):
            for ci in range(last + 1):
                out = jnp.zeros((R, widths[ci]), jnp.float32)
                out = lax.fori_loop(
                    0, n, lambda s, v: v + upq_got[ci][s, e].astype(jnp.float32), out
                )
                out_ref[:, at + e * hq + starts[ci] : at + e * hq + starts[ci] + widths[ci]] = out
            out = jnp.zeros((R, hk), jnp.float32)
            out = lax.fori_loop(0, n, lambda s, v: v + upv_got[s, e].astype(jnp.float32), out)
            out_ref[:, at + qcols + e * hk : at + qcols + (e + 1) * hk] = out

    with jax.named_scope("lowx"):
        @pl.loop(0, n)
        def _(s):
            @pl.when(s != me)
            def _():
                remote(
                    low_got.at[s], low_got.at[s], lo_send.at[s], lo_recv.at[s], {"dp": s}
                ).wait_recv()

        for i in range(2):
            out = jnp.zeros((R, width), jnp.float32)
            out = lax.fori_loop(
                0, n, lambda s, v: v + low_got[s, i * R : (i + 1) * R, :].astype(jnp.float32), out
            )
            out_ref[:, i * width : (i + 1) * width] = out

        for item in range(3 + last):

            @pl.loop(0, n)
            def _(s):
                for p in pieces_of(item):

                    for own in (True, False):

                        @pl.when(((s == me) if own else (s < me)) & ups(item, p, own))
                        def _():
                            z_copy(item, s, p, 0).wait_send()

                        @pl.when(((s == me) if own else (s > me)) & downs(item, p, own))
                        def _():
                            z_copy(item, s, p, 1).wait_send()

        for j in range(1, G):
            for copy in y_copies(j, False):
                copy.wait_send()
            yu_copy(j, False).wait_send()
            for k in range(TOKEN_SUBS):
                yt_copy(j, k, False).wait_send()
        for r in other_planes:
            drain_tokens(r)
        if relief:

            @pl.when(end)
            def _():
                end_meta().wait_send()
                end_down().wait_send()
                for k in range(TOKEN_SUBS):
                    end_tokens(k).wait_send()

            @pl.when(near)
            def _():
                for j in range(1, G):
                    for k in range(TOKEN_SUBS):
                        ey_copy(j, k, False).wait_send()
                for e in range(G):
                    drain_tokens(e, 1)
                    for item in range(2, 3 + last):
                        pp_copy(item, e).wait_send()
                for j in range(1, nt):
                    px_copy(j, False).wait_send()
                ue_copy().wait_send()

        @pl.when(~end)
        def _():
            for j in range(1, nt):
                part_copy(j, False).wait_send()

        for e, j in crossing:
            back_copy(e, j, False).wait_send()
        for ci in range(last + 2):
            others(lambda e, a: up_copy(ci, e, a).wait_send())

        @pl.loop(0, n)
        def _(a):
            @pl.when(a != me)
            def _():
                low_copy(a).wait_send()


def layer(G, relief, x, wq, wk, wv, aq, av, bq, bv, d, blocks_of, slots, ranks, live):
    n, nt = lax.axis_size("dp"), lax.axis_size("tensor")
    rows = x.shape[0]
    depth, qcols = wq.shape
    kcols = wk.shape[1]
    width = aq.shape[1]
    hq, hk = qcols // G, kcols // G
    widths = [c * HD for c in query_chunks(hq // HD)]
    span = n * depth
    blocks = rows // REQUEST_ROWS
    far = (n - 2) * depth
    cosine, sine = rope_tables(REQUEST_ROWS, HD)
    cosine = np.concatenate([cosine, cosine], axis=-1)
    sine = np.concatenate([-sine, sine], axis=-1)
    smem = pl.BlockSpec(memory_space=pltpu.SMEM)
    vmem = pl.BlockSpec(memory_space=pltpu.VMEM)
    hbm = pl.BlockSpec(memory_space=pltpu.HBM)
    bf, f32 = jnp.bfloat16, jnp.float32
    V = pltpu.VMEM
    dma = pltpu.SemaphoreType.DMA

    def pairs_of(shape):
        return [dma(shape), dma(shape)]

    return pl.pallas_call(
        functools.partial(layer_kernel, G, relief),
        out_shape=(
            jax.ShapeDtypeStruct((R, 2 * width + qcols + kcols), f32)
        ),
        in_specs=[smem] * 4 + [hbm] * 9 + [vmem] * 2,
        out_specs=vmem,
        scratch_shapes=[
            V((G, rows, span), bf),
            V((span, 2 * hk), bf),
            [V((span, w), bf) for w in widths],
            V((n, 2 * R, width), bf),
            V((n, G, R, hq + hk), bf),
            V((G, rows, hq), bf),
            V((G, rows, 2 * hk), f32),
            [V((G, rows, w), f32) for w in widths],
            V((nt, 2 * R, rows), f32),
            V((G + 1, 2 * R, rows), bf),
            V((G, rows, hk), bf),
            V((G, rows, hk), bf),
            V((G, rows, hk), f32),
            V((G, 2 * R, rows), f32),
            [V((G, n, R, w), f32) for w in widths],
            V((G, n, R, hk), f32),
            [V((G, n, R, w), bf) for w in widths],
            V((G, n, R, hk), bf),
            [V((n, G, R, w), bf) for w in widths],
            V((n, G, R, hk), bf),
            V((G, 2 * R, rows), bf),
            V((G, nt, 2 * R, rows), bf),
            V((n, 2 * R, width), bf),
            V((n, 2 * R, width), bf),
            pltpu.SMEM((G + 1, 128), jnp.int32),
            V((G, rows, far) if relief else (1, 16, 128), bf),
            V((rows, width) if relief else (16, 128), bf),
            V((nt, 2 * R, rows) if relief else (1, 8, 128), f32),
            [V((G, rows, w) if relief else (1, 16, 128), bf) for w in widths],
            [V((G, rows, w) if relief else (1, 16, 128), bf) for w in widths],
        ]
        + [dma((8 + len(widths),))]
        + [dma((2, 2 + len(widths), n, SUBS)), dma((2 + len(widths), n, SUBS))]
        + pairs_of((G, 4))
        + pairs_of((G, TOKEN_SUBS))
        + pairs_of((2 * G, max(1, nt // 2), TOKEN_SUBS))
        + pairs_of((2 * G, nt, TOKEN_SUBS))
        + pairs_of((nt,))
        + pairs_of((G,))
        + [dma((1 + len(widths), G, n)), dma((1 + len(widths), n, G))]
        + pairs_of((G, nt))
        + pairs_of((n,))
        + [dma, dma]
        + pairs_of((TOKEN_SUBS,))
        + pairs_of((G, TOKEN_SUBS))
        + [dma, dma]
        + pairs_of((nt,))
        + [dma, dma]
        + pairs_of((len(widths), G)),
        compiler_params=pltpu.CompilerParams(
            collective_id=0, has_side_effects=True, vmem_limit_bytes=62 * 1024 * 1024
        ),
        name="layer",
    )(blocks_of, slots, ranks, live, x, wq, wk, wv, aq, av, bq, bv, d, cosine, sine)


def on_device(
    tokens,
    w_query,
    w_key,
    w_value,
    a_query,
    b_query,
    a_value,
    b_value,
    adapter_ranks,
    adapter_slot,
    block_adapter,
    live_tokens,
    d_heads,
):
    ng, nt = lax.axis_size("groups"), lax.axis_size("tensor")
    kv_heads = w_key.shape[1] // HD
    G = ng if nt % 2 == 0 and kv_heads % ng == 0 else 1
    chunks = len(query_chunks(w_query.shape[1] // G // HD))
    relief = G > 1 and lax.axis_size("dp") >= 4 and chunks == 3
    out = layer(
        G, relief, tokens, w_query, w_key, w_value, a_query[0].T, a_value[0].T, b_query[0], b_value[0],
        d_heads, block_adapter.reshape(-1), adapter_slot, adapter_ranks, live_tokens,
    )
    width, qcols = a_query.shape[1], b_query.shape[2]
    low_q, low_v = out[:, :width], out[:, width : 2 * width]
    up_q, up_v = out[:, 2 * width : 2 * width + qcols], out[:, 2 * width + qcols :]
    return low_q.T[None], up_q[None], low_v.T[None], up_v[None]


def solution(mesh):
    in_specs = (
        P(("groups", "dp"), None),
        P("dp", "tensor"),
        P("dp", "tensor"),
        P("dp", "tensor"),
        P(("groups", "dp"), "tensor", None),
        P(("groups", "dp"), None, "tensor"),
        P(("groups", "dp"), "tensor", None),
        P(("groups", "dp"), None, "tensor"),
        P("groups"),
        P(),
        P(("groups", "dp"), None),
        P(("groups", "dp")),
        P(("groups", "dp"), "tensor"),
    )
    out_specs = (
        P(("groups", "dp"), "tensor", None),
        P(("groups", "dp"), None, "tensor"),
        P(("groups", "dp"), "tensor", None),
        P(("groups", "dp"), None, "tensor"),
    )
    return jax.shard_map(
        on_device, mesh=mesh, in_specs=in_specs, out_specs=out_specs, check_vma=False
    )
```

```python
import functools

import jax
import jax.numpy as jnp
import numpy as np
from jax import lax
from jax.experimental import pallas as pl
from jax.experimental.pallas import tpu as pltpu
from jax.sharding import PartitionSpec as P

HD = 128
R = 32
REQUEST_ROWS = 128
MESH = pl.DeviceIdType.MESH

adapter_alpha_factor = 32.0
rope_theta = 500000.0

SUBS = 4
TOKEN_SUBS = 2
FACTORS = 1


def rope_tables(length, width):
    halfway = width // 2
    spread = rope_theta ** (-2.0 * np.arange(halfway, dtype=np.float32) / width)
    angle = np.arange(length, dtype=np.float32)[:, None] * spread.astype(np.float32)[None, :]
    return np.cos(angle).astype(np.float32), np.sin(angle).astype(np.float32)


def scale_of(rank):
    return (adapter_alpha_factor / jnp.full((1, 128), rank, jnp.int32).astype(jnp.float32))[:, :1]


def query_chunks(heads):
    quarter = heads // 4
    return [heads - 2 * quarter, quarter, quarter] if quarter else [heads]


def dot(a, c, left, right):
    return lax.dot_general(
        a, c, (((left,), (right,)), ((), ())), preferred_element_type=jnp.float32
    )


def layer_kernel(
    G,
    relief,
    block_ref,
    slot_ref,
    rank_ref,
    live_ref,
    x_hbm,
    wq_hbm,
    wk_hbm,
    wv_hbm,
    aq_hbm,
    av_hbm,
    bq_hbm,
    bv_hbm,
    d_hbm,
    cos_ref,
    sin_ref,
    out_ref,
    x_all,
    w_kv,
    w_q,
    down_all,
    b_all,
    d_all,
    acc_kv,
    acc_q,
    parts,
    u_all,
    keys_all,
    values_all,
    gv_acc,
    back_acc,
    upq_sum,
    upv_sum,
    upq_send,
    upv_send,
    upq_got,
    upv_got,
    back_send,
    back_got,
    back_all,
    low_send,
    low_got,
    meta,
    x_far,
    x_down,
    parts_extra,
    p_send,
    p_got,
    local_sem,
    z_send,
    z_recv,
    yb_send,
    yb_recv,
    yt_send,
    yt_recv,
    tx_send,
    tx_recv,
    tp_send,
    tp_recv,
    part_send,
    part_recv,
    yu_send,
    yu_recv,
    us_send,
    us_recv,
    bk_send,
    bk_recv,
    lo_send,
    lo_recv,
    em_send,
    em_recv,
    et_send,
    et_recv,
    ey_send,
    ey_recv,
    eu_send,
    eu_recv,
    px_send,
    px_recv,
    ue_send,
    ue_recv,
    pp_send,
    pp_recv,
    ba_send,
    ba_recv,
):
    n = lax.axis_size("dp")
    ng = lax.axis_size("groups")
    nt = lax.axis_size("tensor")
    me = lax.axis_index("dp")
    g = lax.axis_index("groups")
    t = lax.axis_index("tensor")
    split = G > 1
    low_end, high_end = (1, n - 2) if relief else (0, n - 1)
    end = (me < low_end) | (me > high_end)
    near = ((me == 1) | (me == n - 2)) if relief else None
    inward = jnp.where(me == 0, 1, n - 2) if relief else None
    outward = jnp.where(me == 1, 0, n - 1) if relief else None
    gi = g if split else 0
    rows = x_hbm.shape[0]
    depth, qcols = wq_hbm.shape
    kcols = wk_hbm.shape[1]
    hq, hk = qcols // G, kcols // G
    kv_heads = hk // HD
    group = hq // hk
    blocks = rows // REQUEST_ROWS
    width = down_all.shape[2]
    step = depth // SUBS
    widths = [c * HD for c in query_chunks(hq // HD)]
    starts = [sum(widths[:i]) for i in range(len(widths))]
    last = len(widths) - 1
    weights = (w_kv, None) + tuple(w_q)
    wide = pl.ds(pl.multiple_of(t * width, 128), width)
    accs = (acc_kv, None) + tuple(acc_q)
    far = x_far.shape[2]
    far_of_near = jnp.where(me == 1, 2 * depth, 0)
    far_of_end = jnp.where(me == 0, 2 * depth, 0)
    close_of_end = jnp.where(me == 0, 0, far)

    def at_group(index, **rest):
        if split:
            rest["groups"] = index
        return rest

    def remote(src, dst, send, recv, to):
        return pltpu.make_async_remote_copy(
            src_ref=src, dst_ref=dst, send_sem=send, recv_sem=recv, device_id=to, device_id_type=MESH
        )

    mine = pl.ds(pl.multiple_of(me * depth, depth), depth)
    qs = pl.ds(pl.multiple_of(gi * hq, 128), hq)
    ks = pl.ds(pl.multiple_of(gi * hk, 128), hk)
    loads = [
        (wk_hbm.at[:, ks], w_kv.at[mine, pl.ds(0, hk)]),
        (wv_hbm.at[:, ks], w_kv.at[mine, pl.ds(hk, hk)]),
        (aq_hbm, down_all.at[me, pl.ds(0, R), :]),
        (av_hbm, down_all.at[me, pl.ds(R, R), :]),
        (bq_hbm.at[:, qs], b_all.at[me, gi, :, pl.ds(0, hq)]),
        (bv_hbm.at[:, ks], b_all.at[me, gi, :, pl.ds(hq, hk)]),
        (x_hbm, x_all.at[gi]),
        (d_hbm.at[:, qs], d_all.at[gi]),
    ] + [
        (wq_hbm.at[:, pl.ds(pl.multiple_of(gi * hq + c, 128), w)], ref.at[mine, :])
        for c, w, ref in zip(starts, widths, w_q)
    ]
    loads = [pltpu.make_async_copy(s, d, local_sem.at[i]) for i, (s, d) in enumerate(loads)]
    for copy in loads:
        copy.start()

    for b in range(blocks):
        adapter = block_ref[b]
        meta[gi, b] = slot_ref[adapter]
        meta[gi, blocks + b] = rank_ref[adapter]
    meta[gi, 2 * blocks] = live_ref[0]

    with jax.named_scope("greet"):
        barrier = pltpu.get_barrier_semaphore()

        @pl.loop(1, n * G)
        def _(j):
            k = lax.rem(me * G + gi + j, n * G)
            pl.semaphore_signal(
                barrier, inc=1, device_id=at_group(lax.rem(k, G), dp=lax.div(k, G)), device_id_type=MESH
            )

        for j in range(1, nt):
            for e in range(G):
                pl.semaphore_signal(
                    barrier,
                    inc=1,
                    device_id=at_group(lax.rem(gi + e, G), tensor=lax.rem(t + j, nt)),
                    device_id_type=MESH,
                )
        pl.semaphore_wait(barrier, n * G - 1 + G * (nt - 1))

    def z_copy(item, s, p, way):
        if item == FACTORS:
            ref = down_all.at[s] if p == 0 else b_all.at[s]
        else:
            ref = weights[item].at[pl.ds(pl.multiple_of(s * depth + p * step, step), step), :]
        target = jnp.clip(me + (1 if way == 0 else -1), 0, n - 1)
        return remote(
            ref, ref, z_send.at[way, item, s, p], z_recv.at[item, s, p], {"dp": target}
        )

    def pieces_of(item):
        return range(2) if item == FACTORS else range(SUBS)

    def stays_inside(item, p, own):
        if item == FACTORS:
            return p == 0
        return item > FACTORS and not own

    def ups(item, p, own):
        return me < (high_end if stays_inside(item, p, own) else n - 1)

    def downs(item, p, own):
        return me > (low_end if stays_inside(item, p, own) else 0)

    def send_own(item, pieces=None, to_end=None):
        up, down = (me < n, me >= 0) if to_end is None else (me == n - 2, me == 1)
        if to_end is False:
            up, down = ~up, ~down
        for p in pieces_of(item) if pieces is None else pieces:

            @pl.when(ups(item, p, True) & up)
            def _():
                z_copy(item, me, p, 0).start()

            @pl.when(downs(item, p, True) & down)
            def _():
                z_copy(item, me, p, 1).start()

    def forward_piece(item, d, p, static_p):
        for way in (0, 1):
            s = me - d if way == 0 else me + d
            valid = (s >= 0) if way == 0 else (s < n)
            if relief and stays_inside(item, static_p, False):
                valid = valid & (~end if item == FACTORS else ~end | (d == 1))
            onward = ups(item, static_p, False) if way == 0 else downs(item, static_p, False)
            if relief and item > 2:
                valid = valid & ~(near & (d == 1) & ((s == 0) | (s == n - 1)))

            @pl.when(valid)
            def _():
                z_copy(item, s, p, way).wait_recv()

                @pl.when(onward)
                def _():
                    z_copy(item, s, p, way).start()

    def forward_ends(item):
        for way, at in ((0, 1), (1, n - 2)):
            s = 0 if way == 0 else n - 1

            @pl.when(me == at)
            def _():
                for p in pieces_of(item):
                    z_copy(item, s, p, way).wait_recv()
                    z_copy(item, s, p, way).start()

    def line(item, after=None, hooks=()):
        hooks = dict(hooks)
        final = pieces_of(item)[-1]
        if n <= 8:
            for d in range(1, n):
                for p in pieces_of(item):
                    forward_piece(item, d, p, p)
                    if p == final and after is not None:
                        after(d)
                    for key in ((d, p), (d, None) if p == final else None):
                        if key in hooks:
                            hooks.pop(key)()
        else:

            @pl.loop(1, n)
            def _(d):
                for p in pieces_of(item):
                    forward_piece(item, d, p, p)
                if after is not None:
                    after(d)

        for hook in hooks.values():
            hook()

    def y_copies(j, arriving):
        peer = lax.rem(gi + G - j, G) if arriving else lax.rem(gi + j, G)
        at = peer if arriving else gi
        to = {"groups": peer}
        pq = pl.ds(pl.multiple_of(peer * hq, 128), hq)
        pk = pl.ds(pl.multiple_of(peer * hk, 128), hk)
        sources = (
            (bq_hbm.at[:, pq], b_all.at[me, at, :, pl.ds(0, hq)]),
            (bv_hbm.at[:, pk], b_all.at[me, at, :, pl.ds(hq, hk)]),
            (meta.at[at], meta.at[at]),
            (d_hbm.at[:, pq], d_all.at[at]),
        )
        return [
            remote(s, d, yb_send.at[j, i], yb_recv.at[j, i], to) for i, (s, d) in enumerate(sources)
        ]

    quarter = rows // nt
    sub = quarter // TOKEN_SUBS

    def token_piece(r, q, k, bank=0):
        ref = x_far if bank else x_all
        return ref.at[r, pl.ds(pl.multiple_of(q * quarter + k * sub, sub), sub), :]

    def yt_copy(j, k, arriving):
        peer = lax.rem(gi + G - j, G) if arriving else lax.rem(gi + j, G)
        ref = token_piece(peer if arriving else gi, t, k)
        return remote(ref, ref, yt_send.at[j, k], yt_recv.at[j, k], {"groups": peer})

    pairs = nt // 2
    partner = t + 1 - 2 * lax.rem(t, 2)

    def tx_copy(r, i, k, arriving, bank=0):
        peer = lax.rem(t + nt - 2 * i, nt) if arriving else lax.rem(t + 2 * i, nt)
        ref = token_piece(r, peer if arriving else t, k, bank)
        return remote(
            ref, ref, tx_send.at[bank * G + r, i, k], tx_recv.at[bank * G + r, i, k], {"tensor": peer}
        )

    def tp_copy(r, q, k, bank=0):
        ref = token_piece(r, q, k, bank)
        return remote(
            ref, ref, tp_send.at[bank * G + r, q, k], tp_recv.at[bank * G + r, q, k], {"tensor": partner}
        )

    def spread_tokens(r, k, bank=0):
        for i in range(1, pairs):
            tx_copy(r, i, k, False, bank).start()
        tp_copy(r, t, k, bank).start()

    def pass_tokens(r, bank=0):
        for k in range(TOKEN_SUBS):
            for i in range(1, pairs):
                tx_copy(r, i, k, True, bank).wait_recv()
                tp_copy(r, lax.rem(t + nt - 2 * i, nt), k, bank).start()

    def settle_tokens(r, bank=0):
        for k in range(TOKEN_SUBS):
            for i in range(pairs):
                tp_copy(r, lax.rem(partner + 2 * i, nt), k, bank).wait_recv()

    def drain_tokens(r, bank=0):
        for k in range(TOKEN_SUBS):
            for i in range(1, pairs):
                tx_copy(r, i, k, False, bank).wait_send()
            for i in range(pairs):
                tp_copy(r, lax.rem(t + 2 * i, nt), k, bank).wait_send()

    def relay_tokens(k):
        for j in range(1, G):
            yt_copy(j, k, True).wait_recv()
            spread_tokens(lax.rem(gi + G - j, G), k)

    def end_meta():
        return remote(meta.at[gi], meta.at[G], em_send, em_recv, {"dp": inward})

    def end_tokens(k):
        at = pl.ds(pl.multiple_of(t * quarter + k * sub, sub), sub)
        cols = pl.ds(pl.multiple_of(far_of_end, 128), far)
        return remote(
            x_all.at[gi, at, cols], token_piece(gi, t, k, 1), et_send.at[k], et_recv.at[k], {"dp": inward}
        )

    def end_down():
        return remote(x_all.at[gi, :, wide], x_down, eu_send, eu_recv, {"dp": inward})

    def ey_copy(j, k, arriving):
        peer = lax.rem(gi + G - j, G) if arriving else lax.rem(gi + j, G)
        ref = token_piece(peer if arriving else gi, t, k, 1)
        return remote(ref, ref, ey_send.at[j, k], ey_recv.at[j, k], {"groups": peer})

    def px_copy(j, arriving):
        peer = lax.rem(t + nt - j, nt) if arriving else lax.rem(t + j, nt)
        ref = parts_extra.at[peer if arriving else t]
        return remote(ref, ref, px_send.at[j], px_recv.at[j], {"tensor": peer})

    def ue_copy():
        return remote(u_all.at[G], u_all.at[gi], ue_send, ue_recv, {"dp": outward})

    def pp_copy(item, r):
        i = item - 2
        return remote(
            p_send[item - 2].at[r], p_got[item - 2].at[r], pp_send.at[i, r], pp_recv.at[i, r], {"dp": outward}
        )

    tile = 256 if rows % 256 == 0 else 128

    def whole_product(item, r):
        @pl.loop(0, rows // tile)
        def _(i):
            span = pl.ds(pl.multiple_of(i * tile, tile), tile)
            accs[item][r, span, :] = jnp.dot(
                x_all[r, span, :], weights[item][...], preferred_element_type=jnp.float32
            )

    def far_sums(item, r):
        rows_far = pl.ds(pl.multiple_of(far_of_near, 128), far)

        @pl.loop(0, rows // tile)
        def _(i):
            span = pl.ds(pl.multiple_of(i * tile, tile), tile)
            p_send[item - 2][r, span, :] = jnp.dot(
                x_far[r, span, :], weights[item][rows_far, :], preferred_element_type=jnp.float32
            ).astype(jnp.bfloat16)

        pp_copy(item, r).start()

    def close_product(item, r):
        close = pl.ds(pl.multiple_of(close_of_end, 128), 2 * depth)

        @pl.loop(0, rows // tile)
        def _(i):
            span = pl.ds(pl.multiple_of(i * tile, tile), tile)
            accs[item][r, span, :] = jnp.dot(
                x_all[r, span, close], weights[item][close, :], preferred_element_type=jnp.float32
            )

    def close_products(item):
        if relief:

            @pl.when(end)
            def _():
                for r in range(G):
                    close_product(item, r)

    def add_far_sums(item, r):
        remote(
            p_got[item - 2].at[r], p_got[item - 2].at[r], pp_send.at[item - 2, r], pp_recv.at[item - 2, r],
            {"dp": inward},
        ).wait_recv()

        @pl.loop(0, rows // tile)
        def _(i):
            span = pl.ds(pl.multiple_of(i * tile, tile), tile)
            accs[item][r, span, :] += p_got[item - 2][r, span, :].astype(jnp.float32)

    def slice_product(item, s, first):
        k_span = pl.ds(pl.multiple_of(s * depth, 128), depth)

        @pl.loop(0, G * rows // tile)
        def _(i):
            r = lax.div(i, rows // tile)
            span = pl.ds(pl.multiple_of(lax.rem(i, rows // tile) * tile, tile), tile)
            new = jnp.dot(
                x_all[r, span, k_span],
                weights[item][k_span, :],
                preferred_element_type=jnp.float32,
            )
            if first:
                accs[item][r, span, :] = new
            else:
                accs[item][r, span, :] += new

    cosine, sine = cos_ref[...], sin_ref[...]
    dims = (REQUEST_ROWS, REQUEST_ROWS)
    query_at = lax.broadcasted_iota(jnp.int32, dims, 0)
    key_at = lax.broadcasted_iota(jnp.int32, dims, 1)

    def turn(item, sign):
        return item * cosine + pltpu.roll(item, HD // 2, 1) * (sign * sine)

    def spread(total, slot, value):
        slots = jnp.full((R, 128), slot, jnp.int32)[:, :1]

        def add(a):
            total[a] += jnp.where(slots == a, value, 0.0)

        if n <= 8:
            for a in range(n):
                add(a)
        else:
            pl.loop(0, n)(add)

    def attend(r, b, ci):
        span = pl.ds(pl.multiple_of(b * REQUEST_ROWS, REQUEST_ROWS), REQUEST_ROWS)
        slot = meta[r, b]
        scale = scale_of(meta[r, blocks + b])
        live = meta[r, 2 * blocks] - b * REQUEST_ROWS
        u_q, u_v = u_all[r, :R, span], u_all[r, R:, span]
        b_cols = b_all[slot, r, :, starts[ci] : starts[ci] + widths[ci]]
        b_v = b_all[slot, r, :, hq:]
        stores = []
        heads_of = [slice(k * HD, (k + 1) * HD) for k in range(kv_heads)]
        if ci == 0:
            values = (acc_kv[r, span, hk:] + scale * dot(u_v, b_v, 0, 0)).astype(jnp.bfloat16)
            keys = [turn(acc_kv[r, span, kc], 1.0).astype(jnp.bfloat16) for kc in heads_of]
            keys = jnp.concatenate(keys, axis=1)
            yield

            def store_kv():
                keys_all[r, span, :] = keys
                values_all[r, span, :] = values

            if last:
                stores.append(store_kv)
            gv = [jnp.zeros((REQUEST_ROWS, HD), jnp.float32) for _ in heads_of]
            back = 0.0
        else:
            keys, values = keys_all[r, span, :], values_all[r, span, :]
            gv = [gv_acc[r, span, kc] for kc in heads_of]
            back = back_acc[r, :R, span]
        added = dot(u_q, b_cols, 0, 0)
        yield
        full = acc_q[ci][r, span, :] + scale * added
        live_rows = lax.broadcasted_iota(jnp.int32, (REQUEST_ROWS, HD), 0) < live
        allowed = (key_at <= query_at) & ((key_at < live) | (key_at == query_at))
        allowed = allowed.astype(jnp.float32)
        pieces = []
        first = starts[ci] // HD
        for k in range(kv_heads):
            heads = [i for i in range(widths[ci] // HD) if (first + i) // group == k]
            if not heads:
                continue
            head_keys, head_values = keys[:, heads_of[k]], values[:, heads_of[k]]
            queries = jnp.concatenate(
                [turn(full[:, i * HD : (i + 1) * HD], 1.0).astype(jnp.bfloat16) for i in heads],
                axis=0,
            )
            douts = []
            for i in heads:
                rows_in = d_all[r, span, (first + i) * HD : (first + i + 1) * HD]
                kept = jnp.where(live_rows, rows_in.astype(jnp.float32), 0.0)
                douts.append(kept.astype(jnp.bfloat16))
            dout = jnp.concatenate(douts, axis=0)
            yield
            scores = dot(queries, head_keys, 1, 1)
            dprobs = dot(dout, head_values, 1, 1)
            yield
            mask = jnp.concatenate([allowed] * len(heads), axis=0) > 0.5
            scores = jnp.where(mask, scores * HD ** (-0.5), -1e30)
            top = jnp.max(scores, axis=-1, keepdims=True)
            yield
            expo = jnp.exp(scores - top)
            total = jnp.sum(expo, axis=-1, keepdims=True)
            yield
            probs = expo / total
            mean = jnp.sum(dprobs * probs, axis=-1, keepdims=True)
            yield
            dscores = (probs * (dprobs - mean)).astype(jnp.bfloat16)
            dquery = dot(dscores, head_keys, 1, 0)
            gv[k] = gv[k] + dot(probs.astype(jnp.bfloat16), dout, 0, 0)
            yield
            dquery = dquery * HD ** (-0.5)
            for i in range(len(heads)):
                piece = dquery[i * REQUEST_ROWS : (i + 1) * REQUEST_ROWS]
                pieces.append(turn(piece, -1.0).astype(jnp.bfloat16))
            yield
        gq = jnp.concatenate(pieces, axis=1)
        up = dot(u_q, gq, 1, 0)
        back_new = dot(b_cols, gq, 1, 1)
        gv = jnp.concatenate(gv, axis=1)
        if ci == last:
            gv = gv.astype(jnp.bfloat16)
            up_v = dot(u_v, gv, 1, 0)
            back_v = dot(b_v, gv, 1, 1)
        yield
        up = scale * up
        back = back + scale * back_new
        if ci == last:
            up_v, back_v = scale * up_v, scale * back_v

        def store():
            back_acc[r, :R, span] = back
            spread(upq_sum[ci].at[r], slot, up)
            if ci == last:
                back_acc[r, R:, span] = back_v
                spread(upv_sum.at[r], slot, up_v)
            else:
                gv_acc[r, span, :] = gv

        yield stores + [store]

    together = 4 if blocks % 4 == 0 else 1

    def attend_chunk(ci):
        @pl.loop(0, G)
        def _(e):
            r = lax.rem(gi + e, G)
            if relief:

                @pl.when(end)
                def _():
                    add_far_sums(2 + ci, r)

            if ci == 0:

                @pl.when(e == 1)
                def _():
                    for j in range(1, G):
                        yu_copy(j, True).wait_recv()

            @pl.loop(0, blocks // together)
            def _(i):
                running = [attend(r, i * together + j, ci) for j in range(together)]
                for step in zip(*running):
                    for store in [store for stores in step for store in stores or ()]:
                        store()

    def part_copy(j, arriving):
        peer = lax.rem(t + nt - j, nt) if arriving else lax.rem(t + j, nt)
        ref = parts.at[peer if arriving else t]
        return remote(ref, ref, part_send.at[j], part_recv.at[j], {"tensor": peer})

    def down_product(r, x_ref, into):
        for b in range(blocks):
            span = slice(b * REQUEST_ROWS, (b + 1) * REQUEST_ROWS)
            into[t, :, span] = dot(down_all[meta[r, b]], x_ref[span, :], 1, 1)

    def down_sum(r, terms):
        for b in range(blocks):
            span = slice(b * REQUEST_ROWS, (b + 1) * REQUEST_ROWS)
            total = terms[0, :, span]
            for j in range(1, nt):
                total = total + terms[j, :, span]
            kept = jnp.where(row_at < meta[r, blocks + b], total, 0.0)
            u_all[r, :, span] = kept.astype(jnp.bfloat16)

    def down_parts():
        @pl.when(~end)
        def _():
            down_product(gi, x_all.at[gi, :, wide], parts)
            for j in range(1, nt):
                part_copy(j, False).start()

    row_at = lax.broadcasted_iota(jnp.int32, (2 * R, REQUEST_ROWS), 0)
    row_at = jnp.where(row_at >= R, row_at - R, row_at)

    def yu_copy(j, arriving):
        peer = lax.rem(gi + G - j, G) if arriving else lax.rem(gi + j, G)
        ref = u_all.at[peer if arriving else gi]
        return remote(ref, ref, yu_send.at[j], yu_recv.at[j], {"groups": peer})

    def finish_down():
        @pl.when(~end)
        def _():
            for j in range(1, nt):
                part_copy(j, True).wait_recv()
            down_sum(gi, parts)

        if relief:

            @pl.when(end)
            def _():
                ue_copy().wait_recv()

        for j in range(1, G):
            yu_copy(j, False).start()

    def up_copy(ci, e, a):
        there = lax.rem(gi + e, G)
        src = upv_send.at[there, a] if ci > last else upq_send[ci].at[there, a]
        dst = upv_got.at[me, gi] if ci > last else upq_got[ci].at[me, gi]
        return remote(
            src, dst, us_send.at[ci, e, a], us_recv.at[ci, me, gi], at_group(there, dp=a)
        )

    def up_arrival(ci, e, s):
        there = lax.rem(gi + e, G)
        dst = upv_got.at[s, there] if ci > last else upq_got[ci].at[s, there]
        return remote(dst, dst, us_send.at[ci, e, s], us_recv.at[ci, s, there], at_group(there, dp=s))

    def others(body):
        @pl.loop(0, n)
        def _(a):
            for e in range(G):
                if e == 0:

                    @pl.when(a != me)
                    def _():
                        body(e, a)

                else:
                    body(e, a)

    def send_ups(ci):
        if ci > last:
            upv_send[...] = upv_sum[...].astype(jnp.bfloat16)
            upv_got[me, gi] = upv_send[gi, me]
        else:
            upq_send[ci][...] = upq_sum[ci][...].astype(jnp.bfloat16)
            upq_got[ci][me, gi] = upq_send[ci][gi, me]
        others(lambda e, a: up_copy(ci, e, a).start())

    with jax.named_scope("start"):
        own_w = (loads[0], loads[1])
        for copy in own_w:
            copy.wait()
        send_own(0)
        for j in range(1, G):
            for copy in y_copies(j, False)[:3]:
                copy.start()
        if relief:

            @pl.when(end)
            def _():
                end_meta().start()

        loads[6].wait()
        for j in range(1, G):
            for k in range(TOKEN_SUBS):
                yt_copy(j, k, False).start()
            y_copies(j, False)[3].start()
        for copy in loads[2:6]:
            copy.wait()
        send_own(FACTORS, (0,))
        for j in range(1, G):
            for copy in y_copies(j, True)[:3]:
                copy.wait_recv()
        send_own(FACTORS, (1,))
        for copy in loads[8:]:
            copy.wait()
        if relief:

            @pl.when(end)
            def _():
                for k in range(TOKEN_SUBS):
                    end_tokens(k).start()

        if relief:

            @pl.when(end)
            def _():
                send_own(2)
                send_own(3)
                end_down().start()
                send_own(4)

        for ref in upq_sum:
            ref[...] = jnp.zeros_like(ref)
        upv_sum[...] = jnp.zeros_like(upv_sum)
        loads[7].wait()
    other_planes = [lax.rem(gi + j, G) for j in range(1, G)]
    inward_only = False if relief else None

    def next_own(item, to_end):
        @pl.when(~end)
        def _():
            send_own(item, to_end=to_end)

    def after_first():
        next_own(2, None)
        relay_tokens(0)

    with jax.named_scope("line0"):
        relays = [((2, 1), functools.partial(relay_tokens, k)) for k in range(1, TOKEN_SUBS)]
        line(0, hooks=[((1, None), after_first)] + relays)
    if relief:
        with jax.named_scope("relay_extra"):

            @pl.when(near)
            def _():
                remote(meta.at[G], meta.at[G], em_send, em_recv, {"dp": outward}).wait_recv()
                for k in range(TOKEN_SUBS):
                    et = token_piece(gi, t, k, 1)
                    remote(et, et, et_send.at[k], et_recv.at[k], {"dp": outward}).wait_recv()
                    for j in range(1, G):
                        ey_copy(j, k, False).start()
                    spread_tokens(gi, k, 1)

    def pass_other():
        for r in other_planes:
            pass_tokens(r)

    with jax.named_scope("linef"):
        line(FACTORS, hooks=[((1, None), pass_other), ((n - 1, 1), down_parts)])
        if relief:

            @pl.when(near)
            def _():
                for item in range(3, 3 + last):
                    send_own(item, to_end=True)

    def extra_pass():
        if last:
            next_own(3, inward_only)
        if relief:
            forward_ends(3)
            next_own(4, inward_only)

            @pl.when(near)
            def _():
                pass_tokens(gi, 1)
                for j in range(1, G):
                    for k in range(TOKEN_SUBS):
                        ey_copy(j, k, True).wait_recv()
                        spread_tokens(lax.rem(gi + G - j, G), k, 1)

        whole_product(0, gi)

    def tokens_done():
        for r in other_planes:
            settle_tokens(r)
            whole_product(0, r)

        @pl.when(~end)
        def _():
            finish_down()

    with jax.named_scope("line2"):
        line(2, hooks=[((1, None), extra_pass), ((2, None), tokens_done)])

    if relief:
        with jax.named_scope("far_sums"):

            @pl.when(near)
            def _():
                settle_tokens(gi, 1)
                far_sums(2, gi)

    @pl.when(~end)
    def _():
        for ci in range(1, last + 1):
            slice_product(2 + ci, me, True)

    def before_attention():
        @pl.when(~end)
        def _():
            for e in range(G):
                whole_product(2, lax.rem(gi + e, G))

        for j in range(1, G):
            y_copies(j, True)[3].wait_recv()
        if relief:

            @pl.when(near)
            def _():
                for r in other_planes:
                    pass_tokens(r, 1)
                    settle_tokens(r, 1)
                    far_sums(2, r)

            @pl.when(end)
            def _():
                finish_down()

    def extra_down():
        remote(x_down, x_down, eu_send, eu_recv, {"dp": outward}).wait_recv()
        down_product(G, x_down, parts_extra)
        for j in range(1, nt):
            px_copy(j, False).start()

    def extra_down_sum():
        for j in range(1, nt):
            px_copy(j, True).wait_recv()
        down_sum(G, parts_extra)
        ue_copy().start()

    close_products(2)
    if not last:
        before_attention()
    for ci in range(1, last + 1):
        item = 2 + ci

        def products(d):
            if relief and d == n - 2:

                @pl.when(near)
                def _():
                    for e in range(G):
                        far_sums(item, lax.rem(gi + e, G))

            for way in (0, 1):
                s = me - d if way == 0 else me + d

                @pl.when(((s >= 0) if way == 0 else (s < n)) & ~end)
                def _():
                    slice_product(item, s, False)

        def between_distances():
            close_products(item)
            if ci < last and not relief:
                next_own(item + 1, inward_only)
            if ci == 1:
                before_attention()
            if relief and ci == 1:
                pl.when(near)(extra_down)
            with jax.named_scope("att"):
                attend_chunk(ci - 1)
            if relief and ci == 1:
                forward_ends(4)
                pl.when(near)(extra_down_sum)

        with jax.named_scope(f"line{item}"):
            line(item, after=products, hooks=[((1, None), between_distances)])

    with jax.named_scope("ups"):
        for ci in range(last):
            send_ups(ci)
    with jax.named_scope("tail_attend"):
        attend_chunk(last)

    with jax.named_scope("back"):
        for r in range(G):
            for q in range(nt):
                back_send[r, q] = back_acc[r, :, q * quarter : (q + 1) * quarter].astype(jnp.bfloat16)

    def back_copy(e, j, arriving):
        there = lax.rem(gi + e, G)
        peer = lax.rem(t + nt - j, nt) if arriving else lax.rem(t + j, nt)
        if arriving:
            dst = back_got.at[there, peer]
            return remote(
                dst, dst, bk_send.at[e, j], bk_recv.at[there, peer], at_group(there, tensor=peer)
            )
        return remote(
            back_send.at[there, peer],
            back_got.at[gi, t],
            bk_send.at[e, j],
            bk_recv.at[gi, t],
            at_group(there, tensor=peer),
        )

    def all_copy(j, arriving):
        peer = lax.rem(t + nt - j, nt) if arriving else lax.rem(t + j, nt)
        ref = back_all.at[peer if arriving else t]
        return remote(ref, ref, ba_send.at[j], ba_recv.at[j], {"tensor": peer})

    crossing = [(e, j) for e in range(G) for j in range(nt) if (e, j) != (0, 0)]
    with jax.named_scope("backx"):
        for e, j in crossing:
            back_copy(e, j, False).start()
        back_got[gi, t] = back_send[gi, t]
        for e, j in crossing:
            back_copy(e, j, True).wait_recv()
        total = jnp.zeros(back_got.shape[2:], jnp.float32)
        for r in range(G):
            for j in range(nt):
                total = total + back_got[r, j].astype(jnp.float32)
        back_all[t] = total.astype(jnp.bfloat16)
        for j in range(1, nt):
            all_copy(j, False).start()
        send_ups(last)
        send_ups(last + 1)
        for j in range(1, nt):
            all_copy(j, True).wait_recv()
    total = jnp.concatenate([back_all[q] for q in range(nt)], axis=1).astype(jnp.float32)
    kept = []
    for b in range(blocks):
        span = slice(b * REQUEST_ROWS, (b + 1) * REQUEST_ROWS)
        kept.append(jnp.where(row_at < meta[gi, blocks + b], total[:, span], 0.0))
    def low_copy(a):
        return remote(
            low_send.at[a], low_got.at[me], lo_send.at[a], lo_recv.at[me], {"dp": a}
        )

    stack = 4 if n % 4 == 0 else 1

    with jax.named_scope("low"):
        @pl.loop(0, n // stack)
        def _(q):
            chosen = jnp.concatenate(
                [
                    jnp.concatenate(
                        [
                            jnp.where(
                                jnp.full((2 * R, REQUEST_ROWS), meta[gi, b], jnp.int32) == q * stack + i,
                                kept[b],
                                0.0,
                            )
                            for b in range(blocks)
                        ],
                        axis=1,
                    )
                    for i in range(stack)
                ],
                axis=0,
            ).astype(jnp.bfloat16)
            low = jnp.dot(chosen, x_all[gi, :, wide], preferred_element_type=jnp.float32)
            for i in range(stack):
                a = q * stack + i
                low_send[a] = low[i * 2 * R : (i + 1) * 2 * R].astype(jnp.bfloat16)

                @pl.when(a != me)
                def _():
                    low_copy(a).start()

        low_got[me] = low_send[me]

    with jax.named_scope("upsum"):
        for ci in range(last + 2):
            others(lambda e, s: up_arrival(ci, e, s).wait_recv())
        at = 2 * width
        for e in range(G):
            for ci in range(last + 1):
                out = jnp.zeros((R, widths[ci]), jnp.float32)
                out = lax.fori_loop(
                    0, n, lambda s, v: v + upq_got[ci][s, e].astype(jnp.float32), out
                )
                out_ref[:, at + e * hq + starts[ci] : at + e * hq + starts[ci] + widths[ci]] = out
            out = jnp.zeros((R, hk), jnp.float32)
            out = lax.fori_loop(0, n, lambda s, v: v + upv_got[s, e].astype(jnp.float32), out)
            out_ref[:, at + qcols + e * hk : at + qcols + (e + 1) * hk] = out

    with jax.named_scope("lowx"):
        @pl.loop(0, n)
        def _(s):
            @pl.when(s != me)
            def _():
                remote(
                    low_got.at[s], low_got.at[s], lo_send.at[s], lo_recv.at[s], {"dp": s}
                ).wait_recv()

        for i in range(2):
            out = jnp.zeros((R, width), jnp.float32)
            out = lax.fori_loop(
                0, n, lambda s, v: v + low_got[s, i * R : (i + 1) * R, :].astype(jnp.float32), out
            )
            out_ref[:, i * width : (i + 1) * width] = out

        for item in range(3 + last):

            @pl.loop(0, n)
            def _(s):
                for p in pieces_of(item):

                    for own in (True, False):

                        @pl.when(((s == me) if own else (s < me)) & ups(item, p, own))
                        def _():
                            z_copy(item, s, p, 0).wait_send()

                        @pl.when(((s == me) if own else (s > me)) & downs(item, p, own))
                        def _():
                            z_copy(item, s, p, 1).wait_send()

        for j in range(1, G):
            for copy in y_copies(j, False):
                copy.wait_send()
            yu_copy(j, False).wait_send()
            for k in range(TOKEN_SUBS):
                yt_copy(j, k, False).wait_send()
        for r in other_planes:
            drain_tokens(r)
        if relief:

            @pl.when(end)
            def _():
                end_meta().wait_send()
                end_down().wait_send()
                for k in range(TOKEN_SUBS):
                    end_tokens(k).wait_send()

            @pl.when(near)
            def _():
                for j in range(1, G):
                    for k in range(TOKEN_SUBS):
                        ey_copy(j, k, False).wait_send()
                for e in range(G):
                    drain_tokens(e, 1)
                    for item in range(2, 3 + last):
                        pp_copy(item, e).wait_send()
                for j in range(1, nt):
                    px_copy(j, False).wait_send()
                ue_copy().wait_send()

        @pl.when(~end)
        def _():
            for j in range(1, nt):
                part_copy(j, False).wait_send()

        for e, j in crossing:
            back_copy(e, j, False).wait_send()
        for j in range(1, nt):
            all_copy(j, False).wait_send()
        for ci in range(last + 2):
            others(lambda e, a: up_copy(ci, e, a).wait_send())

        @pl.loop(0, n)
        def _(a):
            @pl.when(a != me)
            def _():
                low_copy(a).wait_send()


def layer(G, relief, x, wq, wk, wv, aq, av, bq, bv, d, blocks_of, slots, ranks, live):
    n, nt = lax.axis_size("dp"), lax.axis_size("tensor")
    rows = x.shape[0]
    depth, qcols = wq.shape
    kcols = wk.shape[1]
    width = aq.shape[1]
    hq, hk = qcols // G, kcols // G
    widths = [c * HD for c in query_chunks(hq // HD)]
    span = n * depth
    blocks = rows // REQUEST_ROWS
    far = (n - 2) * depth
    cosine, sine = rope_tables(REQUEST_ROWS, HD)
    cosine = np.concatenate([cosine, cosine], axis=-1)
    sine = np.concatenate([-sine, sine], axis=-1)
    smem = pl.BlockSpec(memory_space=pltpu.SMEM)
    vmem = pl.BlockSpec(memory_space=pltpu.VMEM)
    hbm = pl.BlockSpec(memory_space=pltpu.HBM)
    bf, f32 = jnp.bfloat16, jnp.float32
    V = pltpu.VMEM
    dma = pltpu.SemaphoreType.DMA

    def pairs_of(shape):
        return [dma(shape), dma(shape)]

    return pl.pallas_call(
        functools.partial(layer_kernel, G, relief),
        out_shape=(
            jax.ShapeDtypeStruct((R, 2 * width + qcols + kcols), f32)
        ),
        in_specs=[smem] * 4 + [hbm] * 9 + [vmem] * 2,
        out_specs=vmem,
        scratch_shapes=[
            V((G, rows, span), bf),
            V((span, 2 * hk), bf),
            [V((span, w), bf) for w in widths],
            V((n, 2 * R, width), bf),
            V((n, G, R, hq + hk), bf),
            V((G, rows, hq), bf),
            V((G, rows, 2 * hk), f32),
            [V((G, rows, w), f32) for w in widths],
            V((nt, 2 * R, rows), f32),
            V((G + 1, 2 * R, rows), bf),
            V((G, rows, hk), bf),
            V((G, rows, hk), bf),
            V((G, rows, hk), f32),
            V((G, 2 * R, rows), f32),
            [V((G, n, R, w), f32) for w in widths],
            V((G, n, R, hk), f32),
            [V((G, n, R, w), bf) for w in widths],
            V((G, n, R, hk), bf),
            [V((n, G, R, w), bf) for w in widths],
            V((n, G, R, hk), bf),
            V((G, nt, 2 * R, rows // nt), bf),
            V((G, nt, 2 * R, rows // nt), bf),
            V((nt, 2 * R, rows // nt), bf),
            V((n, 2 * R, width), bf),
            V((n, 2 * R, width), bf),
            pltpu.SMEM((G + 1, 128), jnp.int32),
            V((G, rows, far) if relief else (1, 16, 128), bf),
            V((rows, width) if relief else (16, 128), bf),
            V((nt, 2 * R, rows) if relief else (1, 8, 128), f32),
            [V((G, rows, w) if relief else (1, 16, 128), bf) for w in widths],
            [V((G, rows, w) if relief else (1, 16, 128), bf) for w in widths],
        ]
        + [dma((8 + len(widths),))]
        + [dma((2, 2 + len(widths), n, SUBS)), dma((2 + len(widths), n, SUBS))]
        + pairs_of((G, 4))
        + pairs_of((G, TOKEN_SUBS))
        + pairs_of((2 * G, max(1, nt // 2), TOKEN_SUBS))
        + pairs_of((2 * G, nt, TOKEN_SUBS))
        + pairs_of((nt,))
        + pairs_of((G,))
        + [dma((1 + len(widths), G, n)), dma((1 + len(widths), n, G))]
        + pairs_of((G, nt))
        + pairs_of((n,))
        + [dma, dma]
        + pairs_of((TOKEN_SUBS,))
        + pairs_of((G, TOKEN_SUBS))
        + [dma, dma]
        + pairs_of((nt,))
        + [dma, dma]
        + pairs_of((len(widths), G))
        + pairs_of((nt,)),
        compiler_params=pltpu.CompilerParams(
            collective_id=0, has_side_effects=True, vmem_limit_bytes=62 * 1024 * 1024
        ),
        name="layer",
    )(blocks_of, slots, ranks, live, x, wq, wk, wv, aq, av, bq, bv, d, cosine, sine)


def on_device(
    tokens,
    w_query,
    w_key,
    w_value,
    a_query,
    b_query,
    a_value,
    b_value,
    adapter_ranks,
    adapter_slot,
    block_adapter,
    live_tokens,
    d_heads,
):
    ng, nt = lax.axis_size("groups"), lax.axis_size("tensor")
    kv_heads = w_key.shape[1] // HD
    G = ng if nt % 2 == 0 and kv_heads % ng == 0 else 1
    chunks = len(query_chunks(w_query.shape[1] // G // HD))
    relief = G > 1 and lax.axis_size("dp") >= 4 and chunks == 3
    out = layer(
        G, relief, tokens, w_query, w_key, w_value, a_query[0].T, a_value[0].T, b_query[0], b_value[0],
        d_heads, block_adapter.reshape(-1), adapter_slot, adapter_ranks, live_tokens,
    )
    width, qcols = a_query.shape[1], b_query.shape[2]
    low_q, low_v = out[:, :width], out[:, width : 2 * width]
    up_q, up_v = out[:, 2 * width : 2 * width + qcols], out[:, 2 * width + qcols :]
    return low_q.T[None], up_q[None], low_v.T[None], up_v[None]


def solution(mesh):
    in_specs = (
        P(("groups", "dp"), None),
        P("dp", "tensor"),
        P("dp", "tensor"),
        P("dp", "tensor"),
        P(("groups", "dp"), "tensor", None),
        P(("groups", "dp"), None, "tensor"),
        P(("groups", "dp"), "tensor", None),
        P(("groups", "dp"), None, "tensor"),
        P("groups"),
        P(),
        P(("groups", "dp"), None),
        P(("groups", "dp")),
        P(("groups", "dp"), "tensor"),
    )
    out_specs = (
        P(("groups", "dp"), "tensor", None),
        P(("groups", "dp"), None, "tensor"),
        P(("groups", "dp"), "tensor", None),
        P(("groups", "dp"), None, "tensor"),
    )
    return jax.shard_map(
        on_device, mesh=mesh, in_specs=in_specs, out_specs=out_specs, check_vma=False
    )
```

```python
import functools

import jax
import jax.numpy as jnp
import numpy as np
from jax import lax
from jax.experimental import pallas as pl
from jax.experimental.pallas import tpu as pltpu
from jax.sharding import PartitionSpec as P

HD = 128
R = 32
REQUEST_ROWS = 128
MESH = pl.DeviceIdType.MESH

adapter_alpha_factor = 32.0
rope_theta = 500000.0

SUBS = 2
TOKEN_SUBS = 2
FACTORS = 1


def rope_tables(length, width):
    halfway = width // 2
    spread = rope_theta ** (-2.0 * np.arange(halfway, dtype=np.float32) / width)
    angle = np.arange(length, dtype=np.float32)[:, None] * spread.astype(np.float32)[None, :]
    return np.cos(angle).astype(np.float32), np.sin(angle).astype(np.float32)


def scale_of(rank):
    return (adapter_alpha_factor / jnp.full((1, 128), rank, jnp.int32).astype(jnp.float32))[:, :1]


def query_chunks(heads):
    quarter = heads // 4
    return [heads - 2 * quarter, quarter, quarter] if quarter else [heads]


def dot(a, c, left, right):
    return lax.dot_general(
        a, c, (((left,), (right,)), ((), ())), preferred_element_type=jnp.float32
    )


def layer_kernel(
    G,
    relief,
    block_ref,
    slot_ref,
    rank_ref,
    live_ref,
    x_hbm,
    wq_hbm,
    wk_hbm,
    wv_hbm,
    aq_hbm,
    av_hbm,
    bq_hbm,
    bv_hbm,
    d_hbm,
    cos_ref,
    sin_ref,
    out_ref,
    x_all,
    w_kv,
    w_q,
    down_all,
    b_all,
    d_all,
    acc_kv,
    acc_q,
    parts,
    u_all,
    keys_all,
    values_all,
    gv_acc,
    back_acc,
    upq_sum,
    upv_sum,
    upq_send,
    upv_send,
    upq_got,
    upv_got,
    back_send,
    back_got,
    back_all,
    low_send,
    low_got,
    meta,
    x_far,
    x_down,
    parts_extra,
    p_send,
    p_got,
    local_sem,
    z_send,
    z_recv,
    yb_send,
    yb_recv,
    yt_send,
    yt_recv,
    tx_send,
    tx_recv,
    tp_send,
    tp_recv,
    part_send,
    part_recv,
    yu_send,
    yu_recv,
    us_send,
    us_recv,
    bk_send,
    bk_recv,
    lo_send,
    lo_recv,
    em_send,
    em_recv,
    et_send,
    et_recv,
    ey_send,
    ey_recv,
    eu_send,
    eu_recv,
    px_send,
    px_recv,
    ue_send,
    ue_recv,
    pp_send,
    pp_recv,
    ba_send,
    ba_recv,
):
    n = lax.axis_size("dp")
    ng = lax.axis_size("groups")
    nt = lax.axis_size("tensor")
    me = lax.axis_index("dp")
    g = lax.axis_index("groups")
    t = lax.axis_index("tensor")
    split = G > 1
    low_end, high_end = (1, n - 2) if relief else (0, n - 1)
    end = (me < low_end) | (me > high_end)
    near = ((me == 1) | (me == n - 2)) if relief else None
    inward = jnp.where(me == 0, 1, n - 2) if relief else None
    outward = jnp.where(me == 1, 0, n - 1) if relief else None
    gi = g if split else 0
    rows = x_hbm.shape[0]
    depth, qcols = wq_hbm.shape
    kcols = wk_hbm.shape[1]
    hq, hk = qcols // G, kcols // G
    kv_heads = hk // HD
    group = hq // hk
    blocks = rows // REQUEST_ROWS
    width = down_all.shape[2]
    step = depth // SUBS
    widths = [c * HD for c in query_chunks(hq // HD)]
    starts = [sum(widths[:i]) for i in range(len(widths))]
    last = len(widths) - 1
    weights = (w_kv, None) + tuple(w_q)
    wide = pl.ds(pl.multiple_of(t * width, 128), width)
    accs = (acc_kv, None) + tuple(acc_q)
    far = x_far.shape[2]
    far_of_near = jnp.where(me == 1, 2 * depth, 0)
    far_of_end = jnp.where(me == 0, 2 * depth, 0)
    close_of_end = jnp.where(me == 0, 0, far)

    def at_group(index, **rest):
        if split:
            rest["groups"] = index
        return rest

    def remote(src, dst, send, recv, to):
        return pltpu.make_async_remote_copy(
            src_ref=src, dst_ref=dst, send_sem=send, recv_sem=recv, device_id=to, device_id_type=MESH
        )

    mine = pl.ds(pl.multiple_of(me * depth, depth), depth)
    qs = pl.ds(pl.multiple_of(gi * hq, 128), hq)
    ks = pl.ds(pl.multiple_of(gi * hk, 128), hk)
    loads = [
        (wk_hbm.at[:, ks], w_kv.at[mine, pl.ds(0, hk)]),
        (wv_hbm.at[:, ks], w_kv.at[mine, pl.ds(hk, hk)]),
        (aq_hbm, down_all.at[me, pl.ds(0, R), :]),
        (av_hbm, down_all.at[me, pl.ds(R, R), :]),
        (bq_hbm.at[:, qs], b_all.at[me, gi, :, pl.ds(0, hq)]),
        (bv_hbm.at[:, ks], b_all.at[me, gi, :, pl.ds(hq, hk)]),
        (x_hbm, x_all.at[gi]),
        (d_hbm.at[:, qs], d_all.at[gi]),
    ] + [
        (wq_hbm.at[:, pl.ds(pl.multiple_of(gi * hq + c, 128), w)], ref.at[mine, :])
        for c, w, ref in zip(starts, widths, w_q)
    ]
    loads = [pltpu.make_async_copy(s, d, local_sem.at[i]) for i, (s, d) in enumerate(loads)]
    for copy in loads:
        copy.start()

    for b in range(blocks):
        adapter = block_ref[b]
        meta[gi, b] = slot_ref[adapter]
        meta[gi, blocks + b] = rank_ref[adapter]
    meta[gi, 2 * blocks] = live_ref[0]

    with jax.named_scope("greet"):
        barrier = pltpu.get_barrier_semaphore()

        @pl.loop(1, n * G)
        def _(j):
            k = lax.rem(me * G + gi + j, n * G)
            pl.semaphore_signal(
                barrier, inc=1, device_id=at_group(lax.rem(k, G), dp=lax.div(k, G)), device_id_type=MESH
            )

        for j in range(1, nt):
            for e in range(G):
                pl.semaphore_signal(
                    barrier,
                    inc=1,
                    device_id=at_group(lax.rem(gi + e, G), tensor=lax.rem(t + j, nt)),
                    device_id_type=MESH,
                )
        pl.semaphore_wait(barrier, n * G - 1 + G * (nt - 1))

    def z_copy(item, s, p, way):
        if item == FACTORS:
            ref = down_all.at[s] if p == 0 else b_all.at[s]
        else:
            ref = weights[item].at[pl.ds(pl.multiple_of(s * depth + p * step, step), step), :]
        target = jnp.clip(me + (1 if way == 0 else -1), 0, n - 1)
        return remote(
            ref, ref, z_send.at[way, item, s, p], z_recv.at[item, s, p], {"dp": target}
        )

    def pieces_of(item):
        return range(2) if item == FACTORS else range(SUBS)

    def stays_inside(item, p, own):
        if item == FACTORS:
            return p == 0
        return item > FACTORS and not own

    def ups(item, p, own):
        return me < (high_end if stays_inside(item, p, own) else n - 1)

    def downs(item, p, own):
        return me > (low_end if stays_inside(item, p, own) else 0)

    def send_own(item, pieces=None, to_end=None):
        up, down = (me < n, me >= 0) if to_end is None else (me == n - 2, me == 1)
        if to_end is False:
            up, down = ~up, ~down
        for p in pieces_of(item) if pieces is None else pieces:

            @pl.when(ups(item, p, True) & up)
            def _():
                z_copy(item, me, p, 0).start()

            @pl.when(downs(item, p, True) & down)
            def _():
                z_copy(item, me, p, 1).start()

    def forward_piece(item, d, p, static_p):
        for way in (0, 1):
            s = me - d if way == 0 else me + d
            valid = (s >= 0) if way == 0 else (s < n)
            if relief and stays_inside(item, static_p, False):
                valid = valid & (~end if item == FACTORS else ~end | (d == 1))
            onward = ups(item, static_p, False) if way == 0 else downs(item, static_p, False)
            if relief and item > 2:
                valid = valid & ~(near & (d == 1) & ((s == 0) | (s == n - 1)))

            @pl.when(valid)
            def _():
                z_copy(item, s, p, way).wait_recv()

                @pl.when(onward)
                def _():
                    z_copy(item, s, p, way).start()

    def forward_ends(item):
        for way, at in ((0, 1), (1, n - 2)):
            s = 0 if way == 0 else n - 1

            @pl.when(me == at)
            def _():
                for p in pieces_of(item):
                    z_copy(item, s, p, way).wait_recv()
                    z_copy(item, s, p, way).start()

    def line(item, after=None, hooks=()):
        hooks = dict(hooks)
        final = pieces_of(item)[-1]
        if n <= 8:
            for d in range(1, n):
                for p in pieces_of(item):
                    forward_piece(item, d, p, p)
                    if p == final and after is not None:
                        after(d)
                    for key in ((d, p), (d, None) if p == final else None):
                        if key in hooks:
                            hooks.pop(key)()
        else:

            @pl.loop(1, n)
            def _(d):
                for p in pieces_of(item):
                    forward_piece(item, d, p, p)
                if after is not None:
                    after(d)

        for hook in hooks.values():
            hook()

    def y_copies(j, arriving):
        peer = lax.rem(gi + G - j, G) if arriving else lax.rem(gi + j, G)
        at = peer if arriving else gi
        to = {"groups": peer}
        pq = pl.ds(pl.multiple_of(peer * hq, 128), hq)
        pk = pl.ds(pl.multiple_of(peer * hk, 128), hk)
        sources = (
            (bq_hbm.at[:, pq], b_all.at[me, at, :, pl.ds(0, hq)]),
            (bv_hbm.at[:, pk], b_all.at[me, at, :, pl.ds(hq, hk)]),
            (meta.at[at], meta.at[at]),
            (d_hbm.at[:, pq], d_all.at[at]),
        )
        return [
            remote(s, d, yb_send.at[j, i], yb_recv.at[j, i], to) for i, (s, d) in enumerate(sources)
        ]

    quarter = rows // nt
    sub = quarter // TOKEN_SUBS

    def token_piece(r, q, k, bank=0):
        ref = x_far if bank else x_all
        return ref.at[r, pl.ds(pl.multiple_of(q * quarter + k * sub, sub), sub), :]

    def yt_copy(j, k, arriving):
        peer = lax.rem(gi + G - j, G) if arriving else lax.rem(gi + j, G)
        ref = token_piece(peer if arriving else gi, t, k)
        return remote(ref, ref, yt_send.at[j, k], yt_recv.at[j, k], {"groups": peer})

    pairs = nt // 2
    partner = t + 1 - 2 * lax.rem(t, 2)

    def tx_copy(r, i, k, arriving, bank=0):
        peer = lax.rem(t + nt - 2 * i, nt) if arriving else lax.rem(t + 2 * i, nt)
        ref = token_piece(r, peer if arriving else t, k, bank)
        return remote(
            ref, ref, tx_send.at[bank * G + r, i, k], tx_recv.at[bank * G + r, i, k], {"tensor": peer}
        )

    def tp_copy(r, q, k, bank=0):
        ref = token_piece(r, q, k, bank)
        return remote(
            ref, ref, tp_send.at[bank * G + r, q, k], tp_recv.at[bank * G + r, q, k], {"tensor": partner}
        )

    def spread_tokens(r, k, bank=0):
        for i in range(1, pairs):
            tx_copy(r, i, k, False, bank).start()
        tp_copy(r, t, k, bank).start()

    def pass_tokens(r, bank=0):
        for k in range(TOKEN_SUBS):
            for i in range(1, pairs):
                tx_copy(r, i, k, True, bank).wait_recv()
                tp_copy(r, lax.rem(t + nt - 2 * i, nt), k, bank).start()

    def settle_tokens(r, bank=0):
        for k in range(TOKEN_SUBS):
            for i in range(pairs):
                tp_copy(r, lax.rem(partner + 2 * i, nt), k, bank).wait_recv()

    def drain_tokens(r, bank=0):
        for k in range(TOKEN_SUBS):
            for i in range(1, pairs):
                tx_copy(r, i, k, False, bank).wait_send()
            for i in range(pairs):
                tp_copy(r, lax.rem(t + 2 * i, nt), k, bank).wait_send()

    def relay_tokens(k):
        for j in range(1, G):
            yt_copy(j, k, True).wait_recv()
            spread_tokens(lax.rem(gi + G - j, G), k)

    def end_meta():
        return remote(meta.at[gi], meta.at[G], em_send, em_recv, {"dp": inward})

    def end_tokens(k):
        at = pl.ds(pl.multiple_of(t * quarter + k * sub, sub), sub)
        cols = pl.ds(pl.multiple_of(far_of_end, 128), far)
        return remote(
            x_all.at[gi, at, cols], token_piece(gi, t, k, 1), et_send.at[k], et_recv.at[k], {"dp": inward}
        )

    def end_down():
        return remote(x_all.at[gi, :, wide], x_down, eu_send, eu_recv, {"dp": inward})

    def ey_copy(j, k, arriving):
        peer = lax.rem(gi + G - j, G) if arriving else lax.rem(gi + j, G)
        ref = token_piece(peer if arriving else gi, t, k, 1)
        return remote(ref, ref, ey_send.at[j, k], ey_recv.at[j, k], {"groups": peer})

    def px_copy(j, arriving):
        peer = lax.rem(t + nt - j, nt) if arriving else lax.rem(t + j, nt)
        ref = parts_extra.at[peer if arriving else t]
        return remote(ref, ref, px_send.at[j], px_recv.at[j], {"tensor": peer})

    def ue_copy():
        return remote(u_all.at[G], u_all.at[gi], ue_send, ue_recv, {"dp": outward})

    def pp_copy(item, r):
        i = item - 2
        return remote(
            p_send[item - 2].at[r], p_got[item - 2].at[r], pp_send.at[i, r], pp_recv.at[i, r], {"dp": outward}
        )

    tile = 256 if rows % 256 == 0 else 128

    def whole_product(item, r):
        @pl.loop(0, rows // tile)
        def _(i):
            span = pl.ds(pl.multiple_of(i * tile, tile), tile)
            accs[item][r, span, :] = jnp.dot(
                x_all[r, span, :], weights[item][...], preferred_element_type=jnp.float32
            )

    def far_sums(item, r):
        rows_far = pl.ds(pl.multiple_of(far_of_near, 128), far)

        @pl.loop(0, rows // tile)
        def _(i):
            span = pl.ds(pl.multiple_of(i * tile, tile), tile)
            p_send[item - 2][r, span, :] = jnp.dot(
                x_far[r, span, :], weights[item][rows_far, :], preferred_element_type=jnp.float32
            ).astype(jnp.bfloat16)

        pp_copy(item, r).start()

    def close_product(item, r):
        close = pl.ds(pl.multiple_of(close_of_end, 128), 2 * depth)

        @pl.loop(0, rows // tile)
        def _(i):
            span = pl.ds(pl.multiple_of(i * tile, tile), tile)
            accs[item][r, span, :] = jnp.dot(
                x_all[r, span, close], weights[item][close, :], preferred_element_type=jnp.float32
            )

    def close_products(item):
        if relief:

            @pl.when(end)
            def _():
                for r in range(G):
                    close_product(item, r)

    def add_far_sums(item, r):
        remote(
            p_got[item - 2].at[r], p_got[item - 2].at[r], pp_send.at[item - 2, r], pp_recv.at[item - 2, r],
            {"dp": inward},
        ).wait_recv()

        @pl.loop(0, rows // tile)
        def _(i):
            span = pl.ds(pl.multiple_of(i * tile, tile), tile)
            accs[item][r, span, :] += p_got[item - 2][r, span, :].astype(jnp.float32)

    def slice_product(item, s, first):
        k_span = pl.ds(pl.multiple_of(s * depth, 128), depth)

        @pl.loop(0, G * rows // tile)
        def _(i):
            r = lax.div(i, rows // tile)
            span = pl.ds(pl.multiple_of(lax.rem(i, rows // tile) * tile, tile), tile)
            new = jnp.dot(
                x_all[r, span, k_span],
                weights[item][k_span, :],
                preferred_element_type=jnp.float32,
            )
            if first:
                accs[item][r, span, :] = new
            else:
                accs[item][r, span, :] += new

    cosine, sine = cos_ref[...], sin_ref[...]
    dims = (REQUEST_ROWS, REQUEST_ROWS)
    query_at = lax.broadcasted_iota(jnp.int32, dims, 0)
    key_at = lax.broadcasted_iota(jnp.int32, dims, 1)

    def turn(item, sign):
        return item * cosine + pltpu.roll(item, HD // 2, 1) * (sign * sine)

    def spread(total, slot, value):
        slots = jnp.full((R, 128), slot, jnp.int32)[:, :1]

        def add(a):
            total[a] += jnp.where(slots == a, value, 0.0)

        if n <= 8:
            for a in range(n):
                add(a)
        else:
            pl.loop(0, n)(add)

    def attend(r, b, ci):
        span = pl.ds(pl.multiple_of(b * REQUEST_ROWS, REQUEST_ROWS), REQUEST_ROWS)
        slot = meta[r, b]
        scale = scale_of(meta[r, blocks + b])
        live = meta[r, 2 * blocks] - b * REQUEST_ROWS
        u_q, u_v = u_all[r, :R, span], u_all[r, R:, span]
        b_cols = b_all[slot, r, :, starts[ci] : starts[ci] + widths[ci]]
        b_v = b_all[slot, r, :, hq:]
        stores = []
        heads_of = [slice(k * HD, (k + 1) * HD) for k in range(kv_heads)]
        if ci == 0:
            values = (acc_kv[r, span, hk:] + scale * dot(u_v, b_v, 0, 0)).astype(jnp.bfloat16)
            keys = [turn(acc_kv[r, span, kc], 1.0).astype(jnp.bfloat16) for kc in heads_of]
            keys = jnp.concatenate(keys, axis=1)
            yield

            def store_kv():
                keys_all[r, span, :] = keys
                values_all[r, span, :] = values

            if last:
                stores.append(store_kv)
            gv = [jnp.zeros((REQUEST_ROWS, HD), jnp.float32) for _ in heads_of]
            back = 0.0
        else:
            keys, values = keys_all[r, span, :], values_all[r, span, :]
            gv = [gv_acc[r, span, kc] for kc in heads_of]
            back = back_acc[r, :R, span]
        added = dot(u_q, b_cols, 0, 0)
        yield
        full = acc_q[ci][r, span, :] + scale * added
        live_rows = lax.broadcasted_iota(jnp.int32, (REQUEST_ROWS, HD), 0) < live
        allowed = (key_at <= query_at) & ((key_at < live) | (key_at == query_at))
        allowed = allowed.astype(jnp.float32)
        pieces = []
        first = starts[ci] // HD
        for k in range(kv_heads):
            heads = [i for i in range(widths[ci] // HD) if (first + i) // group == k]
            if not heads:
                continue
            head_keys, head_values = keys[:, heads_of[k]], values[:, heads_of[k]]
            queries = jnp.concatenate(
                [turn(full[:, i * HD : (i + 1) * HD], 1.0).astype(jnp.bfloat16) for i in heads],
                axis=0,
            )
            douts = []
            for i in heads:
                rows_in = d_all[r, span, (first + i) * HD : (first + i + 1) * HD]
                kept = jnp.where(live_rows, rows_in.astype(jnp.float32), 0.0)
                douts.append(kept.astype(jnp.bfloat16))
            dout = jnp.concatenate(douts, axis=0)
            yield
            scores = dot(queries, head_keys, 1, 1)
            dprobs = dot(dout, head_values, 1, 1)
            yield
            mask = jnp.concatenate([allowed] * len(heads), axis=0) > 0.5
            scores = jnp.where(mask, scores * HD ** (-0.5), -1e30)
            top = jnp.max(scores, axis=-1, keepdims=True)
            yield
            expo = jnp.exp(scores - top)
            total = jnp.sum(expo, axis=-1, keepdims=True)
            yield
            probs = expo / total
            mean = jnp.sum(dprobs * probs, axis=-1, keepdims=True)
            yield
            dscores = (probs * (dprobs - mean)).astype(jnp.bfloat16)
            dquery = dot(dscores, head_keys, 1, 0)
            gv[k] = gv[k] + dot(probs.astype(jnp.bfloat16), dout, 0, 0)
            yield
            dquery = dquery * HD ** (-0.5)
            for i in range(len(heads)):
                piece = dquery[i * REQUEST_ROWS : (i + 1) * REQUEST_ROWS]
                pieces.append(turn(piece, -1.0).astype(jnp.bfloat16))
            yield
        gq = jnp.concatenate(pieces, axis=1)
        up = dot(u_q, gq, 1, 0)
        back_new = dot(b_cols, gq, 1, 1)
        gv = jnp.concatenate(gv, axis=1)
        if ci == last:
            gv = gv.astype(jnp.bfloat16)
            up_v = dot(u_v, gv, 1, 0)
            back_v = dot(b_v, gv, 1, 1)
        yield
        up = scale * up
        back = back + scale * back_new
        if ci == last:
            up_v, back_v = scale * up_v, scale * back_v

        def store():
            back_acc[r, :R, span] = back
            spread(upq_sum[ci].at[r], slot, up)
            if ci == last:
                back_acc[r, R:, span] = back_v
                spread(upv_sum.at[r], slot, up_v)
            else:
                gv_acc[r, span, :] = gv

        yield stores + [store]

    together = 4 if blocks % 4 == 0 else 1

    def attend_chunk(ci):
        @pl.loop(0, G)
        def _(e):
            r = lax.rem(gi + e, G)
            if relief:

                @pl.when(end)
                def _():
                    add_far_sums(2 + ci, r)

            if ci == 0:

                @pl.when(e == 1)
                def _():
                    for j in range(1, G):
                        yu_copy(j, True).wait_recv()

            @pl.loop(0, blocks // together)
            def _(i):
                running = [attend(r, i * together + j, ci) for j in range(together)]
                for step in zip(*running):
                    for store in [store for stores in step for store in stores or ()]:
                        store()

    def part_copy(j, arriving):
        peer = lax.rem(t + nt - j, nt) if arriving else lax.rem(t + j, nt)
        ref = parts.at[peer if arriving else t]
        return remote(ref, ref, part_send.at[j], part_recv.at[j], {"tensor": peer})

    def down_product(r, x_ref, into):
        for b in range(blocks):
            span = slice(b * REQUEST_ROWS, (b + 1) * REQUEST_ROWS)
            into[t, :, span] = dot(down_all[meta[r, b]], x_ref[span, :], 1, 1)

    def down_sum(r, terms):
        for b in range(blocks):
            span = slice(b * REQUEST_ROWS, (b + 1) * REQUEST_ROWS)
            total = terms[0, :, span]
            for j in range(1, nt):
                total = total + terms[j, :, span]
            kept = jnp.where(row_at < meta[r, blocks + b], total, 0.0)
            u_all[r, :, span] = kept.astype(jnp.bfloat16)

    def down_parts():
        @pl.when(~end)
        def _():
            down_product(gi, x_all.at[gi, :, wide], parts)
            for j in range(1, nt):
                part_copy(j, False).start()

    row_at = lax.broadcasted_iota(jnp.int32, (2 * R, REQUEST_ROWS), 0)
    row_at = jnp.where(row_at >= R, row_at - R, row_at)

    def yu_copy(j, arriving):
        peer = lax.rem(gi + G - j, G) if arriving else lax.rem(gi + j, G)
        ref = u_all.at[peer if arriving else gi]
        return remote(ref, ref, yu_send.at[j], yu_recv.at[j], {"groups": peer})

    def finish_down():
        @pl.when(~end)
        def _():
            for j in range(1, nt):
                part_copy(j, True).wait_recv()
            down_sum(gi, parts)

        if relief:

            @pl.when(end)
            def _():
                ue_copy().wait_recv()

        for j in range(1, G):
            yu_copy(j, False).start()

    def up_copy(ci, e, a):
        there = lax.rem(gi + e, G)
        src = upv_send.at[there, a] if ci > last else upq_send[ci].at[there, a]
        dst = upv_got.at[me, gi] if ci > last else upq_got[ci].at[me, gi]
        return remote(
            src, dst, us_send.at[ci, e, a], us_recv.at[ci, me, gi], at_group(there, dp=a)
        )

    def up_arrival(ci, e, s):
        there = lax.rem(gi + e, G)
        dst = upv_got.at[s, there] if ci > last else upq_got[ci].at[s, there]
        return remote(dst, dst, us_send.at[ci, e, s], us_recv.at[ci, s, there], at_group(there, dp=s))

    def others(body):
        @pl.loop(0, n)
        def _(a):
            for e in range(G):
                if e == 0:

                    @pl.when(a != me)
                    def _():
                        body(e, a)

                else:
                    body(e, a)

    def send_ups(ci):
        if ci > last:
            upv_send[...] = upv_sum[...].astype(jnp.bfloat16)
            upv_got[me, gi] = upv_send[gi, me]
        else:
            upq_send[ci][...] = upq_sum[ci][...].astype(jnp.bfloat16)
            upq_got[ci][me, gi] = upq_send[ci][gi, me]
        others(lambda e, a: up_copy(ci, e, a).start())

    with jax.named_scope("start"):
        own_w = (loads[0], loads[1])
        for copy in own_w:
            copy.wait()
        send_own(0)
        for j in range(1, G):
            for copy in y_copies(j, False)[:3]:
                copy.start()
        if relief:

            @pl.when(end)
            def _():
                end_meta().start()

        loads[6].wait()
        for j in range(1, G):
            for k in range(TOKEN_SUBS):
                yt_copy(j, k, False).start()
            y_copies(j, False)[3].start()
        for copy in loads[2:6]:
            copy.wait()
        send_own(FACTORS, (0,))
        for j in range(1, G):
            for copy in y_copies(j, True)[:3]:
                copy.wait_recv()
        send_own(FACTORS, (1,))
        for copy in loads[8:]:
            copy.wait()
        if relief:

            @pl.when(end)
            def _():
                for k in range(TOKEN_SUBS):
                    end_tokens(k).start()

        if relief:

            @pl.when(end)
            def _():
                send_own(2)
                send_own(3)
                end_down().start()
                send_own(4)

        for ref in upq_sum:
            ref[...] = jnp.zeros_like(ref)
        upv_sum[...] = jnp.zeros_like(upv_sum)
        loads[7].wait()
    other_planes = [lax.rem(gi + j, G) for j in range(1, G)]
    inward_only = False if relief else None

    def next_own(item, to_end):
        @pl.when(~end)
        def _():
            send_own(item, to_end=to_end)

    def after_first():
        next_own(2, None)
        relay_tokens(0)

    with jax.named_scope("line0"):
        relays = [((2, 1), functools.partial(relay_tokens, k)) for k in range(1, TOKEN_SUBS)]
        line(0, hooks=[((1, None), after_first)] + relays)
    if relief:
        with jax.named_scope("relay_extra"):

            @pl.when(near)
            def _():
                remote(meta.at[G], meta.at[G], em_send, em_recv, {"dp": outward}).wait_recv()
                for k in range(TOKEN_SUBS):
                    et = token_piece(gi, t, k, 1)
                    remote(et, et, et_send.at[k], et_recv.at[k], {"dp": outward}).wait_recv()
                    for j in range(1, G):
                        ey_copy(j, k, False).start()
                    spread_tokens(gi, k, 1)

    def pass_other():
        for r in other_planes:
            pass_tokens(r)

    with jax.named_scope("linef"):
        line(FACTORS, hooks=[((1, None), pass_other), ((n - 1, 1), down_parts)])
        if relief:

            @pl.when(near)
            def _():
                for item in range(3, 3 + last):
                    send_own(item, to_end=True)

    def extra_pass():
        if last:
            next_own(3, inward_only)
        if relief:
            forward_ends(3)
            next_own(4, inward_only)

            @pl.when(near)
            def _():
                pass_tokens(gi, 1)
                for j in range(1, G):
                    for k in range(TOKEN_SUBS):
                        ey_copy(j, k, True).wait_recv()
                        spread_tokens(lax.rem(gi + G - j, G), k, 1)

        whole_product(0, gi)

    def tokens_done():
        for r in other_planes:
            settle_tokens(r)
            whole_product(0, r)

        @pl.when(~end)
        def _():
            finish_down()

    with jax.named_scope("line2"):
        line(2, hooks=[((1, None), extra_pass), ((2, None), tokens_done)])

    if relief:
        with jax.named_scope("far_sums"):

            @pl.when(near)
            def _():
                settle_tokens(gi, 1)
                far_sums(2, gi)

    @pl.when(~end)
    def _():
        for ci in range(1, last + 1):
            slice_product(2 + ci, me, True)

    def before_attention():
        @pl.when(~end)
        def _():
            for e in range(G):
                whole_product(2, lax.rem(gi + e, G))

        for j in range(1, G):
            y_copies(j, True)[3].wait_recv()
        if relief:

            @pl.when(near)
            def _():
                for r in other_planes:
                    pass_tokens(r, 1)
                    settle_tokens(r, 1)
                    far_sums(2, r)

            @pl.when(end)
            def _():
                finish_down()

    def extra_down():
        remote(x_down, x_down, eu_send, eu_recv, {"dp": outward}).wait_recv()
        down_product(G, x_down, parts_extra)
        for j in range(1, nt):
            px_copy(j, False).start()

    def extra_down_sum():
        for j in range(1, nt):
            px_copy(j, True).wait_recv()
        down_sum(G, parts_extra)
        ue_copy().start()

    close_products(2)
    if not last:
        before_attention()
    for ci in range(1, last + 1):
        item = 2 + ci

        def products(d):
            if relief and d == n - 2:

                @pl.when(near)
                def _():
                    for e in range(G):
                        far_sums(item, lax.rem(gi + e, G))

            for way in (0, 1):
                s = me - d if way == 0 else me + d

                @pl.when(((s >= 0) if way == 0 else (s < n)) & ~end)
                def _():
                    slice_product(item, s, False)

        def between_distances():
            close_products(item)
            if ci < last and not relief:
                next_own(item + 1, inward_only)
            if ci == 1:
                before_attention()
            if relief and ci == 1:
                pl.when(near)(extra_down)
            with jax.named_scope("att"):
                attend_chunk(ci - 1)
            if relief and ci == 1:
                forward_ends(4)
                pl.when(near)(extra_down_sum)

        with jax.named_scope(f"line{item}"):
            line(item, after=products, hooks=[((1, None), between_distances)])

    with jax.named_scope("ups"):
        for ci in range(last):
            send_ups(ci)
    with jax.named_scope("tail_attend"):
        attend_chunk(last)

    with jax.named_scope("back"):
        for r in range(G):
            for q in range(nt):
                back_send[r, q] = back_acc[r, :, q * quarter : (q + 1) * quarter].astype(jnp.bfloat16)

    def back_copy(e, j, arriving):
        there = lax.rem(gi + e, G)
        peer = lax.rem(t + nt - j, nt) if arriving else lax.rem(t + j, nt)
        if arriving:
            dst = back_got.at[there, peer]
            return remote(
                dst, dst, bk_send.at[e, j], bk_recv.at[there, peer], at_group(there, tensor=peer)
            )
        return remote(
            back_send.at[there, peer],
            back_got.at[gi, t],
            bk_send.at[e, j],
            bk_recv.at[gi, t],
            at_group(there, tensor=peer),
        )

    def all_copy(j, arriving):
        peer = lax.rem(t + nt - j, nt) if arriving else lax.rem(t + j, nt)
        ref = back_all.at[peer if arriving else t]
        return remote(ref, ref, ba_send.at[j], ba_recv.at[j], {"tensor": peer})

    crossing = [(e, j) for e in range(G) for j in range(nt) if (e, j) != (0, 0)]
    with jax.named_scope("backx"):
        for e, j in crossing:
            back_copy(e, j, False).start()
        back_got[gi, t] = back_send[gi, t]
        for e, j in crossing:
            back_copy(e, j, True).wait_recv()
        total = jnp.zeros(back_got.shape[2:], jnp.float32)
        for r in range(G):
            for j in range(nt):
                total = total + back_got[r, j].astype(jnp.float32)
        back_all[t] = total.astype(jnp.bfloat16)
        for j in range(1, nt):
            all_copy(j, False).start()
        send_ups(last)
        send_ups(last + 1)
        for j in range(1, nt):
            all_copy(j, True).wait_recv()
    total = jnp.concatenate([back_all[q] for q in range(nt)], axis=1).astype(jnp.float32)
    kept = []
    for b in range(blocks):
        span = slice(b * REQUEST_ROWS, (b + 1) * REQUEST_ROWS)
        kept.append(jnp.where(row_at < meta[gi, blocks + b], total[:, span], 0.0))
    def low_copy(a):
        return remote(
            low_send.at[a], low_got.at[me], lo_send.at[a], lo_recv.at[me], {"dp": a}
        )

    stack = 4 if n % 4 == 0 else 1

    with jax.named_scope("low"):
        @pl.loop(0, n // stack)
        def _(q):
            chosen = jnp.concatenate(
                [
                    jnp.concatenate(
                        [
                            jnp.where(
                                jnp.full((2 * R, REQUEST_ROWS), meta[gi, b], jnp.int32) == q * stack + i,
                                kept[b],
                                0.0,
                            )
                            for b in range(blocks)
                        ],
                        axis=1,
                    )
                    for i in range(stack)
                ],
                axis=0,
            ).astype(jnp.bfloat16)
            low = jnp.dot(chosen, x_all[gi, :, wide], preferred_element_type=jnp.float32)
            for i in range(stack):
                a = q * stack + i
                low_send[a] = low[i * 2 * R : (i + 1) * 2 * R].astype(jnp.bfloat16)

                @pl.when(a != me)
                def _():
                    low_copy(a).start()

        low_got[me] = low_send[me]

    with jax.named_scope("upsum"):
        for ci in range(last + 2):
            others(lambda e, s: up_arrival(ci, e, s).wait_recv())
        at = 2 * width
        for e in range(G):
            for ci in range(last + 1):
                out = jnp.zeros((R, widths[ci]), jnp.float32)
                out = lax.fori_loop(
                    0, n, lambda s, v: v + upq_got[ci][s, e].astype(jnp.float32), out
                )
                out_ref[:, at + e * hq + starts[ci] : at + e * hq + starts[ci] + widths[ci]] = out
            out = jnp.zeros((R, hk), jnp.float32)
            out = lax.fori_loop(0, n, lambda s, v: v + upv_got[s, e].astype(jnp.float32), out)
            out_ref[:, at + qcols + e * hk : at + qcols + (e + 1) * hk] = out

    with jax.named_scope("lowx"):
        @pl.loop(0, n)
        def _(s):
            @pl.when(s != me)
            def _():
                remote(
                    low_got.at[s], low_got.at[s], lo_send.at[s], lo_recv.at[s], {"dp": s}
                ).wait_recv()

        for i in range(2):
            out = jnp.zeros((R, width), jnp.float32)
            out = lax.fori_loop(
                0, n, lambda s, v: v + low_got[s, i * R : (i + 1) * R, :].astype(jnp.float32), out
            )
            out_ref[:, i * width : (i + 1) * width] = out

        for item in range(3 + last):

            @pl.loop(0, n)
            def _(s):
                for p in pieces_of(item):

                    for own in (True, False):

                        @pl.when(((s == me) if own else (s < me)) & ups(item, p, own))
                        def _():
                            z_copy(item, s, p, 0).wait_send()

                        @pl.when(((s == me) if own else (s > me)) & downs(item, p, own))
                        def _():
                            z_copy(item, s, p, 1).wait_send()

        for j in range(1, G):
            for copy in y_copies(j, False):
                copy.wait_send()
            yu_copy(j, False).wait_send()
            for k in range(TOKEN_SUBS):
                yt_copy(j, k, False).wait_send()
        for r in other_planes:
            drain_tokens(r)
        if relief:

            @pl.when(end)
            def _():
                end_meta().wait_send()
                end_down().wait_send()
                for k in range(TOKEN_SUBS):
                    end_tokens(k).wait_send()

            @pl.when(near)
            def _():
                for j in range(1, G):
                    for k in range(TOKEN_SUBS):
                        ey_copy(j, k, False).wait_send()
                for e in range(G):
                    drain_tokens(e, 1)
                    for item in range(2, 3 + last):
                        pp_copy(item, e).wait_send()
                for j in range(1, nt):
                    px_copy(j, False).wait_send()
                ue_copy().wait_send()

        @pl.when(~end)
        def _():
            for j in range(1, nt):
                part_copy(j, False).wait_send()

        for e, j in crossing:
            back_copy(e, j, False).wait_send()
        for j in range(1, nt):
            all_copy(j, False).wait_send()
        for ci in range(last + 2):
            others(lambda e, a: up_copy(ci, e, a).wait_send())

        @pl.loop(0, n)
        def _(a):
            @pl.when(a != me)
            def _():
                low_copy(a).wait_send()


def layer(G, relief, x, wq, wk, wv, aq, av, bq, bv, d, blocks_of, slots, ranks, live):
    n, nt = lax.axis_size("dp"), lax.axis_size("tensor")
    rows = x.shape[0]
    depth, qcols = wq.shape
    kcols = wk.shape[1]
    width = aq.shape[1]
    hq, hk = qcols // G, kcols // G
    widths = [c * HD for c in query_chunks(hq // HD)]
    span = n * depth
    blocks = rows // REQUEST_ROWS
    far = (n - 2) * depth
    cosine, sine = rope_tables(REQUEST_ROWS, HD)
    cosine = np.concatenate([cosine, cosine], axis=-1)
    sine = np.concatenate([-sine, sine], axis=-1)
    smem = pl.BlockSpec(memory_space=pltpu.SMEM)
    vmem = pl.BlockSpec(memory_space=pltpu.VMEM)
    hbm = pl.BlockSpec(memory_space=pltpu.HBM)
    bf, f32 = jnp.bfloat16, jnp.float32
    V = pltpu.VMEM
    dma = pltpu.SemaphoreType.DMA

    def pairs_of(shape):
        return [dma(shape), dma(shape)]

    return pl.pallas_call(
        functools.partial(layer_kernel, G, relief),
        out_shape=(
            jax.ShapeDtypeStruct((R, 2 * width + qcols + kcols), f32)
        ),
        in_specs=[smem] * 4 + [hbm] * 9 + [vmem] * 2,
        out_specs=vmem,
        scratch_shapes=[
            V((G, rows, span), bf),
            V((span, 2 * hk), bf),
            [V((span, w), bf) for w in widths],
            V((n, 2 * R, width), bf),
            V((n, G, R, hq + hk), bf),
            V((G, rows, hq), bf),
            V((G, rows, 2 * hk), f32),
            [V((G, rows, w), f32) for w in widths],
            V((nt, 2 * R, rows), f32),
            V((G + 1, 2 * R, rows), bf),
            V((G, rows, hk), bf),
            V((G, rows, hk), bf),
            V((G, rows, hk), f32),
            V((G, 2 * R, rows), f32),
            [V((G, n, R, w), f32) for w in widths],
            V((G, n, R, hk), f32),
            [V((G, n, R, w), bf) for w in widths],
            V((G, n, R, hk), bf),
            [V((n, G, R, w), bf) for w in widths],
            V((n, G, R, hk), bf),
            V((G, nt, 2 * R, rows // nt), bf),
            V((G, nt, 2 * R, rows // nt), bf),
            V((nt, 2 * R, rows // nt), bf),
            V((n, 2 * R, width), bf),
            V((n, 2 * R, width), bf),
            pltpu.SMEM((G + 1, 128), jnp.int32),
            V((G, rows, far) if relief else (1, 16, 128), bf),
            V((rows, width) if relief else (16, 128), bf),
            V((nt, 2 * R, rows) if relief else (1, 8, 128), f32),
            [V((G, rows, w) if relief else (1, 16, 128), bf) for w in widths],
            [V((G, rows, w) if relief else (1, 16, 128), bf) for w in widths],
        ]
        + [dma((8 + len(widths),))]
        + [dma((2, 2 + len(widths), n, SUBS)), dma((2 + len(widths), n, SUBS))]
        + pairs_of((G, 4))
        + pairs_of((G, TOKEN_SUBS))
        + pairs_of((2 * G, max(1, nt // 2), TOKEN_SUBS))
        + pairs_of((2 * G, nt, TOKEN_SUBS))
        + pairs_of((nt,))
        + pairs_of((G,))
        + [dma((1 + len(widths), G, n)), dma((1 + len(widths), n, G))]
        + pairs_of((G, nt))
        + pairs_of((n,))
        + [dma, dma]
        + pairs_of((TOKEN_SUBS,))
        + pairs_of((G, TOKEN_SUBS))
        + [dma, dma]
        + pairs_of((nt,))
        + [dma, dma]
        + pairs_of((len(widths), G))
        + pairs_of((nt,)),
        compiler_params=pltpu.CompilerParams(
            collective_id=0, has_side_effects=True, vmem_limit_bytes=62 * 1024 * 1024
        ),
        name="layer",
    )(blocks_of, slots, ranks, live, x, wq, wk, wv, aq, av, bq, bv, d, cosine, sine)


def on_device(
    tokens,
    w_query,
    w_key,
    w_value,
    a_query,
    b_query,
    a_value,
    b_value,
    adapter_ranks,
    adapter_slot,
    block_adapter,
    live_tokens,
    d_heads,
):
    ng, nt = lax.axis_size("groups"), lax.axis_size("tensor")
    kv_heads = w_key.shape[1] // HD
    G = ng if nt % 2 == 0 and kv_heads % ng == 0 else 1
    chunks = len(query_chunks(w_query.shape[1] // G // HD))
    relief = G > 1 and lax.axis_size("dp") >= 4 and chunks == 3
    out = layer(
        G, relief, tokens, w_query, w_key, w_value, a_query[0].T, a_value[0].T, b_query[0], b_value[0],
        d_heads, block_adapter.reshape(-1), adapter_slot, adapter_ranks, live_tokens,
    )
    width, qcols = a_query.shape[1], b_query.shape[2]
    low_q, low_v = out[:, :width], out[:, width : 2 * width]
    up_q, up_v = out[:, 2 * width : 2 * width + qcols], out[:, 2 * width + qcols :]
    return low_q.T[None], up_q[None], low_v.T[None], up_v[None]


def solution(mesh):
    in_specs = (
        P(("groups", "dp"), None),
        P("dp", "tensor"),
        P("dp", "tensor"),
        P("dp", "tensor"),
        P(("groups", "dp"), "tensor", None),
        P(("groups", "dp"), None, "tensor"),
        P(("groups", "dp"), "tensor", None),
        P(("groups", "dp"), None, "tensor"),
        P("groups"),
        P(),
        P(("groups", "dp"), None),
        P(("groups", "dp")),
        P(("groups", "dp"), "tensor"),
    )
    out_specs = (
        P(("groups", "dp"), "tensor", None),
        P(("groups", "dp"), None, "tensor"),
        P(("groups", "dp"), "tensor", None),
        P(("groups", "dp"), None, "tensor"),
    )
    return jax.shard_map(
        on_device, mesh=mesh, in_specs=in_specs, out_specs=out_specs, check_vma=False
    )
```
